32 devices in a mesh: seq: 8 (over z, x), batch: 4 (over y, core).
Axes of the slice: x: 2, y: 2, z: 4, core: 2. Of those that a mesh axis runs over, the one named last changes fastest.
Arguments:
- inputs: bfloat16 [4, 2048, 1024], P('batch', 'seq'), may hold values from -6 to 6
- cotangent: float32 [4, 2048, 1024], P('batch', 'seq'), may hold values from -6 to 6
- mixer_gain: bfloat16 [1024], P(('seq', 'batch')), may hold values from 0.5 to 1.5
- feed_gain: bfloat16 [1024], P(('seq', 'batch')), may hold values from 0.5 to 1.5
- w_query: bfloat16 [1024, 512], P(('seq', 'batch')), may hold values from -0.1875 to 0.1875
- w_key: bfloat16 [1024, 512], P(('seq', 'batch')), may hold values from -0.1875 to 0.1875
- w_value: bfloat16 [1024, 1024], P(('seq', 'batch')), may hold values from -0.1875 to 0.1875
- w_outgate: bfloat16 [1024, 1024], P(('seq', 'batch')), may hold values from -0.1875 to 0.1875
- w_decay_down: bfloat16 [1024, 16], P(('seq', 'batch')), may hold values from -0.1875 to 0.1875
- w_decay_up: bfloat16 [16, 512], P(None, ('seq', 'batch')), may hold values from -1.5 to 1.5
- decay_bias: bfloat16 [512], P(('seq', 'batch')), may hold values from -1 to 9
- head_gain: bfloat16 [256], P(('seq', 'batch')), may hold values from 0.5 to 1.5
- w_output: bfloat16 [1024, 1024], P(('seq', 'batch')), may hold values from -0.1875 to 0.1875
- w_gate: bfloat16 [1024, 2816], P(('seq', 'batch')), may hold values from -0.1875 to 0.1875
- w_up: bfloat16 [1024, 2816], P(('seq', 'batch')), may hold values from -0.1875 to 0.1875
- w_down: bfloat16 [2816, 1024], P(('seq', 'batch')), may hold values from -0.109375 to 0.109375
Outputs:
- block_output: float32 [4, 2048, 1024], P('batch', 'seq')
- input_grad: float32 [4, 2048, 1024], P('batch', 'seq')
- grad_mixer_gain: float32 [1024], P(('seq', 'batch'))
- grad_feed_gain: float32 [1024], P(('seq', 'batch'))
- grad_query: float32 [1024, 512], P(('seq', 'batch'))
- grad_key: float32 [1024, 512], P(('seq', 'batch'))
- grad_value: float32 [1024, 1024], P(('seq', 'batch'))
- grad_outgate: float32 [1024, 1024], P(('seq', 'batch'))
- grad_decay_down: float32 [1024, 16], P(('seq', 'batch'))
- grad_decay_up: float32 [16, 512], P(None, ('seq', 'batch'))
- grad_decay_bias: float32 [512], P(('seq', 'batch'))
- grad_head_gain: float32 [256], P(('seq', 'batch'))
- grad_output: float32 [1024, 1024], P(('seq', 'batch'))
- grad_gate: float32 [1024, 2816], P(('seq', 'batch'))
- grad_up: float32 [1024, 2816], P(('seq', 'batch'))
- grad_down: float32 [2816, 1024], P(('seq', 'batch'))
The draws below stay inside these ranges and needn't reach their ends.
All inputs are finite; a program needn't handle non-finite values.
Results may differ from the reference program's by a relative error of at most 0.035.
Values may be sent and summed in bfloat16 or wider, within the bound.
A program may use at most 192 MiB of HBM per device.

```python
import jax
import jax.numpy as jnp
from jax import lax

D = 1024
HEADS = 4
KEY_DIM = 128
VALUE_DIM = 256
RANK = 16
FF = 2816
GROUP = 64
KD = 512
VD = 1024
LEN = 2048
SEQS = 4


def level_of(key, extent, cuts, smallest, high):
    def one(dim, shards_of):
        steps = jax.random.uniform(jax.random.fold_in(jax.random.fold_in(key, 6), dim), (shards_of,), jnp.float32, smallest / len(cuts), high / len(cuts))
        return jnp.repeat(jnp.exp(steps), extent[dim] // shards_of).reshape((-1,) + (1,) * (len(extent) - dim - 1))

    factor_of = one(*cuts[0])
    for cut in cuts[1:]:
        factor_of = factor_of * one(*cut)
    return factor_of


def bell_draw(key, dims, deviation, limit, cuts=(), dtype=jnp.bfloat16):
    values = jax.random.normal(key, dims, jnp.float32) * deviation
    if len(cuts) > 0:
        values = level_of(key, dims, cuts, -0.22, 0.18) * values
    return jnp.clip(values, min=-limit, max=limit).astype(dtype)


def setup_inputs(seed: int = 0) -> dict:
    key_of = jax.random.split(jax.random.key(seed), 17)
    inputs = bell_draw(key_of[0], (SEQS, LEN, D), 1.0, 6.0, ((0, 4), (1, 8)))
    cotangent = bell_draw(key_of[1], (SEQS, LEN, D), 1.0, 6.0, ((0, 4), (1, 8)), jnp.float32)
    mixer_gain = jnp.clip(1.0 + 0.1 * jax.random.normal(key_of[2], (D,), jnp.float32), 0.5, 1.5).astype(jnp.bfloat16)
    feed_gain = jnp.clip(1.0 + 0.1 * jax.random.normal(key_of[3], (D,), jnp.float32), 0.5, 1.5).astype(jnp.bfloat16)
    w_query = bell_draw(key_of[4], (D, KD), D ** -0.5, 0.1875, ((0, 32),))
    w_key = bell_draw(key_of[5], (D, KD), D ** -0.5, 0.1875, ((0, 32),))
    w_value = bell_draw(key_of[6], (D, VD), D ** -0.5, 0.1875, ((0, 32),))
    w_outgate = bell_draw(key_of[7], (D, VD), D ** -0.5, 0.1875, ((0, 32),))
    w_decay_down = bell_draw(key_of[8], (D, RANK), D ** -0.5, 0.1875, ((0, 32),))
    w_decay_up = bell_draw(key_of[9], (RANK, KD), RANK ** -0.5, 1.5, ((1, 32),))
    decay_bias = jnp.clip(-1.0 + 10.0 * jax.random.uniform(key_of[10], (KD,), jnp.float32) ** level_of(key_of[10], (KD,), ((0, 32),), -0.2, 0.2), -1.0, 9.0).astype(jnp.bfloat16)
    head_gain = jnp.clip(1.0 + 0.1 * jax.random.normal(key_of[11], (VALUE_DIM,), jnp.float32), 0.5, 1.5).astype(jnp.bfloat16)
    w_output = bell_draw(key_of[12], (VD, D), VD ** -0.5, 0.1875, ((0, 32),))
    w_gate = bell_draw(key_of[13], (D, FF), D ** -0.5, 0.1875, ((0, 32),))
    w_up = bell_draw(key_of[14], (D, FF), D ** -0.5, 0.1875, ((0, 32),))
    w_down = bell_draw(key_of[15], (FF, D), FF ** -0.5, 0.109375, ((0, 32),))
    return {"inputs": inputs, "cotangent": cotangent, "mixer_gain": mixer_gain, "feed_gain": feed_gain, "w_query": w_query, "w_key": w_key, "w_value": w_value, "w_outgate": w_outgate, "w_decay_down": w_decay_down, "w_decay_up": w_decay_up, "decay_bias": decay_bias, "head_gain": head_gain, "w_output": w_output, "w_gate": w_gate, "w_up": w_up, "w_down": w_down}


epsilon = 1e-06
highest = lax.Precision.HIGHEST

def causal_mask():
    return jnp.tril(jnp.ones((GROUP, GROUP), jnp.float32))

def group_tables(query_scaled, key_full, log_decay):
    cumulative = jnp.cumsum(log_decay, axis=1)
    middle = cumulative[:, GROUP // 2 - 1:GROUP // 2]
    ending = cumulative[:, GROUP - 1:]
    gated_query = query_scaled * jnp.exp(cumulative - middle)
    inverse_key = key_full * jnp.exp(middle - cumulative)
    tail_key = key_full * jnp.exp(ending - cumulative)
    state_query = query_scaled * jnp.exp(cumulative)
    return (ending, gated_query, inverse_key, tail_key, state_query)

def group_forward(state, pieces):
    query_scaled, key_full, value_full, log_decay = pieces
    ending, gated_query, inverse_key, tail_key, state_query = group_tables(query_scaled, key_full, log_decay)
    scores = jnp.einsum('sthc,suhc->shtu', gated_query, inverse_key, precision=highest) * causal_mask()
    outputs = jnp.einsum('sthc,shcv->sthv', state_query, state, precision=highest)
    outputs = outputs + jnp.einsum('shtu,suhv->sthv', scores, value_full, precision=highest)
    new_state = jnp.exp(ending[:, 0])[..., None] * state
    new_state = new_state + jnp.einsum('suhc,suhv->shcv', tail_key, value_full, precision=highest)
    return (new_state, outputs)

def split_groups(array):
    lead, length = (array.shape[0], array.shape[1])
    shaped = array.reshape(lead, length // GROUP, GROUP, array.shape[2], array.shape[3])
    return jnp.moveaxis(shaped, 1, 0)

def join_groups(array):
    moved = jnp.moveaxis(array, 0, 1)
    return moved.reshape(moved.shape[0], moved.shape[1] * moved.shape[2], moved.shape[3], moved.shape[4])

def gla_core(query_scaled, key_full, value_full, log_decay):
    start = jnp.zeros((query_scaled.shape[0], HEADS, KEY_DIM, VALUE_DIM), jnp.float32)
    pieces = (split_groups(query_scaled), split_groups(key_full), split_groups(value_full), split_groups(log_decay))
    final_state, outputs = lax.scan(group_forward, start, pieces)
    return join_groups(outputs)

def rms_apply(values, gain):
    scale = lax.rsqrt(lax.optimization_barrier(jnp.mean(values * values, axis=-1, keepdims=True)) + epsilon)
    return values * scale * gain

def gate_apply(mixed, gate_heads, norm_head):
    return rms_apply(mixed, norm_head) * gate_heads * jax.nn.sigmoid(gate_heads)

def swiglu_apply(up_gate, up_lin):
    return up_gate * jax.nn.sigmoid(up_gate) * up_lin

def decay_apply(decay_pre):
    return jax.nn.log_sigmoid(decay_pre) / 16.0

def matmul(left, right):
    return jnp.dot(left, right, preferred_element_type=jnp.float32)

def reference(inputs, cotangent, mixer_gain, feed_gain, w_query, w_key, w_value, w_outgate, w_decay_down, w_decay_up, decay_bias, head_gain, w_output, w_gate, w_up, w_down):
    weights = (mixer_gain, feed_gain, w_query, w_key, w_value, w_outgate, w_decay_down, w_decay_up, decay_bias, head_gain, w_output, w_gate, w_up, w_down)
    key_scale = KEY_DIM ** (-0.5)

    def one_sequence(totals, pair):
        tokens, grad_rows = pair
        length = tokens.shape[0]
        hidden_in = tokens.astype(jnp.float32)
        normed_f, norm_one_vjp = jax.vjp(rms_apply, hidden_in, mixer_gain.astype(jnp.float32))
        normed = normed_f.astype(jnp.bfloat16)
        query_b = matmul(normed, w_query).astype(jnp.bfloat16)
        key_b = matmul(normed, w_key).astype(jnp.bfloat16)
        value_b = matmul(normed, w_value).astype(jnp.bfloat16)
        gate_pre = matmul(normed, w_outgate)
        rank_act = matmul(normed, w_decay_down).astype(jnp.bfloat16)
        decay_pre = matmul(rank_act, w_decay_up) + decay_bias.astype(jnp.float32)
        log_decay, decay_vjp = jax.vjp(decay_apply, decay_pre)
        shape_key = (1, length, HEADS, KEY_DIM)
        shape_value = (1, length, HEADS, VALUE_DIM)
        query_scaled = query_b.astype(jnp.float32).reshape(shape_key) * key_scale
        key_full = key_b.astype(jnp.float32).reshape(shape_key)
        value_full = value_b.astype(jnp.float32).reshape(shape_value)
        mixed, core_vjp = jax.vjp(gla_core, query_scaled, key_full, value_full, log_decay.reshape(shape_key))
        gated_f, gate_vjp = jax.vjp(gate_apply, mixed, gate_pre.reshape(shape_value), head_gain.astype(jnp.float32))
        gated = gated_f.astype(jnp.bfloat16).reshape(length, HEADS * VALUE_DIM)
        middle = hidden_in + matmul(gated, w_output)
        normed_two_f, norm_two_vjp = jax.vjp(rms_apply, middle, feed_gain.astype(jnp.float32))
        normed_two = normed_two_f.astype(jnp.bfloat16)
        up_gate = matmul(normed_two, w_gate)
        up_lin = matmul(normed_two, w_up)
        activated_f, swiglu_vjp = jax.vjp(swiglu_apply, up_gate, up_lin)
        activated = activated_f.astype(jnp.bfloat16)
        result = middle + matmul(activated, w_down)
        grad_b = grad_rows.astype(jnp.bfloat16)
        grad_down = matmul(activated.T, grad_b)
        act_grad = matmul(grad_b, w_down.T)
        gate_grad_f, lin_grad_f = swiglu_vjp(act_grad)
        gate_grad = gate_grad_f.astype(jnp.bfloat16)
        lin_grad = lin_grad_f.astype(jnp.bfloat16)
        grad_gate = matmul(normed_two.T, gate_grad)
        grad_up = matmul(normed_two.T, lin_grad)
        normed_two_grad = matmul(gate_grad, w_gate.T) + matmul(lin_grad, w_up.T)
        middle_part, grad_feed_gain = norm_two_vjp(normed_two_grad)
        middle_grad = grad_rows + middle_part
        middle_b = middle_grad.astype(jnp.bfloat16)
        grad_output = matmul(gated.T, middle_b)
        gated_grad = matmul(middle_b, w_output.T).reshape(shape_value)
        mixed_grad, gate_heads_grad, grad_head_gain = gate_vjp(gated_grad)
        outgate_grad = gate_heads_grad.reshape(length, HEADS * VALUE_DIM).astype(jnp.bfloat16)
        query_grad_f, key_grad_f, value_grad_f, log_grad = core_vjp(mixed_grad)
        query_grad = (query_grad_f * key_scale).reshape(length, HEADS * KEY_DIM).astype(jnp.bfloat16)
        key_grad = key_grad_f.reshape(length, HEADS * KEY_DIM).astype(jnp.bfloat16)
        value_grad = value_grad_f.reshape(length, HEADS * VALUE_DIM).astype(jnp.bfloat16)
        decay_grad = decay_vjp(log_grad.reshape(length, HEADS * KEY_DIM))[0]
        grad_decay_bias = lax.optimization_barrier(jnp.sum(decay_grad, axis=0))
        decay_grad_b = decay_grad.astype(jnp.bfloat16)
        grad_decay_up = matmul(rank_act.T, decay_grad_b)
        rank_grad = matmul(decay_grad_b, w_decay_up.T).astype(jnp.bfloat16)
        grad_decay_down = matmul(normed.T, rank_grad)
        grad_query = matmul(normed.T, query_grad)
        grad_key = matmul(normed.T, key_grad)
        grad_value = matmul(normed.T, value_grad)
        grad_outgate = matmul(normed.T, outgate_grad)
        normed_grad = matmul(query_grad, w_query.T) + matmul(key_grad, w_key.T) + matmul(value_grad, w_value.T)
        normed_grad = normed_grad + matmul(outgate_grad, w_outgate.T) + matmul(rank_grad, w_decay_down.T)
        input_part, grad_mixer_gain = norm_one_vjp(normed_grad)
        input_grad = middle_grad + input_part
        grads = (grad_mixer_gain, grad_feed_gain, grad_query, grad_key, grad_value, grad_outgate, grad_decay_down, grad_decay_up, grad_decay_bias, grad_head_gain, grad_output, grad_gate, grad_up, grad_down)
        updated = tuple((total + grad for total, grad in zip(totals, grads)))
        return (updated, (result, input_grad))
    start = tuple((jnp.zeros(weight.shape, jnp.float32) for weight in weights))
    totals, (results, input_grads) = lax.scan(one_sequence, start, (inputs, cotangent))
    return (results, input_grads, totals[0], totals[1], totals[2], totals[3], totals[4], totals[5], totals[6], totals[7], totals[8], totals[9], totals[10], totals[11], totals[12], totals[13])
```

```python
import functools

import jax
import jax.numpy as jnp
from jax import lax
from jax.experimental import pallas as pl
from jax.experimental.pallas import tpu as pltpu
from jax.sharding import PartitionSpec as P

HEADS = 4
KEY_DIM = 128
VALUE_DIM = 256
GROUP = 64
LANES = 128
MESH = pl.DeviceIdType.MESH

epsilon = 1e-06
highest = lax.Precision.HIGHEST


def grid_of(shape):
    seq, batch = shape["seq"], shape["batch"]
    outer = 4 if seq % 4 == 0 else seq
    core = 2 if batch % 2 == 0 else 1
    return (outer, seq // outer, batch // core, core)


def coords_of(sizes):
    seq, batch = lax.axis_index("seq"), lax.axis_index("batch")
    return (seq // sizes[1], seq % sizes[1], batch // sizes[3], batch % sizes[3])


def device_of(sizes, at):
    return {"seq": at[0] * sizes[1] + at[1], "batch": at[2] * sizes[3] + at[3]}


def moved(sizes, at, axis, by):
    new = list(at)
    new[axis] = lax.rem(at[axis] + (by % sizes[axis]), sizes[axis])
    return tuple(new)


def region(ref, free, at):
    return ref.at[tuple(slice(None) if k in free else at[k] for k in range(4))]


def orders_of(sizes):
    if sizes[1] == sizes[2] and sizes[3] == 2:
        return ((0, 1, 2, 3), (0, 2, 1, 3))
    return ((0, 1, 2, 3),)


def greet(sizes, at):
    barrier = pltpu.get_barrier_semaphore()
    count = 0
    for axis in range(4):
        for by in range(1, sizes[axis]):
            pl.semaphore_signal(
                barrier,
                inc=1,
                device_id=device_of(sizes, moved(sizes, at, axis, by)),
                device_id_type=MESH,
            )
            count += 1
    pl.semaphore_wait(barrier, count)


def gather_kernel(sizes, count, *refs):
    shards, wholes = refs[:count], refs[count : 2 * count]
    send_sem, recv_sem, own_sem = refs[2 * count :]
    at = coords_of(sizes)
    greet(sizes, at)

    def copies(item, order, step, arriving):
        axis, free = order[step], order[:step]
        made = []
        for by in range(1, sizes[axis]):
            source = moved(sizes, at, axis, -by) if arriving else at
            place = region(wholes[item], free, source)
            made.append(
                pltpu.make_async_remote_copy(
                    src_ref=shards[item] if step == 0 and not arriving else place,
                    dst_ref=place,
                    send_sem=send_sem.at[item, step, by - 1],
                    recv_sem=recv_sem.at[item, step, by - 1],
                    device_id=device_of(sizes, moved(sizes, at, axis, by)),
                    device_id_type=MESH,
                )
            )
        return made

    def start(item, order, step):
        for copy in copies(item, order, step, False):
            copy.start()

    def arrive(item, order, step):
        for copy in copies(item, order, step, True):
            copy.wait_recv()

    def own(item):
        return pltpu.make_async_copy(
            shards[item], region(wholes[item], (), at), own_sem.at[item]
        )

    def run(order):
        for item in range(count):
            start(item, order, 0)
            own(item).start()
        for tick in range(count + 3):
            for step in (1, 2, 3):
                item = tick - step + 1
                if 0 <= item < count:
                    arrive(item, order, step - 1)
                    if step == 1:
                        own(item).wait()
                    start(item, order, step)
            if tick >= 3:
                arrive(tick - 3, order, 3)
        for item in range(count):
            for step in range(4):
                for copy in copies(item, order, step, False):
                    copy.wait_send()

    orders = orders_of(sizes)
    for parity, order in enumerate(orders):
        pl.when(lax.rem(at[3], len(orders)) == parity)(functools.partial(run, order))


def gather_all(sizes, shards, collective_id):
    count = len(shards)
    most = max(max(sizes) - 1, 1)
    wholes = pl.pallas_call(
        functools.partial(gather_kernel, sizes, count),
        out_shape=[jax.ShapeDtypeStruct(sizes + s.shape, s.dtype) for s in shards],
        in_specs=[pl.BlockSpec(memory_space=pltpu.VMEM)] * count,
        out_specs=[pl.BlockSpec(memory_space=pl.ANY)] * count,
        scratch_shapes=[
            pltpu.SemaphoreType.DMA((count, 4, most)),
            pltpu.SemaphoreType.DMA((count, 4, most)),
            pltpu.SemaphoreType.DMA((count,)),
        ],
        compiler_params=pltpu.CompilerParams(
            collective_id=collective_id, has_side_effects=True
        ),
    )(*shards)
    return [w.reshape((-1,) + w.shape[4:]) for w in wholes]


def scatter_kernel(sizes, count, *refs):
    grads, outs = refs[:count], refs[count : 2 * count]
    held, near, half, part, last = (
        refs[(2 + k) * count : (3 + k) * count] for k in range(5)
    )
    send_sem, recv_sem, own_sem = refs[7 * count :]
    at = coords_of(sizes)
    greet(sizes, at)

    def landing(item, order, step, by):
        if step == 3:
            return near[item]
        return (last, part, half)[step][item].at[by - 1]

    def copy(item, order, step, by):
        axis, free = order[step], order[:step]
        target = moved(sizes, at, axis, by)
        source = grads[item] if step == 3 else held[item]
        index = tuple(
            slice(None) if k in free else target[k] for k in range(4 if step == 3 else 3)
        )
        return pltpu.make_async_remote_copy(
            src_ref=source.at[index],
            dst_ref=landing(item, order, step, by),
            send_sem=send_sem.at[item, step, by - 1],
            recv_sem=recv_sem.at[item, step, by - 1],
            device_id=device_of(sizes, target),
            device_id_type=MESH,
        )

    def start(item, order, step):
        for by in range(1, sizes[order[step]]):
            copy(item, order, step, by).start()

    def own(item):
        return pltpu.make_async_copy(
            region(grads[item], (0, 1, 2), at), held[item], own_sem.at[item]
        )

    def gather_in(item, order, step):
        axis, free = order[step], order[:step]
        for by in range(1, sizes[axis]):
            copy(item, order, step, by).wait_recv()
        if step == 0:
            total = held[item][at[0], at[1], at[2]].astype(jnp.float32)
            for by in range(1, sizes[axis]):
                total = total + last[item][by - 1].astype(jnp.float32)
            outs[item][...] = total
            return

        def add(k, carry):
            for j in range(sizes[free[1]] if len(free) > 1 else 1):
                for i in range(sizes[free[2]] if len(free) > 2 else 1):
                    within = (k, j, i)[: len(free)]
                    place = list(at[:3])
                    for axis_of, index in zip(free, within):
                        place[axis_of] = index
                    place = tuple(place)
                    total = held[item][place].astype(jnp.float32)
                    if step == 3:
                        total = total + near[item][place].astype(jnp.float32)
                    else:
                        for by in range(1, sizes[axis]):
                            total = total + landing(item, order, step, by)[
                                within
                            ].astype(jnp.float32)
                    held[item][place] = total.astype(held[item].dtype)
            return carry

        lax.fori_loop(0, sizes[0], add, 0)

    def run(order):
        for item in range(count):
            start(item, order, 3)
            own(item).start()
        for tick in range(count + 3):
            for step in (3, 2, 1, 0):
                item = tick - (3 - step)
                if 0 <= item < count:
                    if step == 3:
                        own(item).wait()
                    gather_in(item, order, step)
                    if step > 0:
                        start(item, order, step - 1)
        for item in range(count):
            for step in range(4):
                for by in range(1, sizes[order[step]]):
                    copy(item, order, step, by).wait_send()

    orders = orders_of(sizes)
    for parity, order in enumerate(orders):
        pl.when(lax.rem(at[3], len(orders)) == parity)(functools.partial(run, order))


def scatter_all(sizes, grads, collective_id):
    outer, inner, side, core = sizes
    count = len(grads)
    most = max(max(sizes) - 1, 1)
    shaped = [
        g.reshape(sizes + (g.shape[0] // (outer * inner * side * core), g.shape[1])) for g in grads
    ]
    blocks = [(g.shape[4:], g.dtype) for g in shaped]

    def buffers(lead):
        return [pltpu.VMEM(lead + block, dtype) for block, dtype in blocks]

    return pl.pallas_call(
        functools.partial(scatter_kernel, sizes, count),
        out_shape=[jax.ShapeDtypeStruct(block, jnp.float32) for block, _ in blocks],
        in_specs=[pl.BlockSpec(memory_space=pl.ANY)] * count,
        out_specs=[pl.BlockSpec(memory_space=pltpu.VMEM)] * count,
        scratch_shapes=buffers((outer, inner, side))
        + buffers((outer, inner, side))
        + buffers((max(side - 1, 1), outer, inner))
        + buffers((max(inner - 1, 1), outer))
        + buffers((max(outer - 1, 1),))
        + [
            pltpu.SemaphoreType.DMA((count, 4, most)),
            pltpu.SemaphoreType.DMA((count, 4, most)),
            pltpu.SemaphoreType.DMA((count,)),
        ],
        compiler_params=pltpu.CompilerParams(
            collective_id=collective_id, has_side_effects=True, vmem_limit_bytes=60 * 2**20
        ),
    )(*shaped)


def entering(value, axis, reverse):
    length = lax.axis_size(axis)

    def shifted(pair, by):
        pairs = [
            (k, k - by if reverse else k + by)
            for k in range(length)
            if 0 <= (k - by if reverse else k + by) < length
        ]
        decay, state = pair
        moved_state = lax.ppermute(state.astype(jnp.bfloat16), axis, pairs)
        return (lax.ppermute(decay, axis, pairs), moved_state.astype(jnp.float32))

    def combine(earlier, later):
        return (earlier[0] * later[0], later[0][..., None] * earlier[1] + later[1])

    whole, before, by = value, None, 1
    while by < length:
        come = shifted(whole, by)
        before = come if before is None else combine(come, before)
        whole = combine(come, whole)
        by *= 2
    return before[1]


def small_pack(parts, rows):
    columns = []
    for k, part in enumerate(parts):
        if k not in (0, 3):
            part = part[..., None]
        spare = [(0, 0)] * (part.ndim - 2) + [(0, rows - part.shape[-2]), (0, 0)]
        columns.append(jnp.pad(part, spare))
    joined = jnp.concatenate(columns, axis=-1)
    spare = [(0, 0)] * (joined.ndim - 1) + [(0, LANES - joined.shape[-1])]
    return jnp.pad(joined, spare)


def causal_mask():
    return jnp.tril(jnp.ones((GROUP, GROUP), jnp.float32))


def group_tables(query_scaled, key_full, log_decay):
    cumulative = jnp.cumsum(log_decay, axis=1)
    middle = cumulative[:, GROUP // 2 - 1 : GROUP // 2]
    ending = cumulative[:, GROUP - 1 :]
    gated_query = query_scaled * jnp.exp(cumulative - middle)
    inverse_key = key_full * jnp.exp(middle - cumulative)
    tail_key = key_full * jnp.exp(ending - cumulative)
    state_query = query_scaled * jnp.exp(cumulative)
    return (cumulative, middle, ending, gated_query, inverse_key, tail_key, state_query)


def group_forward(state, pieces):
    query_scaled, key_full, value_full, log_decay = pieces
    cumulative, middle, ending, gated_query, inverse_key, tail_key, state_query = group_tables(
        query_scaled, key_full, log_decay
    )
    scores = (
        jnp.einsum("sthc,suhc->shtu", gated_query, inverse_key, precision=highest) * causal_mask()
    )
    outputs = jnp.einsum("sthc,shcv->sthv", state_query, state, precision=highest)
    outputs = outputs + jnp.einsum("shtu,suhv->sthv", scores, value_full, precision=highest)
    new_state = jnp.exp(ending[:, 0])[..., None] * state
    new_state = new_state + jnp.einsum("suhc,suhv->shcv", tail_key, value_full, precision=highest)
    return (new_state, (outputs, state))


def group_backward(grad_state, pieces):
    query_scaled, key_full, value_full, log_decay, grad_out, state = pieces
    cumulative, middle, ending, gated_query, inverse_key, tail_key, state_query = group_tables(
        query_scaled, key_full, log_decay
    )
    lower = causal_mask()
    scores = jnp.einsum("sthc,suhc->shtu", gated_query, inverse_key, precision=highest) * lower
    grad_scores = jnp.einsum("sthv,suhv->shtu", grad_out, value_full, precision=highest) * lower
    grad_query = jnp.exp(cumulative) * jnp.einsum(
        "sthv,shcv->sthc", grad_out, state, precision=highest
    )
    grad_query = grad_query + jnp.exp(cumulative - middle) * jnp.einsum(
        "shtu,suhc->sthc", grad_scores, inverse_key, precision=highest
    )
    grad_key = jnp.exp(middle - cumulative) * jnp.einsum(
        "shtu,sthc->suhc", grad_scores, gated_query, precision=highest
    )
    grad_key = grad_key + jnp.exp(ending - cumulative) * jnp.einsum(
        "suhv,shcv->suhc", value_full, grad_state, precision=highest
    )
    grad_value = jnp.einsum("shtu,sthv->suhv", scores, grad_out, precision=highest)
    grad_value = grad_value + jnp.einsum("suhc,shcv->suhv", tail_key, grad_state, precision=highest)
    decay_end = jnp.exp(ending[:, 0])[..., None]
    end_state = decay_end * state + jnp.einsum(
        "suhc,suhv->shcv", tail_key, value_full, precision=highest
    )
    grad_cumul = query_scaled * grad_query - key_full * grad_key
    grad_log = jnp.einsum("ut,suhc->sthc", lower, grad_cumul, precision=highest)
    grad_log = grad_log + jnp.sum(end_state * grad_state, axis=-1)[:, None]
    previous = decay_end * grad_state + jnp.einsum(
        "sthc,sthv->shcv", state_query, grad_out, precision=highest
    )
    return (previous, (grad_query, grad_key, grad_value, grad_log))


def split_groups(array):
    lead, length = (array.shape[0], array.shape[1])
    shaped = array.reshape(lead, length // GROUP, GROUP, array.shape[2], array.shape[3])
    return jnp.moveaxis(shaped, 1, 0)


def join_groups(array):
    moved = jnp.moveaxis(array, 0, 1)
    return moved.reshape(
        moved.shape[0], moved.shape[1] * moved.shape[2], moved.shape[3], moved.shape[4]
    )


def matmul(left, right):
    return jnp.dot(left, right, preferred_element_type=jnp.float32)


def contract_rows(left, right):
    return lax.dot_general(
        left, right, (((0,), (0,)), ((), ())), preferred_element_type=jnp.float32
    )


def times_transpose(left, right):
    return lax.dot_general(
        left, right, (((1,), (1,)), ((), ())), preferred_element_type=jnp.float32
    )


def local(
    sizes,
    inputs,
    cotangent,
    mixer_gain,
    feed_gain,
    w_query,
    w_key,
    w_value,
    w_outgate,
    w_decay_down,
    w_decay_up,
    decay_bias,
    head_gain,
    w_output,
    w_gate,
    w_up,
    w_down,
):
    rows_of, kd_here, vd_here = w_query.shape[0], w_decay_up.shape[1], head_gain.shape[0]
    small = small_pack(
        (w_decay_down, mixer_gain, feed_gain, w_decay_up.T, decay_bias, head_gain), rows_of
    )
    shards = (
        small, w_query, w_key, w_value, w_outgate, w_output, w_gate, w_up, w_down
    )
    whole = gather_all(sizes, shards, 0)
    devices = whole[0].shape[0]
    small_all = whole[0]
    decay_down = small_all[:, :, 0:16].reshape(-1, 16)
    gain_one = small_all[:, :, 16].reshape(-1)
    gain_two = small_all[:, :, 17].reshape(-1)
    decay_up = small_all[:, :kd_here, 18:34].reshape(-1, 16).T
    bias_full = small_all[:, :kd_here, 34].reshape(-1)
    norm_head = small_all[:, :vd_here, 35].reshape(-1)
    (proj_query, proj_key, proj_value, proj_gate, proj_output, feed_gate, feed_up, feed_down) = (
        w.reshape(-1, w.shape[-1]) for w in whole[1:]
    )
    seqs_here, tokens_here, width = inputs.shape
    rows = seqs_here * tokens_here
    key_scale = KEY_DIM ** (-0.5)
    shape_key = (seqs_here, tokens_here, HEADS, KEY_DIM)
    shape_value = (seqs_here, tokens_here, HEADS, VALUE_DIM)
    hidden_in = inputs.reshape(rows, width).astype(jnp.float32)
    mixer_scale = lax.rsqrt(jnp.mean(hidden_in * hidden_in, axis=-1, keepdims=True) + epsilon)
    normed = (hidden_in * mixer_scale * gain_one.astype(jnp.float32)).astype(jnp.bfloat16)
    query_b = matmul(normed, proj_query).astype(jnp.bfloat16)
    key_b = matmul(normed, proj_key).astype(jnp.bfloat16)
    value_b = matmul(normed, proj_value).astype(jnp.bfloat16)
    gate_pre = matmul(normed, proj_gate)
    rank_act = matmul(normed, decay_down).astype(jnp.bfloat16)
    decay_pre = matmul(rank_act, decay_up) + bias_full.astype(jnp.float32)
    log_decay = jax.nn.log_sigmoid(decay_pre) / 16.0
    query_scaled = query_b.astype(jnp.float32).reshape(shape_key) * key_scale
    key_full = key_b.astype(jnp.float32).reshape(shape_key)
    value_full = value_b.astype(jnp.float32).reshape(shape_value)
    decay_rows = log_decay.reshape(shape_key)
    cumulative_dev = jnp.cumsum(decay_rows, axis=1)
    total = cumulative_dev[:, -1]
    decay_total = jnp.exp(total)
    local_state = jnp.einsum(
        "sthc,sthv->shcv",
        key_full * jnp.exp(total[:, None] - cumulative_dev),
        value_full,
        precision=highest,
    )
    start_state = entering((decay_total, local_state), "seq", False)
    group_pieces = (
        split_groups(query_scaled),
        split_groups(key_full),
        split_groups(value_full),
        split_groups(decay_rows),
    )
    final_state, (group_out, group_starts) = lax.scan(group_forward, start_state, group_pieces)
    mixed = join_groups(group_out)
    head_scale = lax.rsqrt(jnp.mean(mixed * mixed, axis=-1, keepdims=True) + epsilon)
    head_normed = mixed * head_scale * norm_head.astype(jnp.float32)
    gate_heads = gate_pre.reshape(shape_value)
    gate_sig = jax.nn.sigmoid(gate_heads)
    swish = gate_heads * gate_sig
    gated = (head_normed * swish).astype(jnp.bfloat16).reshape(rows, HEADS * VALUE_DIM)
    middle = hidden_in + matmul(gated, proj_output)
    feed_scale = lax.rsqrt(jnp.mean(middle * middle, axis=-1, keepdims=True) + epsilon)
    normed_two = (middle * feed_scale * gain_two.astype(jnp.float32)).astype(jnp.bfloat16)
    up_gate = matmul(normed_two, feed_gate)
    up_lin = matmul(normed_two, feed_up)
    up_sig = jax.nn.sigmoid(up_gate)
    activated = (up_gate * up_sig * up_lin).astype(jnp.bfloat16)
    result = middle + matmul(activated, feed_down)
    grad_rows = cotangent.reshape(rows, width)
    grad_b = grad_rows.astype(jnp.bfloat16)
    grad_down = contract_rows(activated, grad_b)
    act_grad = times_transpose(grad_b, feed_down)
    gate_grad = (act_grad * up_lin * up_sig * (1.0 + up_gate * (1.0 - up_sig))).astype(jnp.bfloat16)
    lin_grad = (act_grad * up_gate * up_sig).astype(jnp.bfloat16)
    grad_gate = contract_rows(normed_two, gate_grad)
    grad_up = contract_rows(normed_two, lin_grad)
    normed_two_grad = times_transpose(gate_grad, feed_gate) + times_transpose(lin_grad, feed_up)
    grad_feed_gain = jnp.sum(normed_two_grad * middle * feed_scale, axis=0)
    scaled_two = normed_two_grad * gain_two.astype(jnp.float32)
    middle_grad = (
        grad_rows
        + feed_scale * scaled_two
        - middle * feed_scale**3 * jnp.mean(scaled_two * middle, axis=-1, keepdims=True)
    )
    middle_b = middle_grad.astype(jnp.bfloat16)
    grad_output = contract_rows(gated, middle_b)
    gated_grad = times_transpose(middle_b, proj_output).reshape(shape_value)
    head_normed_grad = gated_grad * swish
    grad_head_gain = jnp.sum(head_normed_grad * mixed * head_scale, axis=(0, 1, 2))
    scaled_head = head_normed_grad * norm_head.astype(jnp.float32)
    mixed_grad = head_scale * scaled_head - mixed * head_scale**3 * jnp.mean(
        scaled_head * mixed, axis=-1, keepdims=True
    )
    outgate_grad = (
        (gated_grad * head_normed * gate_sig * (1.0 + gate_heads * (1.0 - gate_sig)))
        .reshape(rows, HEADS * VALUE_DIM)
        .astype(jnp.bfloat16)
    )
    local_grad = jnp.einsum(
        "sthc,sthv->shcv", query_scaled * jnp.exp(cumulative_dev), mixed_grad, precision=highest
    )
    end_grad = entering((decay_total, local_grad), "seq", True)
    back_pieces = group_pieces + (split_groups(mixed_grad), group_starts)
    begin_grad, (query_groups, key_groups, value_groups, log_groups) = lax.scan(
        group_backward, end_grad, back_pieces, reverse=True
    )
    query_grad = (
        (join_groups(query_groups) * key_scale).reshape(rows, HEADS * KEY_DIM).astype(jnp.bfloat16)
    )
    key_grad = join_groups(key_groups).reshape(rows, HEADS * KEY_DIM).astype(jnp.bfloat16)
    value_grad = join_groups(value_groups).reshape(rows, HEADS * VALUE_DIM).astype(jnp.bfloat16)
    log_grad = join_groups(log_groups).reshape(rows, HEADS * KEY_DIM)
    decay_grad = log_grad * jax.nn.sigmoid(-decay_pre) / 16.0
    grad_decay_bias = jnp.sum(decay_grad, axis=0)
    decay_grad_b = decay_grad.astype(jnp.bfloat16)
    grad_decay_up = contract_rows(rank_act, decay_grad_b)
    rank_grad = times_transpose(decay_grad_b, decay_up).astype(jnp.bfloat16)
    grad_decay_down = contract_rows(normed, rank_grad)
    grad_query = contract_rows(normed, query_grad)
    grad_key = contract_rows(normed, key_grad)
    grad_value = contract_rows(normed, value_grad)
    grad_outgate = contract_rows(normed, outgate_grad)
    normed_grad = (
        times_transpose(query_grad, proj_query)
        + times_transpose(key_grad, proj_key)
        + times_transpose(value_grad, proj_value)
    )
    normed_grad = (
        normed_grad
        + times_transpose(outgate_grad, proj_gate)
        + times_transpose(rank_grad, decay_down)
    )
    grad_mixer_gain = jnp.sum(normed_grad * hidden_in * mixer_scale, axis=0)
    scaled_one = normed_grad * gain_one.astype(jnp.float32)
    input_grad = (
        middle_grad
        + mixer_scale * scaled_one
        - hidden_in * mixer_scale**3 * jnp.mean(scaled_one * hidden_in, axis=-1, keepdims=True)
    )
    small_grad = small_pack(
        (
            grad_decay_down.reshape(devices, rows_of, -1),
            grad_mixer_gain.reshape(devices, rows_of),
            grad_feed_gain.reshape(devices, rows_of),
            grad_decay_up.T.reshape(devices, kd_here, -1),
            grad_decay_bias.reshape(devices, kd_here),
            grad_head_gain.reshape(devices, vd_here),
        ),
        rows_of,
    ).reshape(devices * rows_of, LANES)
    bf = jnp.bfloat16
    summed = scatter_all(
        sizes,
        (
            grad_down.astype(bf),
            grad_gate.astype(bf),
            grad_up.astype(bf),
            grad_output.astype(bf),
            grad_query.astype(bf),
            grad_key.astype(bf),
            grad_value.astype(bf),
            grad_outgate.astype(bf),
            small_grad,
        ),
        1,
    )
    sum_down, sum_gate, sum_up, sum_output, sum_query, sum_key, sum_value, sum_outgate, mine = (
        summed
    )
    summed = (
        mine[:, 16],
        mine[:, 17],
        sum_query,
        sum_key,
        sum_value,
        sum_outgate,
        mine[:, 0:16],
        mine[:kd_here, 18:34].T,
        mine[:kd_here, 34],
        mine[:vd_here, 35],
        sum_output,
        sum_gate,
        sum_up,
        sum_down,
    )
    return (result.reshape(inputs.shape), input_grad.reshape(inputs.shape)) + tuple(summed)


def solution(mesh):
    placed = (
        P("batch", "seq", None),
        P("batch", "seq", None),
        P(("seq", "batch")),
        P(("seq", "batch")),
        P(("seq", "batch"), None),
        P(("seq", "batch"), None),
        P(("seq", "batch"), None),
        P(("seq", "batch"), None),
        P(("seq", "batch"), None),
        P(None, ("seq", "batch")),
        P(("seq", "batch")),
        P(("seq", "batch")),
        P(("seq", "batch"), None),
        P(("seq", "batch"), None),
        P(("seq", "batch"), None),
        P(("seq", "batch"), None),
    )
    return jax.shard_map(
        functools.partial(local, grid_of(mesh.shape)),
        mesh=mesh,
        in_specs=placed,
        out_specs=(
            P("batch", "seq", None),
            P("batch", "seq", None),
            P(("seq", "batch")),
            P(("seq", "batch")),
            P(("seq", "batch"), None),
            P(("seq", "batch"), None),
            P(("seq", "batch"), None),
            P(("seq", "batch"), None),
            P(("seq", "batch"), None),
            P(None, ("seq", "batch")),
            P(("seq", "batch")),
            P(("seq", "batch")),
            P(("seq", "batch"), None),
            P(("seq", "batch"), None),
            P(("seq", "batch"), None),
            P(("seq", "batch"), None),
        ),
        check_vma=False,
    )
```

```python
import functools

import jax
import jax.numpy as jnp
from jax import lax
from jax.experimental import pallas as pl
from jax.experimental.pallas import tpu as pltpu
from jax.sharding import PartitionSpec as P

HEADS = 4
KEY_DIM = 128
VALUE_DIM = 256
GROUP = 64
LANES = 128
RANK = 16
VECTORS = 32
MESH = pl.DeviceIdType.MESH
VMEM_LIMIT = 63 * 2**20

epsilon = 1e-06
key_scale = KEY_DIM ** (-0.5)
highest = lax.Precision.HIGHEST
high = lax.Precision.HIGH
f32 = jnp.float32
bf16 = jnp.bfloat16


def grid_of(shape):
    seq, batch = shape["seq"], shape["batch"]
    outer = 4 if seq % 4 == 0 else seq
    core = 2 if batch % 2 == 0 else 1
    return (outer, seq // outer, batch // core, core)


def coords_of(sizes):
    seq, batch = lax.axis_index("seq"), lax.axis_index("batch")
    return (seq // sizes[1], seq % sizes[1], batch // sizes[3], batch % sizes[3])


def device_of(sizes, at):
    return {"seq": at[0] * sizes[1] + at[1], "batch": at[2] * sizes[3] + at[3]}


def moved(sizes, at, axis, by):
    new = list(at)
    new[axis] = lax.rem(at[axis] + (by % sizes[axis]), sizes[axis])
    return tuple(new)


def region(ref, free, at):
    return ref.at[tuple(slice(None) if k in free else at[k] for k in range(4))]


def orders_of(sizes):
    if sizes[1] == sizes[2] and sizes[3] == 2:
        return ((0, 1, 2, 3), (0, 2, 1, 3))
    return ((0, 1, 2, 3),)


def hops_of(sizes):
    length, hops = sizes[0] * sizes[1], []
    while 2 ** len(hops) < length:
        hops.append(2 ** len(hops))
    return hops


def greet(sizes, at):
    barrier = pltpu.get_barrier_semaphore()
    length = sizes[0] * sizes[1]
    seq, batch = lax.axis_index("seq"), lax.axis_index("batch")
    targets = [
        device_of(sizes, moved(sizes, at, axis, by))
        for axis in range(4)
        for by in range(1, sizes[axis])
    ]
    for hop in hops_of(sizes):
        for by in (hop, length - hop):
            targets.append({"seq": lax.rem(seq + by, length), "batch": batch})
    for target in targets:
        pl.semaphore_signal(barrier, inc=1, device_id=target, device_id_type=MESH)
    pl.semaphore_wait(barrier, len(targets))


def by_order(sizes, at, act):
    orders = orders_of(sizes)
    if len(orders) == 1:
        act(orders[0])
        return
    for parity, order in enumerate(orders):
        pl.when(at[3] == parity)(functools.partial(act, order))


def loop(count, body):
    def step(k, carry):
        body(k)
        return carry

    lax.fori_loop(0, count, step, 0)


def dot(left, right, dims, precision=None):
    return lax.dot_general(
        left, right, (dims, ((), ())), precision=precision, preferred_element_type=f32
    )


NN = ((1,), (0,))
NT = ((1,), (1,))
TN = ((0,), (0,))


class Gather:
    def __init__(self, sizes, at, shards, wholes, send_sem, recv_sem, own_sem):
        self.sizes, self.at = sizes, at
        self.shards, self.wholes = shards, wholes
        self.send_sem, self.recv_sem, self.own_sem = send_sem, recv_sem, own_sem
        self.count = len(shards)
        self.todo = []
        for tick in range(self.count + 3):
            for step in (1, 2, 3, 4):
                item = tick - step + 1
                if 0 <= item < self.count:
                    self.todo.append((item, step))

    def copies(self, item, order, step, arriving):
        axis, free = order[step], order[:step]
        made = []
        for by in range(1, self.sizes[axis]):
            source = moved(self.sizes, self.at, axis, -by) if arriving else self.at
            place = region(self.wholes[item], free, source)
            made.append(
                pltpu.make_async_remote_copy(
                    src_ref=self.shards[item] if step == 0 and not arriving else place,
                    dst_ref=place,
                    send_sem=self.send_sem.at[item, step, by - 1],
                    recv_sem=self.recv_sem.at[item, step, by - 1],
                    device_id=device_of(self.sizes, moved(self.sizes, self.at, axis, by)),
                    device_id_type=MESH,
                )
            )
        return made

    def own(self, item):
        return pltpu.make_async_copy(
            self.shards[item], region(self.wholes[item], (), self.at), self.own_sem.at[item]
        )

    def begin(self):
        for item in range(self.count):
            for copy in self.copies(item, orders_of(self.sizes)[0], 0, False):
                copy.start()
            self.own(item).start()

    def advance(self, item, step):
        if step == 1:
            self.own(item).wait()

        def act(order):
            for copy in self.copies(item, order, step - 1, True):
                copy.wait_recv()
            if step < 4:
                for copy in self.copies(item, order, step, False):
                    copy.start()

        by_order(self.sizes, self.at, act)

    def pump(self, steps):
        for _ in range(min(steps, len(self.todo))):
            self.advance(*self.todo.pop(0))

    def need(self, item):
        while (item, 4) in self.todo:
            self.pump(1)

    def finish(self):
        self.pump(len(self.todo))

        def act(order):
            for item in range(self.count):
                for step in range(4):
                    for copy in self.copies(item, order, step, False):
                        copy.wait_send()

        by_order(self.sizes, self.at, act)


class Scan:
    def __init__(self, sizes, reverse, total, state, before_total, before_state, buffers, sems):
        self.sizes, self.reverse = sizes, reverse
        self.total, self.state = total, state
        self.before_total, self.before_state = before_total, before_state
        self.total_out, self.total_in, self.state_out, self.state_in = buffers
        self.sems = sems
        self.hops = hops_of(sizes)
        self.length = sizes[0] * sizes[1]
        self.place = self.length - 1 - lax.axis_index("seq") if reverse else lax.axis_index("seq")

    def copies(self, k):
        seq = lax.axis_index("seq")
        hop = self.length - self.hops[k] if self.reverse else self.hops[k]
        target = {"seq": lax.rem(seq + hop, self.length), "batch": lax.axis_index("batch")}
        pairs = ((self.total_out, self.total_in), (self.state_out, self.state_in))
        return [
            pltpu.make_async_remote_copy(
                src_ref=out.at[k],
                dst_ref=come.at[k],
                send_sem=self.sems.at[0, k, n],
                recv_sem=self.sems.at[1, k, n],
                device_id=target,
                device_id_type=MESH,
            )
            for n, (out, come) in enumerate(pairs)
        ]

    def send(self, k):
        if k == 0:
            self.before_total[...] = jnp.ones_like(self.before_total)
            self.before_state[...] = jnp.zeros_like(self.before_state)
        self.total_out[k] = self.total[...]
        for h in range(HEADS):
            self.state_out[k, h] = self.state[h].astype(bf16)

        @pl.when(self.place + self.hops[k] < self.length)
        def _():
            for copy in self.copies(k):
                copy.start()

    def receive(self, k):
        @pl.when(self.place >= self.hops[k])
        def _():
            for copy in self.copies(k):
                copy.wait_recv()
            come = self.total_in[k]
            for h in range(HEADS):
                keys = slice(h * KEY_DIM, (h + 1) * KEY_DIM)
                state = self.state_in[k, h].astype(f32)
                self.before_state[h] = (
                    self.before_state[h] + self.before_total[0:1, keys] * state
                )
                if k + 1 < len(self.hops):
                    self.state[h] = self.state[h] + self.total[0:1, keys] * state
            self.before_total[...] = self.before_total[...] * come
            if k + 1 < len(self.hops):
                self.total[...] = self.total[...] * come

    def finish(self):
        for k in range(len(self.hops)):

            @pl.when(self.place + self.hops[k] < self.length)
            def _(k=k):
                for copy in self.copies(k):
                    copy.wait_send()


def scan_scratch(sizes):
    hops = len(hops_of(sizes))
    keys = HEADS * KEY_DIM
    return [
        pltpu.VMEM((8, keys), f32),
        pltpu.VMEM((HEADS, VALUE_DIM, KEY_DIM), f32),
        pltpu.VMEM((8, keys), f32),
        pltpu.VMEM((HEADS, VALUE_DIM, KEY_DIM), f32),
        pltpu.VMEM((hops, 8, keys), f32),
        pltpu.VMEM((hops, 8, keys), f32),
        pltpu.VMEM((hops, HEADS, VALUE_DIM, KEY_DIM), bf16),
        pltpu.VMEM((hops, HEADS, VALUE_DIM, KEY_DIM), bf16),
        pltpu.SemaphoreType.DMA((2, hops, 2)),
    ]


def lower_mask():
    rows = lax.broadcasted_iota(jnp.int32, (GROUP, GROUP), 0)
    columns = lax.broadcasted_iota(jnp.int32, (GROUP, GROUP), 1)
    return jnp.where(rows >= columns, 1.0, 0.0).astype(f32)


def log_decay_of(decay_pre):
    return jax.nn.log_sigmoid(decay_pre) * (1.0 / 16.0)


def spread(block, offset, per, width):
    devices = width // per
    lane = lax.broadcasted_iota(jnp.int32, (LANES, width), 0)
    column = lax.broadcasted_iota(jnp.int32, (LANES, width), 1)
    pick = jnp.where(lane == offset + column % per, 1.0, 0.0).astype(bf16)
    wide = dot(block.astype(bf16), pick, NN)
    rows = block.shape[0] // devices
    wide = wide.reshape(devices, rows, width)
    device = lax.broadcasted_iota(jnp.int32, wide.shape, 0)
    column = lax.broadcasted_iota(jnp.int32, wide.shape, 2)
    return jnp.sum(jnp.where(device == column // per, wide, 0.0), axis=0)


def forward_kernel(sizes, count, *refs):
    shards, tokens = refs[:count], refs[count]
    refs = refs[count + 1 :]
    far = list(refs[: count - 1])
    refs = refs[count - 1 :]
    (vectors, decay_up, normed, query, key, value, gate_pre, rank_act, decay_pre) = refs[:9]
    (starts, mixed, gated) = refs[9:12]
    refs = refs[12:]
    near = list(refs[:6])
    (query_dev, offsets) = refs[6:8]
    (total, state, before_total, before_state) = refs[8:12]
    scan_buffers, scan_sems = refs[12:16], refs[16]
    send_sem, recv_sem, own_sem, out_sem = refs[17:21]

    at = coords_of(sizes)
    devices = sizes[0] * sizes[1] * sizes[2] * sizes[3]
    width = tokens.shape[1]
    keys, values = HEADS * KEY_DIM, HEADS * VALUE_DIM
    count_rows = tokens.shape[0]
    greet(sizes, at)
    gather = Gather(sizes, at, shards, near + far[5:], send_sem, recv_sem, own_sem)
    gather.begin()

    gather.need(0)
    tiny = near[0][...].reshape(devices, RANK, LANES)
    per_feature, per_key, per_value = width // devices, keys // devices, VALUE_DIM // devices
    vectors[...] = jnp.zeros_like(vectors)
    vectors[0:1, :] = spread(tiny[:, 0], VECTORS, per_feature, width)
    vectors[1:2, :] = spread(tiny[:, 1], VECTORS, per_feature, width)
    vectors[2:3, 0:keys] = spread(tiny[:, 2], VECTORS, per_key, keys)
    vectors[3:4, 0:VALUE_DIM] = spread(tiny[:, 3], VECTORS, per_value, VALUE_DIM)
    decay_up[...] = jnp.zeros_like(decay_up)
    decay_up[0:RANK, :] = spread(tiny.reshape(devices * RANK, LANES), 0, per_key, keys).astype(bf16)

    def norm_rows(k):
        rows = pl.ds(pl.multiple_of(k * 32, 32), 32)
        hidden = tokens[rows, :].astype(f32)
        scale = lax.rsqrt(jnp.mean(hidden * hidden, axis=-1, keepdims=True) + epsilon)
        normed[rows, :] = (hidden * scale * vectors[0:1, :]).astype(bf16)

    loop(count_rows // 32, norm_rows)

    def project(item, into):
        gather.need(item)
        weight = near[item]
        size = min(into.shape[1], 256)

        def columns(k):
            here = pl.ds(pl.multiple_of(k * size, size), size)
            panel = weight[..., here].reshape(width, size)
            into[:, here] = dot(normed[...], panel, NN).astype(into.dtype)

        loop(into.shape[1] // size, columns)

    project(1, rank_act)
    decay_pre[...] = dot(rank_act[...], decay_up[...], NN) + vectors[2:3, 0:keys]
    project(2, query)
    project(3, key)
    project(4, value)

    lower = lower_mask()
    total[...] = jnp.zeros_like(total)
    state[...] = jnp.zeros_like(state)

    def group(k):
        rows = pl.ds(pl.multiple_of(k * GROUP, GROUP), GROUP)
        cumulative = dot(lower, log_decay_of(decay_pre[rows, :]), NN, highest)
        middle = cumulative[GROUP // 2 - 1 : GROUP // 2]
        ending = cumulative[GROUP - 1 :]
        query_scaled = query[rows, :].astype(f32) * key_scale
        key_full = key[rows, :].astype(f32)
        gated_query = query_scaled * jnp.exp(cumulative - middle)
        inverse_key = key_full * jnp.exp(middle - cumulative)
        tail_key = key_full * jnp.exp(ending - cumulative)
        state_query = query_scaled * jnp.exp(cumulative)
        offset = total[0:1, :]
        query_dev[rows, :] = state_query * jnp.exp(offset)
        offsets[k] = total[...]
        for h in range(HEADS):
            across = slice(h * KEY_DIM, (h + 1) * KEY_DIM)
            along = slice(h * VALUE_DIM, (h + 1) * VALUE_DIM)
            value_full = value[rows, along].astype(f32)
            scores = dot(gated_query[:, across], inverse_key[:, across], NT, high) * lower
            start = state[h]
            starts[k, h] = start.astype(bf16)
            mixed[rows, along] = dot(state_query[:, across], start, NT, high) + dot(
                scores, value_full, NN, high
            )
            state[h] = jnp.exp(ending[:, across]) * start + dot(
                value_full, tail_key[:, across], TN, high
            )
        total[...] = total[...] + ending

    loop(count_rows // GROUP, group)
    total[...] = jnp.exp(total[...])
    scan = Scan(
        sizes, False, total, state, before_total, before_state, scan_buffers, scan_sems
    )
    for k in range(len(scan.hops)):
        scan.send(k)
        if k == 0:
            project(5, gate_pre)
        else:
            gather.pump(2)
        scan.receive(k)

    def add_start(k):
        factor = jnp.exp(offsets[k])
        for h in range(HEADS):
            across = slice(h * KEY_DIM, (h + 1) * KEY_DIM)
            whole = starts[k, h].astype(f32) + factor[0:1, across] * before_state[h]
            starts[k, h] = whole.astype(bf16)

    loop(count_rows // GROUP, add_start)

    def finish_rows(k):
        rows = pl.ds(pl.multiple_of(k * GROUP, GROUP), GROUP)
        for h in range(HEADS):
            across = slice(h * KEY_DIM, (h + 1) * KEY_DIM)
            along = slice(h * VALUE_DIM, (h + 1) * VALUE_DIM)
            whole = mixed[rows, along] + dot(
                query_dev[rows, across], before_state[h], NT, high
            )
            mixed[rows, along] = whole
            scale = lax.rsqrt(jnp.mean(whole * whole, axis=-1, keepdims=True) + epsilon)
            gate = gate_pre[rows, along]
            swish = gate * jax.nn.sigmoid(gate)
            gated[rows, along] = (whole * scale * vectors[3:4, 0:VALUE_DIM] * swish).astype(bf16)

    loop(count_rows // GROUP, finish_rows)

    out = [pltpu.make_async_copy(near[k + 1], far[k], out_sem.at[k]) for k in range(5)]
    for copy in out:
        copy.start()
    gather.finish()
    scan.finish()
    for copy in out:
        copy.wait()


def forward(sizes, tokens, shards):
    count = len(shards)
    most = max(max(sizes) - 1, 1)
    rows, width = tokens.shape
    keys, values = HEADS * KEY_DIM, HEADS * VALUE_DIM
    groups = rows // GROUP
    whole = [jax.ShapeDtypeStruct(sizes + s.shape, s.dtype) for s in shards]
    shape = jax.ShapeDtypeStruct
    local_outs = [
        shape((8, width), f32),
        shape((LANES, keys), bf16),
        shape((rows, width), bf16),
        shape((rows, keys), bf16),
        shape((rows, keys), bf16),
        shape((rows, values), bf16),
        shape((rows, values), f32),
        shape((rows, LANES), bf16),
        shape((rows, keys), f32),
        shape((groups, HEADS, VALUE_DIM, KEY_DIM), bf16),
        shape((rows, values), f32),
        shape((rows, values), bf16),
    ]
    results = pl.pallas_call(
        functools.partial(forward_kernel, sizes, count),
        out_shape=whole[1:] + local_outs,
        in_specs=[pl.BlockSpec(memory_space=pltpu.VMEM)] * (count + 1),
        out_specs=[pl.BlockSpec(memory_space=pl.ANY)] * (count - 1)
        + [pl.BlockSpec(memory_space=pltpu.VMEM)] * len(local_outs),
        scratch_shapes=[pltpu.VMEM(w.shape, w.dtype) for w in whole[:6]]
        + [pltpu.VMEM((rows, keys), f32), pltpu.VMEM((groups, 8, keys), f32)]
        + scan_scratch(sizes)
        + [
            pltpu.SemaphoreType.DMA((count, 4, most)),
            pltpu.SemaphoreType.DMA((count, 4, most)),
            pltpu.SemaphoreType.DMA((count,)),
            pltpu.SemaphoreType.DMA((5,)),
        ],
        compiler_params=pltpu.CompilerParams(
            collective_id=0, has_side_effects=True, vmem_limit_bytes=VMEM_LIMIT
        ),
    )(*shards, tokens)
    weights = [w.reshape((-1,) + w.shape[5:]) for w in results[: count - 1]]
    return weights, results[count - 1 :]


class Scatter:
    def __init__(self, sizes, at, sources, stages, near, half, part, last, sums, sems):
        self.sizes, self.at = sizes, at
        self.sources, self.stages, self.near = sources, stages, near
        self.landings = (last, part, half)
        self.sums = sums
        self.send_sem, self.recv_sem, self.own_sem = sems
        self.todo = []
        self.begun = []

    def copy(self, item, order, step, by):
        axis, free = order[step], order[:step]
        target = moved(self.sizes, self.at, axis, by)
        if step == 3:
            source, landing = self.sources[item], self.near[item]
        else:
            source, landing = self.near[item], self.landings[step][item].at[by - 1]
        index = tuple(
            slice(None) if k in free else target[k] for k in range(4 if step == 3 else 3)
        )
        return pltpu.make_async_remote_copy(
            src_ref=source.at[index],
            dst_ref=landing,
            send_sem=self.send_sem.at[item, step, by - 1],
            recv_sem=self.recv_sem.at[item, step, by - 1],
            device_id=device_of(self.sizes, target),
            device_id_type=MESH,
        )

    def own(self, item, k):
        slot = k % 2
        return pltpu.make_async_copy(
            self.sources[item].at[k, :, :, self.at[3]],
            self.stages[item].at[slot],
            self.own_sem.at[item, slot],
        )

    def begin(self, items):
        for item in items:
            self.copy(item, orders_of(self.sizes)[0], 3, 1).start()
            self.begun.append(item)
        for tick in range(len(items) + 3):
            for step in (3, 2, 1, 0):
                k = tick - (3 - step)
                if 0 <= k < len(items):
                    self.todo.append((items[k], step))

    def load(self, item):
        if self.stages[item] is not None:
            for k in range(min(2, self.sizes[0])):
                self.own(item, k).start()

    def advance(self, item, step):
        def act(order):
            self.add(item, order, step)
            if step > 0:
                for by in range(1, self.sizes[order[step - 1]]):
                    self.copy(item, order, step - 1, by).start()

        by_order(self.sizes, self.at, act)

    def add(self, item, order, step):
        sizes, at = self.sizes, self.at
        axis, free = order[step], order[:step]
        near = self.near[item]
        for by in range(1, sizes[axis]):
            self.copy(item, order, step, by).wait_recv()
        if step == 0:
            total = near[at[0], at[1], at[2]].astype(f32)
            for by in range(1, sizes[axis]):
                total = total + self.landings[0][item][by - 1].astype(f32)
            self.sums[item][...] = total
            return

        staged = step == 3 and self.stages[item] is not None

        def at_outer(k):
            if staged:
                self.own(item, k).wait()
            for j in range(sizes[free[1]] if len(free) > 1 else 1):
                for i in range(sizes[free[2]] if len(free) > 2 else 1):
                    within = (k, j, i)[: len(free)]
                    place = list(at[:3])
                    for axis_of, index in zip(free, within):
                        place[axis_of] = index
                    place = tuple(place)
                    total = near[place].astype(f32)
                    if step == 3:
                        if staged:
                            mine = self.stages[item][(k % 2,) + place[1:]]
                        else:
                            mine = self.sources[item][place + (at[3],)]
                        total = total + mine.astype(f32)
                    else:
                        for by in range(1, sizes[axis]):
                            come = self.landings[step][item].at[by - 1]
                            total = total + come[within].astype(f32)
                    near[place] = total.astype(near.dtype)
            if staged:

                @pl.when(k + 2 < sizes[0])
                def _():
                    self.own(item, k + 2).start()

        loop(sizes[0], at_outer)

    def pump(self, steps):
        for _ in range(min(steps, len(self.todo))):
            self.advance(*self.todo.pop(0))

    def finish(self):
        self.pump(len(self.todo))

        def act(order):
            for item in self.begun:
                for step in range(4):
                    for by in range(1, self.sizes[order[step]]):
                        self.copy(item, order, step, by).wait_send()

        by_order(self.sizes, self.at, act)


def fold(rows, offset, per):
    count, width = rows.shape
    devices = width // per
    lane = lax.broadcasted_iota(jnp.int32, (LANES, width), 0)
    column = lax.broadcasted_iota(jnp.int32, (LANES, width), 1)
    pick = jnp.where(lane == offset + column % per, 1.0, 0.0).astype(f32)
    shape = (devices, count, width)
    device = lax.broadcasted_iota(jnp.int32, shape, 0)
    column = lax.broadcasted_iota(jnp.int32, shape, 2)
    wide = jnp.where(device == column // per, jnp.broadcast_to(rows[None], shape), 0.0)
    return dot(wide.reshape(devices * count, width), pick, NT, highest).reshape(
        devices, count, LANES
    )


FAR_ITEMS = 4
NEAR_ITEMS = 6


def backward_kernel(sizes, *refs):
    count = FAR_ITEMS + NEAR_ITEMS
    far_grads, far_weights, far_arrays = refs[:4], refs[4:9], refs[9:13]
    (query, key, value, decay_pre, starts, normed, rank_act, decay_up, vectors, side, tokens) = refs[
        13:24
    ]
    refs = refs[24:]
    sums, input_grad = refs[:count], refs[count]
    refs = refs[count + 1 :]
    local, stages = list(refs[:NEAR_ITEMS]), list(refs[NEAR_ITEMS : NEAR_ITEMS + 3])
    refs = refs[NEAR_ITEMS + 3 :]
    near, half, part, last = (refs[k * count : (k + 1) * count] for k in range(4))
    refs = refs[4 * count :]
    weights = refs[:5]
    (wide_a, wide_b, wide_c, outgate_grad) = refs[5:9]
    (cumulative_all, query_dev, query_grad, key_grad, value_grad, decay_grad) = refs[9:15]
    (rank_grad, rows_sum) = refs[15:17]
    (total, state, before_total, before_state) = refs[17:21]
    scan_buffers, scan_sems = refs[21:25], refs[25]
    send_sem, recv_sem, own_sem, load_sem = refs[26:30]

    at = coords_of(sizes)
    devices = sizes[0] * sizes[1] * sizes[2] * sizes[3]
    count_rows, width = tokens.shape
    keys, values = HEADS * KEY_DIM, HEADS * VALUE_DIM
    groups = count_rows // GROUP

    loads = [
        pltpu.make_async_copy(source, target, load_sem.at[k])
        for k, (source, target) in enumerate(
            zip(far_arrays[:3] + far_weights, (wide_a, wide_b, wide_c) + tuple(weights))
        )
    ]
    for copy in loads:
        copy.start()
    greet(sizes, at)
    scatter = Scatter(
        sizes,
        at,
        list(far_grads) + local,
        [stages[0], stages[1], stages[1], stages[2]] + [None] * NEAR_ITEMS,
        near,
        half,
        part,
        last,
        sums,
        (send_sem, recv_sem, own_sem),
    )
    for item in (0, 1, 3):
        scatter.load(item)
    scatter.begin([0, 1, 2, 3])
    for copy in loads[:3]:
        copy.wait()
    gated_grad, mixed, gate_pre = wide_a, wide_b, wide_c
    mixed_grad = mixed

    rows_sum[...] = jnp.zeros_like(rows_sum)

    def gate_rows(k):
        rows = pl.ds(pl.multiple_of(k * GROUP, GROUP), GROUP)
        for h in range(HEADS):
            along = slice(h * VALUE_DIM, (h + 1) * VALUE_DIM)
            whole, gate, grad = mixed[rows, along], gate_pre[rows, along], gated_grad[rows, along]
            scale = lax.rsqrt(jnp.mean(whole * whole, axis=-1, keepdims=True) + epsilon)
            sig = jax.nn.sigmoid(gate)
            plain = whole * scale
            gain = vectors[3:4, 0:VALUE_DIM]
            through = grad * (gate * sig)
            rows_sum[3:4, 0:VALUE_DIM] = rows_sum[3:4, 0:VALUE_DIM] + jnp.sum(
                through * plain, axis=0, keepdims=True
            )
            back = through * gain
            mixed_grad[rows, along] = scale * (
                back - plain * jnp.mean(back * plain, axis=-1, keepdims=True)
            )
            outgate_grad[rows, along] = (
                grad * plain * gain * sig * (1.0 + gate * (1.0 - sig))
            ).astype(bf16)

    loop(groups, gate_rows)

    lower = lower_mask()
    total[...] = jnp.zeros_like(total)
    state[...] = jnp.zeros_like(state)

    def state_rows(k):
        rows = pl.ds(pl.multiple_of(k * GROUP, GROUP), GROUP)
        cumulative = dot(lower, log_decay_of(decay_pre[rows, :]), NN, highest)
        cumulative_all[rows, :] = cumulative
        query_scaled = query[rows, :].astype(f32) * key_scale
        query_dev[rows, :] = (query_scaled * jnp.exp(cumulative + total[0:1, :])).astype(bf16)
        total[...] = total[...] + cumulative[GROUP - 1 :]

    loop(groups, state_rows)
    for h in range(HEADS):
        across = slice(h * KEY_DIM, (h + 1) * KEY_DIM)
        along = slice(h * VALUE_DIM, (h + 1) * VALUE_DIM)
        state[h] = dot(mixed_grad[:, along].astype(bf16), query_dev[:, across], TN)
    total[...] = jnp.exp(total[...])
    scan = Scan(
        sizes, True, total, state, before_total, before_state, scan_buffers, scan_sems
    )

    def weight_grad(target, right):
        block = width // sizes[0]
        size = min(right.shape[1], 256)

        def features(a):
            left = normed[:, pl.ds(pl.multiple_of(a * block, block), block)]

            def columns(k):
                here = pl.ds(pl.multiple_of(k * size, size), size)
                made = dot(left, right[:, here], TN)
                shaped = made.reshape(target.shape[1:5] + (size,))
                target[a, :, :, :, :, here] = shaped.astype(bf16)

            loop(right.shape[1] // size, columns)

        loop(sizes[0], features)

    for k in range(len(scan.hops)):
        scan.send(k)
        if k == 0:
            scatter.pump(1)
            weight_grad(local[3], outgate_grad)
        else:
            scatter.pump(2)
        if k == 1:
            scatter.load(2)
        scan.receive(k)

    def group(k):
        g = groups - 1 - k
        rows = pl.ds(pl.multiple_of(g * GROUP, GROUP), GROUP)
        cumulative = cumulative_all[rows, :]
        middle = cumulative[GROUP // 2 - 1 : GROUP // 2]
        ending = cumulative[GROUP - 1 :]
        query_scaled = query[rows, :].astype(f32) * key_scale
        key_full = key[rows, :].astype(f32)
        from_middle, to_middle = jnp.exp(cumulative - middle), jnp.exp(middle - cumulative)
        to_end, from_start = jnp.exp(ending - cumulative), jnp.exp(cumulative)
        decay_end = jnp.exp(ending)
        gated_query = (query_scaled * from_middle).astype(bf16)
        inverse_key = (key_full * to_middle).astype(bf16)
        tail_key = (key_full * to_end).astype(bf16)
        state_query = (query_scaled * from_start).astype(bf16)
        grad_cumul, through_end = [], []
        for h in range(HEADS):
            across = slice(h * KEY_DIM, (h + 1) * KEY_DIM)
            along = slice(h * VALUE_DIM, (h + 1) * VALUE_DIM)
            start_b, after = starts[g, h], before_state[h]
            start, after_b = start_b.astype(f32), after.astype(bf16)
            grad_out = mixed_grad[rows, along].astype(bf16)
            value_b = value[rows, along]
            scores = (dot(gated_query[:, across], inverse_key[:, across], NT) * lower).astype(bf16)
            grad_scores = (dot(grad_out, value_b, NT) * lower).astype(bf16)
            to_query = from_start[:, across] * dot(grad_out, start_b, NN)
            to_query = to_query + from_middle[:, across] * dot(
                grad_scores, inverse_key[:, across], NN
            )
            to_key = to_middle[:, across] * dot(grad_scores, gated_query[:, across], TN)
            to_key = to_key + to_end[:, across] * dot(value_b, after_b, NN)
            to_value = dot(scores, grad_out, TN) + dot(tail_key[:, across], after_b, NT)
            end_state = decay_end[:, across] * start + dot(value_b, tail_key[:, across], TN)
            through_end.append(jnp.sum(end_state * after, axis=0, keepdims=True))
            grad_cumul.append(query_scaled[:, across] * to_query - key_full[:, across] * to_key)
            before_state[h] = decay_end[:, across] * after + dot(
                grad_out, state_query[:, across], TN
            )
            query_grad[rows, across] = (to_query * key_scale).astype(bf16)
            key_grad[rows, across] = to_key.astype(bf16)
            value_grad[rows, along] = to_value.astype(bf16)
        log_grad = dot(lower, jnp.concatenate(grad_cumul, axis=1), TN, highest)
        log_grad = log_grad + jnp.concatenate(through_end, axis=1)
        to_decay = log_grad * jax.nn.sigmoid(-decay_pre[rows, :]) * (1.0 / 16.0)
        rows_sum[2:3, 0:keys] = rows_sum[2:3, 0:keys] + jnp.sum(to_decay, axis=0, keepdims=True)
        decay_grad[rows, :] = to_decay.astype(bf16)
        for turn in range(groups):
            pl.when(k == turn)(lambda: scatter.pump(2))

    loop(groups, group)

    weight_grad(local[0], query_grad)
    weight_grad(local[1], key_grad)
    weight_grad(local[2], value_grad)
    rank_grad[...] = dot(decay_grad[...], decay_up[...], NT).astype(bf16)
    weight_grad(local[4], rank_grad)
    scatter.begin([7, 4, 5, 6, 8])
    decay_up_grad = dot(rank_act[...], decay_grad[...], TN)[0:RANK]

    for copy in loads[3:]:
        copy.wait()
    middle_load = pltpu.make_async_copy(far_arrays[3], wide_c, load_sem.at[8])
    middle_load.start()
    gradients = (rank_grad, query_grad, key_grad, value_grad, outgate_grad)

    def features(k):
        here = pl.ds(pl.multiple_of(k * 256, 256), 256)
        made = dot(gradients[0][...], weights[0][here, :], NT)
        for grad, weight in zip(gradients[1:], weights[1:]):
            made = made + dot(grad[...], weight[here, :], NT)
        wide_a[:, here] = made

    loop(width // 256, features)
    middle_load.wait()

    def input_rows(k):
        rows = pl.ds(pl.multiple_of(k * 32, 32), 32)
        hidden = tokens[rows, :].astype(f32)
        scale = lax.rsqrt(jnp.mean(hidden * hidden, axis=-1, keepdims=True) + epsilon)
        plain = hidden * scale
        grad = wide_a[rows, :]
        rows_sum[0:1, :] = rows_sum[0:1, :] + jnp.sum(grad * plain, axis=0, keepdims=True)
        grad = grad * vectors[0:1, :]
        input_grad[rows, :] = wide_c[rows, :] + scale * (
            grad - plain * jnp.mean(grad * plain, axis=-1, keepdims=True)
        )

    loop(count_rows // 32, input_rows)

    per_feature, per_key, per_value = width // devices, keys // devices, VALUE_DIM // devices
    tiny = fold(decay_up_grad, 0, per_key)
    row_of = lax.broadcasted_iota(jnp.int32, tiny.shape, 1)
    for k, vector in enumerate(
        (
            fold(rows_sum[0:1, :], VECTORS, per_feature),
            fold(side[0:1, :], VECTORS, per_feature),
            fold(rows_sum[2:3, 0:keys], VECTORS, per_key),
            fold(rows_sum[3:4, 0:VALUE_DIM], VECTORS, per_value),
        )
    ):
        tiny = tiny + jnp.where(row_of == k, jnp.broadcast_to(vector, tiny.shape), 0.0)
    local[5][...] = tiny.reshape(local[5].shape)
    scatter.begin([9])
    scatter.finish()
    scan.finish()


def backward(sizes, far_grads, weights, arrays, local_arrays):
    outer, inner, side, core = sizes
    devices = outer * inner * side * core
    shape = jax.ShapeDtypeStruct
    most = max(max(sizes) - 1, 1)
    rows, width = local_arrays[-1].shape
    keys, values = HEADS * KEY_DIM, HEADS * VALUE_DIM
    far = [g.reshape(sizes + (g.shape[0] // devices, g.shape[1])) for g in far_grads]
    mine = width // devices
    made = [((mine, n), bf16) for n in (keys, keys, values, values, LANES)] + [((RANK, LANES), f32)]
    blocks = [(g.shape[4:], g.dtype) for g in far] + made

    def buffers(lead, of):
        return [pltpu.VMEM(lead + block, dtype) for block, dtype in of]

    outs = [shape(block, f32) for block, _ in blocks] + [shape((rows, width), f32)]
    vmem = pl.BlockSpec(memory_space=pltpu.VMEM)
    anywhere = pl.BlockSpec(memory_space=pl.ANY)
    results = pl.pallas_call(
        functools.partial(backward_kernel, sizes),
        out_shape=outs,
        in_specs=[anywhere] * (len(far) + len(weights) + len(arrays)) + [vmem] * len(local_arrays),
        out_specs=[vmem] * len(outs),
        scratch_shapes=buffers(sizes, made)
        + buffers((2, inner, side), [blocks[0], blocks[1], blocks[3]])
        + buffers((outer, inner, side), blocks)
        + buffers((max(side - 1, 1), outer, inner), blocks)
        + buffers((max(inner - 1, 1), outer), blocks)
        + buffers((max(outer - 1, 1),), blocks)
        + [pltpu.VMEM(w.shape, w.dtype) for w in weights]
        + [
            pltpu.VMEM((rows, values), f32),
            pltpu.VMEM((rows, values), f32),
            pltpu.VMEM((rows, values), f32),
            pltpu.VMEM((rows, values), bf16),
            pltpu.VMEM((rows, keys), f32),
            pltpu.VMEM((rows, keys), bf16),
            pltpu.VMEM((rows, keys), bf16),
            pltpu.VMEM((rows, keys), bf16),
            pltpu.VMEM((rows, values), bf16),
            pltpu.VMEM((rows, keys), bf16),
            pltpu.VMEM((rows, LANES), bf16),
            pltpu.VMEM((8, width), f32),
        ]
        + scan_scratch(sizes)
        + [
            pltpu.SemaphoreType.DMA((len(blocks), 4, most)),
            pltpu.SemaphoreType.DMA((len(blocks), 4, most)),
            pltpu.SemaphoreType.DMA((len(blocks), 2)),
            pltpu.SemaphoreType.DMA((9,)),
        ],
        compiler_params=pltpu.CompilerParams(
            collective_id=1, has_side_effects=True, vmem_limit_bytes=VMEM_LIMIT
        ),
    )(*far, *weights, *arrays, *local_arrays)
    return results[:-1], results[-1]


def matmul(left, right):
    return jnp.dot(left, right, preferred_element_type=f32)


def contract_rows(left, right):
    return dot(left, right, TN)


def times_transpose(left, right):
    return dot(left, right, NT)


def tiny_pack(decay_up, vectors):
    rows = [jnp.pad(decay_up.astype(f32), ((0, 0), (0, VECTORS - decay_up.shape[1])))]
    stacked = jnp.stack(
        [jnp.pad(v.astype(f32), (0, LANES - VECTORS - v.shape[0])) for v in vectors]
    )
    rows.append(jnp.pad(stacked, ((0, RANK - len(vectors)), (0, 0))))
    return jnp.concatenate(rows, axis=1)


def local(
    sizes,
    inputs,
    cotangent,
    mixer_gain,
    feed_gain,
    w_query,
    w_key,
    w_value,
    w_outgate,
    w_decay_down,
    w_decay_up,
    decay_bias,
    head_gain,
    w_output,
    w_gate,
    w_up,
    w_down,
):
    width = inputs.shape[2]
    rows = inputs.shape[0] * inputs.shape[1]
    per_feature, per_key, per_value = (
        mixer_gain.shape[0],
        decay_bias.shape[0],
        head_gain.shape[0],
    )
    tokens = inputs.reshape(rows, width)
    tiny = tiny_pack(w_decay_up, (mixer_gain, feed_gain, decay_bias, head_gain))
    down_padded = jnp.pad(w_decay_down, ((0, 0), (0, LANES - RANK)))
    shards = (
        tiny, down_padded, w_query, w_key, w_value, w_outgate, w_output, w_gate, w_up, w_down,
    )
    weights, arrays = forward(sizes, tokens, shards)
    weights = [w.reshape(-1, w.shape[-1]) for w in weights]
    proj_output, feed_gate, feed_up, feed_down = weights[5:]
    (vectors, decay_up, normed, query, key, value, gate_pre, rank_act, decay_pre) = arrays[:9]
    (starts, mixed, gated) = arrays[9:]
    gain_two = vectors[1:2]
    hidden_in = tokens.astype(f32)
    middle = hidden_in + matmul(gated, proj_output)
    feed_scale = lax.rsqrt(jnp.mean(middle * middle, axis=-1, keepdims=True) + epsilon)
    normed_two = (middle * feed_scale * gain_two).astype(bf16)
    up_gate = matmul(normed_two, feed_gate)
    up_lin = matmul(normed_two, feed_up)
    up_sig = jax.nn.sigmoid(up_gate)
    activated = (up_gate * up_sig * up_lin).astype(bf16)
    result = middle + matmul(activated, feed_down)
    grad_rows = cotangent.reshape(rows, width)
    grad_b = grad_rows.astype(bf16)
    grad_down = contract_rows(activated, grad_b).astype(bf16)
    act_grad = times_transpose(grad_b, feed_down)
    gate_grad = (act_grad * up_lin * up_sig * (1.0 + up_gate * (1.0 - up_sig))).astype(bf16)
    lin_grad = (act_grad * up_gate * up_sig).astype(bf16)
    grad_gate = contract_rows(normed_two, gate_grad).astype(bf16)
    grad_up = contract_rows(normed_two, lin_grad).astype(bf16)
    normed_two_grad = times_transpose(gate_grad, feed_gate) + times_transpose(lin_grad, feed_up)
    grad_feed_gain = jnp.sum(normed_two_grad * middle * feed_scale, axis=0)
    scaled_two = normed_two_grad * gain_two
    middle_grad = (
        grad_rows
        + feed_scale * scaled_two
        - middle * feed_scale**3 * jnp.mean(scaled_two * middle, axis=-1, keepdims=True)
    )
    middle_b = middle_grad.astype(bf16)
    grad_output = contract_rows(gated, middle_b).astype(bf16)
    gated_grad = times_transpose(middle_b, proj_output)
    side = jnp.broadcast_to(grad_feed_gain[None], (8, width))
    sums, input_grad = backward(
        sizes,
        (grad_down, grad_gate, grad_up, grad_output),
        weights[:5],
        (gated_grad, mixed, gate_pre, middle_grad),
        (query, key, value, decay_pre, starts, normed, rank_act, decay_up, vectors, side, tokens),
    )
    (down, gate, up, output, g_query, g_key, g_value, g_outgate, decay_down, small) = sums
    return (
        result.reshape(inputs.shape),
        input_grad.reshape(inputs.shape),
        small[0, VECTORS : VECTORS + per_feature],
        small[1, VECTORS : VECTORS + per_feature],
        g_query,
        g_key,
        g_value,
        g_outgate,
        decay_down[:, :RANK],
        small[:, :per_key],
        small[2, VECTORS : VECTORS + per_key],
        small[3, VECTORS : VECTORS + per_value],
        output,
        gate,
        up,
        down,
    )


def solution(mesh):
    placed = (
        P("batch", "seq", None),
        P("batch", "seq", None),
        P(("seq", "batch")),
        P(("seq", "batch")),
        P(("seq", "batch"), None),
        P(("seq", "batch"), None),
        P(("seq", "batch"), None),
        P(("seq", "batch"), None),
        P(("seq", "batch"), None),
        P(None, ("seq", "batch")),
        P(("seq", "batch")),
        P(("seq", "batch")),
        P(("seq", "batch"), None),
        P(("seq", "batch"), None),
        P(("seq", "batch"), None),
        P(("seq", "batch"), None),
    )
    return jax.shard_map(
        functools.partial(local, grid_of(mesh.shape)),
        mesh=mesh,
        in_specs=placed,
        out_specs=(
            P("batch", "seq", None),
            P("batch", "seq", None),
            P(("seq", "batch")),
            P(("seq", "batch")),
            P(("seq", "batch"), None),
            P(("seq", "batch"), None),
            P(("seq", "batch"), None),
            P(("seq", "batch"), None),
            P(("seq", "batch"), None),
            P(None, ("seq", "batch")),
            P(("seq", "batch")),
            P(("seq", "batch")),
            P(("seq", "batch"), None),
            P(("seq", "batch"), None),
            P(("seq", "batch"), None),
            P(("seq", "batch"), None),
        ),
        check_vma=False,
    )
```

```python
import functools
from types import SimpleNamespace

import jax
import jax.numpy as jnp
from jax import lax
from jax.experimental import pallas as pl
from jax.experimental.pallas import tpu as pltpu
from jax.sharding import PartitionSpec as P

HEADS = 4
KEY_DIM = 128
VALUE_DIM = 256
GROUP = 64
LANES = 128
RANK = 16
VECTORS = 32
MESH = pl.DeviceIdType.MESH
VMEM_LIMIT = 63 * 2**20


class Names:
    def __getattr__(self, name):
        return name


N = Names()
epsilon = 1e-06
key_scale = KEY_DIM ** (-0.5)
highest = lax.Precision.HIGHEST
high = lax.Precision.HIGH
f32 = jnp.float32
bf16 = jnp.bfloat16


def grid_of(shape):
    seq, batch = shape["seq"], shape["batch"]
    outer = 4 if seq % 4 == 0 else seq
    core = 2 if batch % 2 == 0 else 1
    return (outer, seq // outer, batch // core, core)


def coords_of(sizes):
    seq, batch = lax.axis_index("seq"), lax.axis_index("batch")
    return (seq // sizes[1], seq % sizes[1], batch // sizes[3], batch % sizes[3])


def device_of(sizes, at):
    return {"seq": at[0] * sizes[1] + at[1], "batch": at[2] * sizes[3] + at[3]}


def moved(sizes, at, axis, by):
    new = list(at)
    new[axis] = lax.rem(at[axis] + (by % sizes[axis]), sizes[axis])
    return tuple(new)


def region(ref, free, at):
    return ref.at[tuple(slice(None) if k in free else at[k] for k in range(4))]


def orders_of(sizes, late=False):
    orders = ((1, 2, 0, 3), (2, 1, 0, 3)) if late else ((0, 1, 2, 3), (0, 2, 1, 3))
    return orders if sizes[1] == sizes[2] and sizes[3] == 2 else orders[:1]


def hops_of(sizes):
    length, hops = sizes[0] * sizes[1], []
    while 2 ** len(hops) < length:
        hops.append(2 ** len(hops))
    return hops


def greet(sizes, at):
    barrier = pltpu.get_barrier_semaphore()
    length = sizes[0] * sizes[1]
    seq, batch = lax.axis_index("seq"), lax.axis_index("batch")
    targets = [
        device_of(sizes, moved(sizes, at, axis, by))
        for axis in range(4)
        for by in range(1, sizes[axis])
    ]
    for hop in hops_of(sizes):
        for by in (hop, length - hop):
            targets.append({"seq": lax.rem(seq + by, length), "batch": batch})
    for target in targets:
        pl.semaphore_signal(barrier, inc=1, device_id=target, device_id_type=MESH)
    pl.semaphore_wait(barrier, len(targets))


def by_order(sizes, at, act, late=False):
    orders = orders_of(sizes, late)
    if len(orders) == 1:
        act(orders[0])
        return
    for parity, order in enumerate(orders):
        pl.when(at[3] == parity)(functools.partial(act, order))


def loop(count, body):
    def step(k, carry):
        body(k)
        return carry

    lax.fori_loop(0, count, step, 0)


def dot(left, right, dims, precision=None):
    return lax.dot_general(
        left, right, (dims, ((), ())), precision=precision, preferred_element_type=f32
    )


NN = ((1,), (0,))
NT = ((1,), (1,))
TN = ((0,), (0,))


class Item:
    def __init__(self, ref, start=0, size=None):
        self.ref, self.start = ref, start
        self.size = ref.shape[-1] if size is None else size
        self.part = self.size != ref.shape[-1]

    def tail(self):
        return (slice(None), slice(self.start, self.start + self.size)) if self.part else ()

    def at(self, index):
        return self.ref.at[tuple(index) + self.tail()]


def blocks_of(free, at, axes=4):
    return tuple(slice(None) if k in free else at[k] for k in range(axes))


class Gather:
    def __init__(self, sizes, at, shards, wholes, sems, late):
        self.sizes, self.at, self.late = sizes, at, late
        self.shards, self.wholes = shards, wholes
        self.send_sem, self.recv_sem, self.own_sem = sems
        self.done = {item: 0 for item in range(len(shards))}

    def copies(self, item, order, step, arriving):
        axis, free = order[step], order[:step]
        made = []
        for by in range(1, self.sizes[axis]):
            source = moved(self.sizes, self.at, axis, -by) if arriving else self.at
            place = self.wholes[item].at(blocks_of(free, source))
            made.append(
                pltpu.make_async_remote_copy(
                    src_ref=self.shards[item].at(()) if step == 0 and not arriving else place,
                    dst_ref=place,
                    send_sem=self.send_sem.at[item, step, by - 1],
                    recv_sem=self.recv_sem.at[item, step, by - 1],
                    device_id=device_of(self.sizes, moved(self.sizes, self.at, axis, by)),
                    device_id_type=MESH,
                )
            )
        return made

    def own(self, item):
        return pltpu.make_async_copy(
            self.shards[item].at(()),
            self.wholes[item].at(blocks_of((), self.at)),
            self.own_sem.at[item],
        )

    def begin(self, items):
        for item in items:

            def act(order, item=item):
                for copy in self.copies(item, order, 0, False):
                    copy.start()

            if item in self.late:
                by_order(self.sizes, self.at, act, True)
            else:
                act(orders_of(self.sizes)[0])
            self.own(item).start()

    def advance(self, item, step):
        while self.done[item] < step:
            now = self.done[item] = self.done[item] + 1
            if now == 1:
                self.own(item).wait()

            def act(order, now=now):
                for copy in self.copies(item, order, now - 1, True):
                    copy.wait_recv()
                if now < 4:
                    for copy in self.copies(item, order, now, False):
                        copy.start()

            by_order(self.sizes, self.at, act, item in self.late)

    def finish(self):
        for item in self.done:
            self.advance(item, 4)
        for late in (False, True):

            def act(order, late=late):
                for item in self.done:
                    if (item in self.late) == late:
                        for step in range(4):
                            for copy in self.copies(item, order, step, False):
                                copy.wait_send()

            by_order(self.sizes, self.at, act, late)


class Scatter:
    def __init__(self, sizes, at, sources, stages, near, half, part, last, sums, sems, late):
        self.sizes, self.at, self.late = sizes, at, late
        self.sources, self.stages, self.near = sources, stages, near
        self.landings = (last, part, half)
        self.sums = sums
        self.send_sem, self.recv_sem, self.own_sem = sems
        self.left = {}
        self.released = set()

    def copy(self, item, order, step, by):
        axis, free = order[step], order[:step]
        target = moved(self.sizes, self.at, axis, by)
        if step == 3:
            source = self.sources[item].at(blocks_of(free, target))
            landing = self.near[item]
        else:
            source = self.near[item].at[blocks_of(free, target, 3)]
            landing = self.landings[step][item].at[by - 1]
        return pltpu.make_async_remote_copy(
            src_ref=source,
            dst_ref=landing,
            send_sem=self.send_sem.at[item, step, by - 1],
            recv_sem=self.recv_sem.at[item, step, by - 1],
            device_id=device_of(self.sizes, target),
            device_id_type=MESH,
        )

    def own(self, item, k):
        slot = k % 2
        return pltpu.make_async_copy(
            self.sources[item].at((k, slice(None), slice(None), self.at[3])),
            self.stages[item].at[slot],
            self.own_sem.at[item, slot],
        )

    def begin(self, item):
        self.left[item] = 4
        self.copy(item, orders_of(self.sizes)[0], 3, 1).start()
        if item in self.stages:
            for k in range(min(2, self.sizes[0])):
                self.own(item, k).start()

    def advance(self, item, step):
        while self.left[item] > step:
            now = self.left[item] = self.left[item] - 1

            def act(order, now=now):
                self.add(item, order, now)
                if now > 0:
                    for by in range(1, self.sizes[order[now - 1]]):
                        self.copy(item, order, now - 1, by).start()

            by_order(self.sizes, self.at, act, item in self.late)

    def add(self, item, order, step):
        sizes, at = self.sizes, self.at
        axis, free = order[step], sorted(order[:step])
        near = self.near[item]
        for by in range(1, sizes[axis]):
            self.copy(item, order, step, by).wait_recv()
        if step == 0:
            total = near[at[0], at[1], at[2]].astype(f32)
            for by in range(1, sizes[axis]):
                total = total + self.landings[0][item][by - 1].astype(f32)
            kept = self.sums[item]
            kept.ref[:, kept.start : kept.start + kept.size] = total
            return
        staged = step == 3 and item in self.stages

        def at_outer(k):
            if staged:
                self.own(item, k).wait()
            for j in range(sizes[free[1]] if len(free) > 1 else 1):
                for i in range(sizes[free[2]] if len(free) > 2 else 1):
                    within = (k, j, i)[: len(free)]
                    place = list(at[:3])
                    for axis_of, index in zip(free, within):
                        place[axis_of] = index
                    place = tuple(place)
                    total = near[place].astype(f32)
                    if staged:
                        total = total + self.stages[item][(k % 2,) + place[1:]].astype(f32)
                    elif step == 3:
                        source = self.sources[item]
                        mine = source.ref[place + (at[3],) + source.tail()]
                        total = total + mine.astype(f32)
                    else:
                        for by in range(1, sizes[axis]):
                            come = self.landings[step][item].at[by - 1]
                            total = total + come[within].astype(f32)
                    near[place] = total.astype(near.dtype)
            if staged:

                @pl.when(k + 2 < sizes[0])
                def _():
                    self.own(item, k + 2).start()

        loop(sizes[free[0]], at_outer)

    def release(self, item):
        self.advance(item, 3)
        self.released.add(item)
        self.copy(item, orders_of(self.sizes)[0], 3, 1).wait_send()

    def finish(self):
        for item in self.left:
            self.advance(item, 0)
        for late in (False, True):

            def act(order, late=late):
                for item in self.left:
                    if (item in self.late) == late:
                        for step in range(3 if item in self.released else 4):
                            for by in range(1, self.sizes[order[step]]):
                                self.copy(item, order, step, by).wait_send()

            by_order(self.sizes, self.at, act, late)


class Scan:
    def __init__(self, sizes, reverse, total, state, before_total, before_state, buffers, sems):
        self.sizes, self.reverse = sizes, reverse
        self.total, self.state = total, state
        self.before_total, self.before_state = before_total, before_state
        self.total_out, self.total_in, self.state_out, self.state_in = buffers
        self.sems = sems
        self.hops = hops_of(sizes)
        self.length = sizes[0] * sizes[1]
        self.place = self.length - 1 - lax.axis_index("seq") if reverse else lax.axis_index("seq")

    def copies(self, k):
        seq = lax.axis_index("seq")
        hop = self.length - self.hops[k] if self.reverse else self.hops[k]
        target = {"seq": lax.rem(seq + hop, self.length), "batch": lax.axis_index("batch")}
        pairs = ((self.total_out, self.total_in), (self.state_out, self.state_in))
        return [
            pltpu.make_async_remote_copy(
                src_ref=out.at[k],
                dst_ref=come.at[k],
                send_sem=self.sems.at[0, k, n],
                recv_sem=self.sems.at[1, k, n],
                device_id=target,
                device_id_type=MESH,
            )
            for n, (out, come) in enumerate(pairs)
        ]

    def send(self, k):
        if k == 0:
            self.before_total[...] = jnp.ones_like(self.before_total)
            self.before_state[...] = jnp.zeros_like(self.before_state)
        self.total_out[k] = self.total[...]
        for h in range(HEADS):
            self.state_out[k, h] = self.state[h].astype(bf16)

        @pl.when(self.place + self.hops[k] < self.length)
        def _():
            for copy in self.copies(k):
                copy.start()

    def receive(self, k):
        @pl.when(self.place >= self.hops[k])
        def _():
            for copy in self.copies(k):
                copy.wait_recv()
            come = self.total_in[k]
            for h in range(HEADS):
                keys = slice(h * KEY_DIM, (h + 1) * KEY_DIM)
                state = self.state_in[k, h].astype(f32)
                self.before_state[h] = (
                    self.before_state[h] + self.before_total[0:1, keys] * state
                )
                if k + 1 < len(self.hops):
                    self.state[h] = self.state[h] + self.total[0:1, keys] * state
            self.before_total[...] = self.before_total[...] * come
            if k + 1 < len(self.hops):
                self.total[...] = self.total[...] * come

    def finish(self):
        for k in range(len(self.hops)):

            @pl.when(self.place + self.hops[k] < self.length)
            def _(k=k):
                for copy in self.copies(k):
                    copy.wait_send()


def lower_mask():
    rows = lax.broadcasted_iota(jnp.int32, (GROUP, GROUP), 0)
    columns = lax.broadcasted_iota(jnp.int32, (GROUP, GROUP), 1)
    return jnp.where(rows >= columns, 1.0, 0.0).astype(f32)


def log_decay_of(decay_pre):
    return jax.nn.log_sigmoid(decay_pre) * (1.0 / 16.0)


def spread(block, offset, per, width):
    devices = width // per
    lane = lax.broadcasted_iota(jnp.int32, (LANES, width), 0)
    column = lax.broadcasted_iota(jnp.int32, (LANES, width), 1)
    pick = jnp.where(lane == offset + column % per, 1.0, 0.0).astype(bf16)
    wide = dot(block.astype(bf16), pick, NN)
    rows = block.shape[0] // devices
    wide = wide.reshape(devices, rows, width)
    device = lax.broadcasted_iota(jnp.int32, wide.shape, 0)
    column = lax.broadcasted_iota(jnp.int32, wide.shape, 2)
    return jnp.sum(jnp.where(device == column // per, wide, 0.0), axis=0)


def scan_scratch(sizes):
    hops = len(hops_of(sizes))
    keys = HEADS * KEY_DIM
    return dict(
        total=pltpu.VMEM((8, keys), f32),
        state=pltpu.VMEM((HEADS, VALUE_DIM, KEY_DIM), f32),
        before_total=pltpu.VMEM((8, keys), f32),
        before_state=pltpu.VMEM((HEADS, VALUE_DIM, KEY_DIM), f32),
        total_out=pltpu.VMEM((hops, 8, keys), f32),
        total_in=pltpu.VMEM((hops, 8, keys), f32),
        state_out=pltpu.VMEM((hops, HEADS, VALUE_DIM, KEY_DIM), bf16),
        state_in=pltpu.VMEM((hops, HEADS, VALUE_DIM, KEY_DIM), bf16),
        scan_sem=pltpu.SemaphoreType.DMA((2, hops, 2)),
    )


def scan_of(sizes, reverse, r):
    return Scan(
        sizes,
        reverse,
        r.total,
        r.state,
        r.before_total,
        r.before_state,
        (r.total_out, r.total_in, r.state_out, r.state_in),
        r.scan_sem,
    )


def head_slices(h):
    return slice(h * KEY_DIM, (h + 1) * KEY_DIM), slice(h * VALUE_DIM, (h + 1) * VALUE_DIM)


def tile(k, size):
    return pl.ds(pl.multiple_of(k * size, size), size)


def halves(columns):
    first = -(-columns // 512) * 256
    return ((0, first), (first, columns - first))


WEIGHTS = (N.decay_down, N.query, N.key, N.value, N.outgate, N.output, N.gate, N.up, N.down)
KEPT = WEIGHTS[:5]
LATE_GATHERED = ()
FORWARD_PLAN = (
    1001, 1011, 1002, 1021, 1012, 1003, 1031, 1013, 1022, 1004, 0, 1032, 1014, 1, 1041, 2,
    1023, 1024, 3, 1051, 1033, 1042, 1034, 4, 1061, 1052, 1062, 1071, 1043, 1044, 5, 6,
    1081, 1053, 1072, 100, 1091, 1063, 1054, 7, 1064, 1101, 1082, 200, 101, 1111, 1073, 1092,
    1121, 1074, 201, 102, 1102, 1083, 1112, 202, 300, 8, 9, 1084, 1122, 1093, 10, 1094,
    1103, 1104, 11, 1113, 12, 1114, 13, 1123, 15, 1124, 14, 17, 18, 16,
)


def forward_kernel(sizes, names, *refs):
    r = SimpleNamespace(**dict(zip(names, refs)))
    at = coords_of(sizes)
    devices = sizes[0] * sizes[1] * sizes[2] * sizes[3]
    count_rows, width = r.tokens.shape
    keys, values = HEADS * KEY_DIM, HEADS * VALUE_DIM
    hidden = r.up_gate.shape[1]
    groups = count_rows // GROUP
    vectors = r.vectors
    per_feature, per_key, per_value = width // devices, keys // devices, VALUE_DIM // devices

    tiny = r.tiny_mine
    tiny[...] = jnp.zeros_like(tiny)
    tiny[:, 0:per_key] = r.w_decay_up[...].astype(f32)
    for k, name in enumerate((N.mixer_gain, N.feed_gain, N.decay_bias, N.head_gain)):
        vector = getattr(r, name)
        tiny[k : k + 1, VECTORS : VECTORS + vector.shape[1]] = vector[...].astype(f32)
    down_mine = r.down_mine
    down_mine[...] = jnp.zeros_like(down_mine)
    down_mine[:, 0:RANK] = turned(r.w_decay_down[...]).astype(bf16)
    greet(sizes, at)

    shards, wholes, index = [Item(tiny)], [Item(r.tiny_all)], {N.tiny: 0}
    late = set()

    def item(name, shard, whole, start=0, size=None):
        index[name] = len(shards)
        if name in LATE_GATHERED:
            late.add(len(shards))
        shards.append(Item(shard, start, size))
        wholes.append(Item(whole, start, size))

    item(N.decay_down, down_mine, r.all_decay_down)
    for name in (N.query, N.key, N.value, N.outgate, N.output):
        item(name, getattr(r, N.w_ + name), getattr(r, N.all_ + name))
    for k in range(2):
        for name in (N.gate, N.up):
            item(name + str(k), getattr(r, N.w_ + name), getattr(r, N.all_ + name), *halves(hidden)[k])
    for k in range(2):
        item(N.down + str(k), r.w_down, r.all_down, *halves(width)[k])
    gather = Gather(
        sizes, at, shards, wholes, (r.send_sem, r.recv_sem, r.own_sem), late
    )
    gather.begin([index[name] for name in index])
    scan = scan_of(sizes, False, r)
    saved = []

    def save(*names_of):
        for name in names_of:
            source = getattr(r, N.all_ + name[7:]) if name.startswith(N.weight_) else getattr(r, name)
            copy = pltpu.make_async_copy(source, getattr(r, N.out_ + name), r.save_sem.at[len(saved)])
            copy.start()
            saved.append(copy)

    def need(*names_of):
        for name in names_of:
            gather.advance(index[name], 4)

    lower = lower_mask()

    def unpack():
        need(N.tiny)
        whole = r.tiny_all[...].reshape(devices, RANK, LANES)
        vectors[...] = jnp.zeros_like(vectors)
        vectors[0:1, :] = spread(whole[:, 0], VECTORS, per_feature, width)
        vectors[1:2, :] = spread(whole[:, 1], VECTORS, per_feature, width)
        vectors[2:3, 0:keys] = spread(whole[:, 2], VECTORS, per_key, keys)
        vectors[3:4, 0:VALUE_DIM] = spread(whole[:, 3], VECTORS, per_value, VALUE_DIM)
        decay_up = r.decay_up
        decay_up[...] = jnp.zeros_like(decay_up)
        decay_up[0:RANK, :] = spread(
            whole.reshape(devices * RANK, LANES), 0, per_key, keys
        ).astype(bf16)
        save(N.vectors, N.decay_up)

    def norm():
        def some(k):
            rows = tile(k, 32)
            plain = r.tokens[rows, :].astype(f32)
            scale = lax.rsqrt(jnp.mean(plain * plain, axis=-1, keepdims=True) + epsilon)
            r.normed[rows, :] = (plain * scale * vectors[0:1, :]).astype(bf16)
            r.grad_b[rows, :] = r.cotangent[rows, :].astype(bf16)

        loop(count_rows // 32, some)
        save(N.normed)

    def project(name, into):
        need(name)
        weight = getattr(r, N.all_ + name)
        size = min(into.shape[1], 256)

        def columns(k):
            here = tile(k, size)
            panel = weight[..., here].reshape(width, size)
            into[:, here] = dot(r.normed[...], panel, NN).astype(into.dtype)

        loop(into.shape[1] // size, columns)
        save(N.weight_ + name)

    def decay():
        project(N.decay_down, r.rank_act)
        r.decay_pre[...] = (
            dot(r.rank_act[...], r.decay_up[...], NN) + vectors[2:3, 0:keys]
        )
        save(N.rank_act, N.decay_pre)

    def attention():
        total, state = r.total, r.state
        total[...] = jnp.zeros_like(total)
        state[...] = jnp.zeros_like(state)

        def group(k):
            rows = tile(k, GROUP)
            cumulative = dot(lower, log_decay_of(r.decay_pre[rows, :]), NN, highest)
            middle = cumulative[GROUP // 2 - 1 : GROUP // 2]
            ending = cumulative[GROUP - 1 :]
            query_scaled = r.query[rows, :].astype(f32) * key_scale
            key_full = r.key[rows, :].astype(f32)
            gated_query = query_scaled * jnp.exp(cumulative - middle)
            inverse_key = key_full * jnp.exp(middle - cumulative)
            tail_key = key_full * jnp.exp(ending - cumulative)
            state_query = query_scaled * jnp.exp(cumulative)
            r.query_dev[rows, :] = state_query * jnp.exp(total[0:1, :])
            r.offsets[k] = total[...]
            for h in range(HEADS):
                across, along = head_slices(h)
                value_full = r.value[rows, along].astype(f32)
                scores = dot(gated_query[:, across], inverse_key[:, across], NT, high) * lower
                start = state[h]
                r.starts[k, h] = start.astype(bf16)
                r.mixed[rows, along] = dot(state_query[:, across], start, NT, high) + dot(
                    scores, value_full, NN, high
                )
                state[h] = jnp.exp(ending[:, across]) * start + dot(
                    value_full, tail_key[:, across], TN, high
                )
            total[...] = total[...] + ending

        loop(groups, group)
        total[...] = jnp.exp(total[...])
        save(N.query, N.key, N.value)

    def heads():
        before = r.before_state

        def some(k):
            rows = tile(k, GROUP)
            factor = jnp.exp(r.offsets[k])
            for h in range(HEADS):
                across, along = head_slices(h)
                begin = r.starts[k, h].astype(f32) + factor[0:1, across] * before[h]
                r.starts[k, h] = begin.astype(bf16)
                whole = r.mixed[rows, along] + dot(
                    r.query_dev[rows, across], before[h], NT, high
                )
                r.mixed[rows, along] = whole
                scale = lax.rsqrt(jnp.mean(whole * whole, axis=-1, keepdims=True) + epsilon)
                gate = r.gate_pre[rows, along]
                swish = gate * jax.nn.sigmoid(gate)
                r.gated[rows, along] = (
                    whole * scale * vectors[3:4, 0:VALUE_DIM] * swish
                ).astype(bf16)

        loop(groups, some)
        save(N.starts, N.gated)

    def middle():
        need(N.output)

        def columns(k):
            here = tile(k, 256)
            panel = r.all_output[..., here].reshape(values, 256)
            r.middle[:, here] = r.tokens[:, here].astype(f32) + dot(
                r.gated[...], panel, NN
            )

        loop(width // 256, columns)

        def some(k):
            rows = tile(k, 32)
            plain = r.middle[rows, :]
            scale = lax.rsqrt(jnp.mean(plain * plain, axis=-1, keepdims=True) + epsilon)
            r.normed_two[rows, :] = (plain * scale * vectors[1:2, :]).astype(bf16)

        loop(count_rows // 32, some)
        save(N.normed_two)

    def up(half):
        need(N.gate + str(half), N.up + str(half))
        start, size = halves(hidden)[half]

        def columns(k):
            here = pl.ds(pl.multiple_of(start + k * 256, 256), 256)
            normed_two = r.normed_two[...]
            gate = dot(normed_two, r.all_gate[..., here].reshape(width, 256), NN)
            line = dot(normed_two, r.all_up[..., here].reshape(width, 256), NN)
            r.up_gate[:, here] = gate
            r.up_lin[:, here] = line
            r.activated[:, here] = (gate * jax.nn.sigmoid(gate) * line).astype(bf16)

        loop(size // 256, columns)

    def down_grad():
        def out(k, slot):
            return pltpu.make_async_copy(
                r.panels.at[slot], r.out_down_grad.at[tile(k, 256), :], r.panel_sem.at[slot]
            )

        def some(k):
            slot = lax.rem(k, 2)

            @pl.when(k >= 2)
            def _():
                out(k - 2, slot).wait()

            left = r.activated[:, tile(k, 256)]
            r.panels[slot] = dot(left, r.grad_b[...], TN).astype(bf16)
            out(k, slot).start()

        count = hidden // 256
        loop(count, some)
        for k in range(max(count - 2, 0), count):
            out(k, k % 2).wait()

    down = r.all_down

    def act(half):
        need(N.down + str(half))
        start, size = halves(width)[half]
        along = slice(start, start + size)
        act_grad = r.act_grad
        count = 2 if sizes[0] % 2 == 0 else 1
        some, wide = down.shape[0] // count, hidden // count
        for k in range(count):
            here = slice(k * wide, (k + 1) * wide)
            panel = down[k * some : (k + 1) * some, :, :, :, :, along].reshape(wide, size)
            made = dot(r.grad_b[:, along], panel, NT)
            act_grad[:, here] = made if half == 0 else act_grad[:, here] + made
        if half == 0:
            return

        def finish(k):
            here = tile(k, 256)
            grad, gate, line = act_grad[:, here], r.up_gate[:, here], r.up_lin[:, here]
            sig = jax.nn.sigmoid(gate)
            r.gate_grad[:, here] = (grad * line * sig * (1.0 + gate * (1.0 - sig))).astype(bf16)
            r.lin_grad[:, here] = (grad * gate * sig).astype(bf16)

        loop(hidden // 256, finish)

    def block(half):
        need(N.down + str(half))
        start, size = halves(width)[half]

        def columns(k):
            here = pl.ds(pl.multiple_of(start + k * 256, 256), 256)
            r.block_output[:, here] = r.middle[:, here] + dot(
                r.activated[...], down[..., here].reshape(hidden, 256), NN
            )

        loop(size // 256, columns)

    def feed_back():
        save(N.gate_grad, N.lin_grad)
        part = width // sizes[0]

        def features(a):
            here = tile(a, part)
            r.normed_two_grad[:, here] = dot(
                r.gate_grad[...], r.all_gate[a].reshape(part, hidden), NT
            ) + dot(r.lin_grad[...], r.all_up[a].reshape(part, hidden), NT)

        loop(sizes[0], features)
        side = r.side
        side[...] = jnp.zeros_like(side)

        def some(k):
            rows = tile(k, 32)
            before = r.middle[rows, :]
            scale = lax.rsqrt(jnp.mean(before * before, axis=-1, keepdims=True) + epsilon)
            plain = before * scale
            grad = r.normed_two_grad[rows, :]
            side[1:2, :] = side[1:2, :] + jnp.sum(grad * plain, axis=0, keepdims=True)
            grad = grad * vectors[1:2, :]
            whole = r.cotangent[rows, :] + scale * (
                grad - plain * jnp.mean(grad * plain, axis=-1, keepdims=True)
            )
            r.middle_grad[rows, :] = whole
            r.middle_b[rows, :] = whole.astype(bf16)

        loop(count_rows // 32, some)
        save(N.middle_grad, N.middle_b)

    def heads_back():
        side = r.side
        gain = vectors[3:4, 0:VALUE_DIM]
        part = values // sizes[0]
        for h in range(HEADS):
            across, along = head_slices(h)
            first, count = h * VALUE_DIM // part, max(VALUE_DIM // part, 1)
            weight = r.all_output[first : first + count].reshape(count * part, width)
            r.gated_grad[...] = dot(r.middle_b[...], weight, NT)

            def some(k, along=along):
                rows = tile(k, GROUP)
                whole, gate = r.mixed[rows, along], r.gate_pre[rows, along]
                grad = r.gated_grad[rows, :]
                scale = lax.rsqrt(jnp.mean(whole * whole, axis=-1, keepdims=True) + epsilon)
                sig = jax.nn.sigmoid(gate)
                plain = whole * scale
                through = grad * (gate * sig)
                side[3:4, 0:VALUE_DIM] = side[3:4, 0:VALUE_DIM] + jnp.sum(
                    through * plain, axis=0, keepdims=True
                )
                back = through * gain
                r.mixed_grad[rows, along] = (
                    scale * (back - plain * jnp.mean(back * plain, axis=-1, keepdims=True))
                ).astype(bf16)
                r.outgate_grad[rows, along] = (
                    grad * plain * gain * sig * (1.0 + gate * (1.0 - sig))
                ).astype(bf16)

            loop(groups, some)
        save(N.mixed_grad, N.outgate_grad, N.side)

    pieces = dict(
        unpack=unpack,
        norm=norm,
        decay=decay,
        query=lambda: project(N.query, r.query),
        key=lambda: project(N.key, r.key),
        value=lambda: project(N.value, r.value),
        attention=attention,
        outgate=lambda: project(N.outgate, r.gate_pre),
        heads=heads,
        middle=middle,
        up0=lambda: up(0),
        up1=lambda: up(1),
        down_grad=down_grad,
        act0=lambda: act(0),
        act1=lambda: act(1),
        block0=lambda: block(0),
        block1=lambda: block(1),
        feed_back=feed_back,
        heads_back=heads_back,
    )
    run_plan(
        FORWARD_PLAN,
        pieces,
        scan,
        list(index),
        lambda name, step: gather.advance(index[name], step),
    )
    save(N.block_output)
    gather.finish()
    scan.finish()
    for copy in saved:
        copy.wait()


def run_plan(plan, pieces, scan, names, advance):
    hops = len(scan.hops)
    steps = list(pieces.values())
    for code in plan:
        if code >= 1000:
            advance(names[(code - 1000) // 10], code % 10)
        elif code < 100:
            steps[code]()
        elif code == 300:
            for k in range(3, hops):
                scan.send(k)
                scan.receive(k)
        elif code % 100 < hops:
            (scan.send if code < 200 else scan.receive)(code % 100)


def kernel_call(body, sizes, ins, outs, scratch, collective_id):
    vmem = pl.BlockSpec(memory_space=pltpu.VMEM)
    anywhere = pl.BlockSpec(memory_space=pl.ANY)
    names = list(ins) + list(outs) + list(scratch)
    assert len(set(names)) == len(names)
    results = pl.pallas_call(
        functools.partial(body, sizes, names),
        out_shape=[jax.ShapeDtypeStruct(o[0], o[1]) for o in outs.values()],
        in_specs=[vmem if i[1] else anywhere for i in ins.values()],
        out_specs=[vmem if o[2] else anywhere for o in outs.values()],
        scratch_shapes=list(scratch.values()),
        compiler_params=pltpu.CompilerParams(
            collective_id=collective_id, has_side_effects=True, vmem_limit_bytes=VMEM_LIMIT
        ),
    )(*(i[0] for i in ins.values()))
    return dict(zip(outs, results))


def forward(sizes, tokens, cotangent, small, weights):
    rows, width = tokens.shape
    keys, values = HEADS * KEY_DIM, HEADS * VALUE_DIM
    hidden = weights[N.gate].shape[1]
    groups = rows // GROUP
    most = max(max(sizes) - 1, 1)
    mine = weights[N.query].shape[0]
    ins = {N.tokens: (tokens, True), N.cotangent: (cotangent, True)}
    ins.update({name: (a, True) for name, a in small.items()})
    ins.update({N.w_ + name: (a, True) for name, a in weights.items()})
    shape_of = {name: sizes + a.shape for name, a in weights.items()}
    shape_of[N.decay_down] = sizes + (mine, LANES)
    made = dict(
        vectors=((8, width), f32),
        decay_up=((LANES, keys), bf16),
        normed=((rows, width), bf16),
        rank_act=((rows, LANES), bf16),
        decay_pre=((rows, keys), f32),
        query=((rows, keys), bf16),
        key=((rows, keys), bf16),
        value=((rows, values), bf16),
        starts=((groups, HEADS, VALUE_DIM, KEY_DIM), bf16),
        gated=((rows, values), bf16),
        normed_two=((rows, width), bf16),
        gate_grad=((rows, hidden), bf16),
        lin_grad=((rows, hidden), bf16),
        middle_grad=((rows, width), f32),
        middle_b=((rows, width), bf16),
        mixed_grad=((rows, values), bf16),
        outgate_grad=((rows, values), bf16),
        side=((8, width), f32),
        block_output=((rows, width), f32),
    )
    outs = {N.out_weight_ + name: (shape_of[name], bf16, False) for name in KEPT}
    outs.update({N.out_ + name: o + (False,) for name, o in made.items()})
    outs[N.out_down_grad] = ((hidden, width), bf16, False)
    scratch = {N.all_ + name: pltpu.VMEM(shape_of[name], bf16) for name in WEIGHTS}
    scratch.update({name: pltpu.VMEM(*o) for name, o in made.items()})
    scratch.update(
        tiny_mine=pltpu.VMEM((RANK, LANES), f32),
        tiny_all=pltpu.VMEM(sizes + (RANK, LANES), f32),
        down_mine=pltpu.VMEM((mine, LANES), bf16),
        grad_b=pltpu.VMEM((rows, width), bf16),
        gate_pre=pltpu.VMEM((rows, values), f32),
        query_dev=pltpu.VMEM((rows, keys), f32),
        offsets=pltpu.VMEM((groups, 8, keys), f32),
        mixed=pltpu.VMEM((rows, values), f32),
        middle=pltpu.VMEM((rows, width), f32),
        up_gate=pltpu.VMEM((rows, hidden), f32),
        up_lin=pltpu.VMEM((rows, hidden), f32),
        activated=pltpu.VMEM((rows, hidden), bf16),
        act_grad=pltpu.VMEM((rows, hidden), f32),
        panels=pltpu.VMEM((2, 256, width), bf16),
        normed_two_grad=pltpu.VMEM((rows, width), f32),
        gated_grad=pltpu.VMEM((rows, VALUE_DIM), f32),
        send_sem=pltpu.SemaphoreType.DMA((13, 4, most)),
        recv_sem=pltpu.SemaphoreType.DMA((13, 4, most)),
        own_sem=pltpu.SemaphoreType.DMA((13,)),
        save_sem=pltpu.SemaphoreType.DMA((len(made) + len(KEPT),)),
        panel_sem=pltpu.SemaphoreType.DMA((2,)),
    )
    scratch.update(scan_scratch(sizes))
    results = kernel_call(forward_kernel, sizes, ins, outs, scratch, 0)
    return {name[4:]: a for name, a in results.items()}


LATE_SCATTERED = (N.output,)
BACKWARD_PLAN = (
    0, 100, 2, 3, 1003, 6, 1013, 7, 200, 1023, 101, 4, 1033, 5, 1063, 1002,
    1073, 201, 102, 1043, 1053, 1012, 1001, 1011, 1022, 1062, 1032, 1021, 202, 300, 1, 1031,
    1072, 1000, 10, 8, 9, 1042, 11, 12, 1083, 1093, 1010, 1103, 1071, 1113, 13, 1020,
    1052, 1041, 1123, 1061, 1030, 1051, 1060, 1082, 1070, 1092, 1081, 1040, 1102, 1112, 1091, 1122,
    1050, 1101, 1111, 1121, 1080, 1090, 1100, 1110, 1120,
)
NORMED_BACK = (
    (N.decay_down, N.rank_grad),
    (N.query, N.query_grad),
    (N.key, N.key_grad),
    (N.value, N.value_grad),
    (N.outgate, N.outgate_grad),
)
LOADED = (
    N.query,
    N.decay_pre,
    N.mixed_grad,
    N.vectors,
    N.normed_two,
    N.gate_grad,
    N.lin_grad,
    N.gated,
    N.middle_b,
    N.normed,
    N.outgate_grad,
    N.key,
    N.value,
    N.starts,
    N.decay_up,
    N.rank_act,
    N.side,
    N.tokens,
)


def scatter_items(hidden, width):
    keys, values = HEADS * KEY_DIM, HEADS * VALUE_DIM
    items = {}
    for k, (start, size) in enumerate(halves(width)):
        items[N.down + str(k)] = (size, None, N.down, start)
    for k, (start, size) in enumerate(halves(hidden)):
        items[N.gate + str(k)] = (size, N.panel + str(k), N.gate, start)
    for k, (start, size) in enumerate(halves(hidden)):
        items[N.up + str(k)] = (size, N.panel + str(k), N.up, start)
    items[N.output] = (width, N.square0, N.output, 0)
    items[N.outgate] = (values, N.square1, N.outgate, 0)
    items[N.value] = (values, N.square0, N.value, 0)
    items[N.query] = (keys, N.query, N.query, 0)
    items[N.key] = (keys, N.key, N.key, 0)
    items[N.decay_down] = (LANES, N.decay_down, N.decay_down, 0)
    items[N.tiny] = (LANES, N.tiny, N.tiny, 0)
    return items


def backward_kernel(sizes, names, *refs):
    r = SimpleNamespace(**dict(zip(names, refs)))
    at = coords_of(sizes)
    devices = sizes[0] * sizes[1] * sizes[2] * sizes[3]
    count_rows, width = r.tokens.shape
    keys, values = HEADS * KEY_DIM, HEADS * VALUE_DIM
    hidden = r.gate_grad.shape[1]
    groups = count_rows // GROUP
    part = width // sizes[0]
    vectors, rows_sum = r.vectors, r.rows_sum
    per_feature, per_key, per_value = width // devices, keys // devices, VALUE_DIM // devices

    loads = {}
    for name in LOADED:
        loads[name] = pltpu.make_async_copy(
            getattr(r, N.in_ + name), getattr(r, name), r.load_sem.at[len(loads)]
        )
        loads[name].start()
    middle_load = pltpu.make_async_copy(
        r.in_middle_grad, r.input_grad, r.load_sem.at[len(loads)]
    )
    middle_load.start()

    def ready(*names_of):
        for name in names_of:
            if name in loads:
                loads.pop(name).wait()

    greet(sizes, at)
    items = scatter_items(hidden, width)
    index = {name: k for k, name in enumerate(items)}
    sources, stages, sums = {}, {}, {}
    for name, (size, slot, out, start) in items.items():
        k = index[name]
        if slot is None:
            sources[k] = Item(r.in_down_grad, start, size)
            stages[k] = getattr(r, N.stage_ + name)
        else:
            sources[k] = Item(getattr(r, N.slot_ + slot), 0, size)
        sums[k] = Item(getattr(r, N.sum_ + out), start, size)
    scatter = Scatter(
        sizes,
        at,
        sources,
        stages,
        [getattr(r, N.near_ + name) for name in items],
        [getattr(r, N.half_ + name) for name in items],
        [getattr(r, N.part_ + name) for name in items],
        [getattr(r, N.last_ + name) for name in items],
        sums,
        (r.send_sem, r.recv_sem, r.own_sem),
        {index[name] for name in LATE_SCATTERED},
    )
    scan = scan_of(sizes, True, r)
    in_slot = {}

    def take_slot(name):
        slot = items[name][1]
        if slot in in_slot:
            scatter.release(index[in_slot[slot]])
        in_slot[slot] = name
        return getattr(r, N.slot_ + slot)

    lower = lower_mask()
    scatter.begin(index[N.down0])
    scatter.begin(index[N.down1])

    def weight_grad(name, left, right, start=0):
        ready(left, right)
        target, columns_of = take_slot(name), items[name][0]
        size = min(columns_of, 256)

        def features(a):
            transposed = getattr(r, left)[:, tile(a, part)]

            def columns(k):
                here = pl.ds(pl.multiple_of(start + k * size, size), size)
                made = dot(transposed, getattr(r, right)[:, here], TN)
                shaped = made.reshape(target.shape[1:5] + (size,))
                target[a, :, :, :, :, tile(k, size)] = shaped.astype(bf16)

            loop(columns_of // size, columns)

        loop(sizes[0], features)
        scatter.begin(index[name])

    def begin_state():
        total, state, query_dev = r.total, r.state, r.query_grad
        rows_sum[...] = jnp.zeros_like(rows_sum)
        total[...] = jnp.zeros_like(total)
        ready(N.query, N.decay_pre, N.mixed_grad, N.vectors)

        def some(k):
            rows = tile(k, GROUP)
            cumulative = dot(lower, log_decay_of(r.decay_pre[rows, :]), NN, highest)
            r.cumulative[rows, :] = cumulative
            query_scaled = r.query[rows, :].astype(f32) * key_scale
            query_dev[rows, :] = (query_scaled * jnp.exp(cumulative + total[0:1, :])).astype(bf16)
            total[...] = total[...] + cumulative[GROUP - 1 :]

        loop(groups, some)
        for h in range(HEADS):
            across, along = head_slices(h)
            state[h] = dot(r.mixed_grad[:, along], query_dev[:, across], TN)
        total[...] = jnp.exp(total[...])

    def attention():
        ready(N.key, N.value, N.starts)
        after_state = r.before_state

        def group(k):
            g = groups - 1 - k
            rows = tile(g, GROUP)
            cumulative = r.cumulative[rows, :]
            middle = cumulative[GROUP // 2 - 1 : GROUP // 2]
            ending = cumulative[GROUP - 1 :]
            query_scaled = r.query[rows, :].astype(f32) * key_scale
            key_full = r.key[rows, :].astype(f32)
            from_middle, to_middle = jnp.exp(cumulative - middle), jnp.exp(middle - cumulative)
            to_end, from_start = jnp.exp(ending - cumulative), jnp.exp(cumulative)
            decay_end = jnp.exp(ending)
            gated_query = (query_scaled * from_middle).astype(bf16)
            inverse_key = (key_full * to_middle).astype(bf16)
            tail_key = (key_full * to_end).astype(bf16)
            state_query = (query_scaled * from_start).astype(bf16)
            grad_cumul, through_end = [], []
            for h in range(HEADS):
                across, along = head_slices(h)
                start_b, after = r.starts[g, h], after_state[h]
                start, after_b = start_b.astype(f32), after.astype(bf16)
                grad_out = r.mixed_grad[rows, along]
                value_b = r.value[rows, along]
                query_h, key_h, tail_h = (
                    gated_query[:, across],
                    inverse_key[:, across],
                    tail_key[:, across],
                )
                scores = (dot(query_h, key_h, NT) * lower).astype(bf16)
                grad_scores = (dot(grad_out, value_b, NT) * lower).astype(bf16)
                to_query = from_start[:, across] * dot(grad_out, start_b, NN)
                to_query = to_query + from_middle[:, across] * dot(grad_scores, key_h, NN)
                to_key = to_middle[:, across] * dot(grad_scores, query_h, TN)
                to_key = to_key + to_end[:, across] * dot(value_b, after_b, NN)
                to_value = dot(scores, grad_out, TN) + dot(tail_h, after_b, NT)
                end_state = decay_end[:, across] * start + dot(value_b, tail_h, TN)
                through_end.append(jnp.sum(end_state * after, axis=0, keepdims=True))
                grad_cumul.append(
                    query_scaled[:, across] * to_query - key_full[:, across] * to_key
                )
                after_state[h] = decay_end[:, across] * after + dot(
                    grad_out, state_query[:, across], TN
                )
                r.query_grad[rows, across] = (to_query * key_scale).astype(bf16)
                r.key_grad[rows, across] = to_key.astype(bf16)
                r.value_grad[rows, along] = to_value.astype(bf16)
            log_grad = dot(lower, jnp.concatenate(grad_cumul, axis=1), TN, highest)
            log_grad = log_grad + jnp.concatenate(through_end, axis=1)
            to_decay = log_grad * jax.nn.sigmoid(-r.decay_pre[rows, :]) * (1.0 / 16.0)
            rows_sum[2:3, 0:keys] = rows_sum[2:3, 0:keys] + jnp.sum(
                to_decay, axis=0, keepdims=True
            )
            r.decay_grad[rows, :] = to_decay.astype(bf16)

        loop(groups, group)

    def decay_down():
        ready(N.decay_up)
        r.rank_grad[...] = dot(r.decay_grad[...], r.decay_up[...], NT).astype(bf16)
        weight_grad(N.decay_down, N.normed, N.rank_grad)

    def input_grad():
        def panel(a, slot):
            return [
                pltpu.make_async_copy(
                    getattr(r, N.in_weight_ + name).at[a],
                    getattr(r, N.panel_ + name).at[slot],
                    r.panel_sem.at[k, slot],
                )
                for k, (name, _) in enumerate(NORMED_BACK)
            ]

        for a in range(min(2, sizes[0])):
            for copy in panel(a, a):
                copy.start()

        def features(a):
            slot = lax.rem(a, 2)
            for copy in panel(a, slot):
                copy.wait()
            made = None
            for name, grad in NORMED_BACK:
                weight = getattr(r, N.panel_ + name).at[slot]
                term = dot(getattr(r, grad)[...], weight[...].reshape(part, weight.shape[-1]), NT)
                made = term if made is None else made + term
            r.normed_grad[:, tile(a, part)] = made

            @pl.when(a + 2 < sizes[0])
            def _():
                for copy in panel(a + 2, slot):
                    copy.start()

        loop(sizes[0], features)
        middle_load.wait()
        ready(N.tokens)

        def some(k):
            rows = tile(k, 32)
            before = r.tokens[rows, :].astype(f32)
            scale = lax.rsqrt(jnp.mean(before * before, axis=-1, keepdims=True) + epsilon)
            plain = before * scale
            grad = r.normed_grad[rows, :]
            rows_sum[0:1, :] = rows_sum[0:1, :] + jnp.sum(grad * plain, axis=0, keepdims=True)
            grad = grad * vectors[0:1, :]
            r.input_grad[rows, :] = r.input_grad[rows, :] + scale * (
                grad - plain * jnp.mean(grad * plain, axis=-1, keepdims=True)
            )

        loop(count_rows // 32, some)

    def tiny():
        ready(N.rank_act, N.side)
        side = r.side
        decay_up_grad = dot(r.rank_act[...], r.decay_grad[...], TN)[0:RANK]
        row = lax.broadcasted_iota(jnp.int32, (RANK, LANES), 0)
        lane = lax.broadcasted_iota(jnp.int32, (RANK, LANES), 1)
        vectors_of = (
            (rows_sum[0:1, :], per_feature),
            (side[1:2, :], per_feature),
            (rows_sum[2:3, 0:keys], per_key),
            (side[3:4, 0:VALUE_DIM], per_value),
        )

        def cut(values_of, device, per, offset):
            group, first = divmod(device * per, LANES)
            piece = values_of[:, group * LANES : (group + 1) * LANES]
            return pltpu.roll(piece, (offset - first) % LANES, 1)

        target = take_slot(N.tiny)
        for device in range(devices):
            whole = jnp.where(lane < per_key, cut(decay_up_grad, device, per_key, 0), 0.0)
            for k, (vector, per) in enumerate(vectors_of):
                wide = jnp.broadcast_to(vector, (RANK, vector.shape[1]))
                here = (row == k) & (lane >= VECTORS) & (lane < VECTORS + per)
                whole = jnp.where(here, cut(wide, device, per, VECTORS), whole)
            place, rest = [], device
            for size in reversed(sizes):
                rest, last = divmod(rest, size)
                place.insert(0, last)
            target[tuple(place)] = whole
        scatter.begin(index[N.tiny])

    first = halves(hidden)[1][0]
    pieces = dict(
        state=begin_state,
        attention=attention,
        gate0=lambda: weight_grad(N.gate0, N.normed_two, N.gate_grad),
        gate1=lambda: weight_grad(N.gate1, N.normed_two, N.gate_grad, first),
        up0=lambda: weight_grad(N.up0, N.normed_two, N.lin_grad),
        up1=lambda: weight_grad(N.up1, N.normed_two, N.lin_grad, first),
        output=lambda: weight_grad(N.output, N.gated, N.middle_b),
        outgate=lambda: weight_grad(N.outgate, N.normed, N.outgate_grad),
        query=lambda: weight_grad(N.query, N.normed, N.query_grad),
        key=lambda: weight_grad(N.key, N.normed, N.key_grad),
        value=lambda: weight_grad(N.value, N.normed, N.value_grad),
        decay_down=decay_down,
        input_grad=input_grad,
        tiny=tiny,
    )
    run_plan(
        BACKWARD_PLAN,
        pieces,
        scan,
        list(items),
        lambda name, step: scatter.advance(index[name], step),
    )
    scatter.finish()
    scan.finish()
    ready(*list(loads))


def backward(sizes, tokens, saved):
    outer, inner, side, core = sizes
    devices = outer * inner * side * core
    most = max(max(sizes) - 1, 1)
    rows, width = tokens.shape
    hidden = saved[N.gate_grad].shape[1]
    keys, values = HEADS * KEY_DIM, HEADS * VALUE_DIM
    mine, mine_down = width // devices, hidden // devices
    down_grad = saved[N.down_grad].reshape(sizes + (mine_down, width))
    saved = dict(saved, tokens=tokens)
    ins = {N.in_ + name: (saved[name], False) for name in LOADED}
    ins[N.in_middle_grad] = (saved[N.middle_grad], False)
    ins[N.in_down_grad] = (down_grad, False)
    ins.update({N.in_weight_ + name: (saved[N.weight_ + name], False) for name in KEPT})
    items = scatter_items(hidden, width)
    block, scratch, sums = {}, {}, {}
    for name, (size, slot, out, start) in items.items():
        rows_of = {N.down: mine_down, N.tiny: RANK}.get(out, mine)
        dtype = f32 if out == N.tiny else bf16
        block = (rows_of, size)
        sums[N.sum_ + out] = ((rows_of, start + size), f32, True)
        if slot is None:
            scratch[N.stage_ + name] = pltpu.VMEM((2, inner, side) + block, dtype)
        elif N.slot_ + slot not in scratch:
            scratch[N.slot_ + slot] = pltpu.VMEM(sizes + block, dtype)
        scratch[N.near_ + name] = pltpu.VMEM((outer, inner, side) + block, dtype)
        order = orders_of(sizes, name in LATE_SCATTERED)[0]
        for step, landing in ((2, N.half_), (1, N.part_), (0, N.last_)):
            lead = (max(sizes[order[step]] - 1, 1),) + tuple(sizes[k] for k in order[:step])
            scratch[landing + name] = pltpu.VMEM(lead + block, dtype)
    scratch.update({n: pltpu.VMEM(saved[n].shape, saved[n].dtype) for n in LOADED})
    scratch.update(
        {
            N.panel_ + n: pltpu.VMEM((2,) + saved[N.weight_ + n].shape[1:], bf16)
            for n, _ in NORMED_BACK
        }
    )
    scratch.update(
        rows_sum=pltpu.VMEM((8, width), f32),
        cumulative=pltpu.VMEM((rows, keys), f32),
        query_grad=pltpu.VMEM((rows, keys), bf16),
        key_grad=pltpu.VMEM((rows, keys), bf16),
        value_grad=pltpu.VMEM((rows, values), bf16),
        decay_grad=pltpu.VMEM((rows, keys), bf16),
        rank_grad=pltpu.VMEM((rows, LANES), bf16),
        normed_grad=pltpu.VMEM((rows, width), f32),
        send_sem=pltpu.SemaphoreType.DMA((len(items), 4, most)),
        recv_sem=pltpu.SemaphoreType.DMA((len(items), 4, most)),
        own_sem=pltpu.SemaphoreType.DMA((len(items), 2)),
        load_sem=pltpu.SemaphoreType.DMA((len(LOADED) + 1,)),
        panel_sem=pltpu.SemaphoreType.DMA((len(NORMED_BACK), 2)),
    )
    scratch.update(scan_scratch(sizes))
    outs = dict(sums, input_grad=((rows, width), f32, True))
    return kernel_call(backward_kernel, sizes, ins, outs, scratch, 1)


def turned(array, precision=None):
    size = array.shape[0]
    rows = lax.broadcasted_iota(jnp.int32, (size, size), 0)
    columns = lax.broadcasted_iota(jnp.int32, (size, size), 1)
    return dot(array, jnp.where(rows == columns, 1.0, 0.0).astype(array.dtype), TN, precision)


def hand_out_kernel(count, cuts, *refs):
    whole, down, tiny = refs[:count], refs[count], refs[count + 1]
    outs, small, sems = refs[count + 2 : 2 * count + 2], refs[2 * count + 2 : -1], refs[-1]
    copies = []
    for k, (source, target) in enumerate(zip(whole, outs)):
        copies.append(pltpu.make_async_copy(source, target, sems.at[k]))
        copies[-1].start()
    small[0][...] = turned(down[...], highest)[0 : small[0].shape[0]]
    for target, (row, column) in zip(small[1:], cuts):
        target[...] = tiny[row : row + target.shape[0], column : column + target.shape[1]]
    for copy in copies:
        copy.wait()


def hand_out(arrays, decay_down, tiny, cuts):
    vmem = pl.BlockSpec(memory_space=pltpu.VMEM)
    shapes = [a.shape for a in arrays] + [(RANK, decay_down.shape[0])] + [c[0] for c in cuts]
    return pl.pallas_call(
        functools.partial(hand_out_kernel, len(arrays), [c[1] for c in cuts]),
        out_shape=[jax.ShapeDtypeStruct(s, f32) for s in shapes],
        in_specs=[vmem] * (len(arrays) + 2),
        out_specs=[pl.BlockSpec(memory_space=pl.ANY)] * len(arrays) + [vmem] * (len(cuts) + 1),
        scratch_shapes=[pltpu.SemaphoreType.DMA((len(arrays),))],
        compiler_params=pltpu.CompilerParams(vmem_limit_bytes=VMEM_LIMIT),
    )(*arrays, decay_down, tiny)


def local(
    sizes,
    inputs,
    cotangent,
    mixer_gain,
    feed_gain,
    w_query,
    w_key,
    w_value,
    w_outgate,
    w_decay_down,
    w_decay_up,
    decay_bias,
    head_gain,
    w_output,
    w_gate,
    w_up,
    w_down,
):
    width = inputs.shape[2]
    rows = inputs.shape[0] * inputs.shape[1]
    per_feature, per_key, per_value = (
        mixer_gain.shape[0],
        decay_bias.shape[0],
        head_gain.shape[0],
    )
    tokens = inputs.reshape(rows, width)
    small = dict(
        w_decay_up=w_decay_up,
        mixer_gain=mixer_gain.reshape(1, -1),
        feed_gain=feed_gain.reshape(1, -1),
        decay_bias=decay_bias.reshape(1, -1),
        head_gain=head_gain.reshape(1, -1),
    )
    weights = dict(
        decay_down=w_decay_down.T,
        query=w_query,
        key=w_key,
        value=w_value,
        outgate=w_outgate,
        output=w_output,
        gate=w_gate,
        up=w_up,
        down=w_down,
    )
    saved = forward(sizes, tokens, cotangent.reshape(rows, width), small, weights)
    got = backward(sizes, tokens, saved)
    names = (N.query, N.key, N.value, N.outgate, N.output, N.gate, N.up, N.down)
    handed = hand_out(
        [saved[N.block_output], got[N.input_grad]] + [got[N.sum_ + name] for name in names],
        got[N.sum_decay_down],
        got[N.sum_tiny],
        (
            ((RANK, per_key), (0, 0)),
            ((1, per_feature), (0, VECTORS)),
            ((1, per_feature), (1, VECTORS)),
            ((1, per_key), (2, VECTORS)),
            ((1, per_value), (3, VECTORS)),
        ),
    )
    result, input_grad = (a.reshape(inputs.shape) for a in handed[:2])
    g_query, g_key, g_value, g_outgate, g_output, g_gate, g_up, g_down = handed[2:10]
    decay_down, decay_up = handed[10:12]
    g_mixer, g_feed, g_bias, g_head = (a.reshape(-1) for a in handed[12:])
    return (
        result,
        input_grad,
        g_mixer,
        g_feed,
        g_query,
        g_key,
        g_value,
        g_outgate,
        decay_down.T,
        decay_up,
        g_bias,
        g_head,
        g_output,
        g_gate,
        g_up,
        g_down,
    )


def solution(mesh):
    placed = (
        P("batch", "seq", None),
        P("batch", "seq", None),
        P(("seq", "batch")),
        P(("seq", "batch")),
        P(("seq", "batch"), None),
        P(("seq", "batch"), None),
        P(("seq", "batch"), None),
        P(("seq", "batch"), None),
        P(("seq", "batch"), None),
        P(None, ("seq", "batch")),
        P(("seq", "batch")),
        P(("seq", "batch")),
        P(("seq", "batch"), None),
        P(("seq", "batch"), None),
        P(("seq", "batch"), None),
        P(("seq", "batch"), None),
    )
    return jax.shard_map(
        functools.partial(local, grid_of(mesh.shape)),
        mesh=mesh,
        in_specs=placed,
        out_specs=(
            P("batch", "seq", None),
            P("batch", "seq", None),
            P(("seq", "batch")),
            P(("seq", "batch")),
            P(("seq", "batch"), None),
            P(("seq", "batch"), None),
            P(("seq", "batch"), None),
            P(("seq", "batch"), None),
            P(("seq", "batch"), None),
            P(None, ("seq", "batch")),
            P(("seq", "batch")),
            P(("seq", "batch")),
            P(("seq", "batch"), None),
            P(("seq", "batch"), None),
            P(("seq", "batch"), None),
            P(("seq", "batch"), None),
        ),
        check_vma=False,
    )
```

```python
import functools
from types import SimpleNamespace

import jax
import jax.numpy as jnp
from jax import lax
from jax.experimental import pallas as pl
from jax.experimental.pallas import tpu as pltpu
from jax.sharding import PartitionSpec as P

HEADS = 4
KEY_DIM = 128
VALUE_DIM = 256
GROUP = 64
LANES = 128
RANK = 16
VECTORS = 32
MESH = pl.DeviceIdType.MESH
VMEM_LIMIT = 67_000_000


class Names:
    def __getattr__(self, name):
        return name


N = Names()
epsilon = 1e-06
key_scale = KEY_DIM ** (-0.5)
highest = lax.Precision.HIGHEST
high = lax.Precision.HIGH
f32 = jnp.float32
bf16 = jnp.bfloat16


def grid_of(shape):
    seq, batch = shape["seq"], shape["batch"]
    outer = 4 if seq % 4 == 0 else seq
    core = 2 if batch % 2 == 0 else 1
    return (outer, seq // outer, batch // core, core)


def coords_of(sizes):
    seq, batch = lax.axis_index("seq"), lax.axis_index("batch")
    return (seq // sizes[1], seq % sizes[1], batch // sizes[3], batch % sizes[3])


def device_of(sizes, at):
    return {"seq": at[0] * sizes[1] + at[1], "batch": at[2] * sizes[3] + at[3]}


def place_of(sizes, device):
    place = []
    for size in reversed(sizes):
        device, last = divmod(device, size)
        place.insert(0, last)
    return tuple(place)


def moved(sizes, at, axis, by):
    new = list(at)
    new[axis] = lax.rem(at[axis] + (by % sizes[axis]), sizes[axis])
    return tuple(new)


def region(ref, free, at):
    return ref.at[tuple(slice(None) if k in free else at[k] for k in range(4))]


def orders_of(sizes, late=False):
    orders = ((1, 2, 0, 3), (2, 1, 0, 3)) if late else ((0, 1, 2, 3), (0, 2, 1, 3))
    return orders if sizes[1] == sizes[2] and sizes[3] == 2 else orders[:1]


def hops_of(sizes):
    length, hops = sizes[0] * sizes[1], []
    while 2 ** len(hops) < length:
        hops.append(2 ** len(hops))
    return hops


def greet(sizes, at):
    barrier = pltpu.get_barrier_semaphore()
    length = sizes[0] * sizes[1]
    seq, batch = lax.axis_index("seq"), lax.axis_index("batch")
    targets = [
        device_of(sizes, moved(sizes, at, axis, by))
        for axis in range(4)
        for by in range(1, sizes[axis])
    ]
    for hop in hops_of(sizes):
        for by in (hop, length - hop):
            targets.append({"seq": lax.rem(seq + by, length), "batch": batch})
    for target in targets:
        pl.semaphore_signal(barrier, inc=1, device_id=target, device_id_type=MESH)
    pl.semaphore_wait(barrier, len(targets))


def by_order(sizes, at, act, late=False):
    orders = orders_of(sizes, late)
    if len(orders) == 1:
        act(orders[0])
        return
    for parity, order in enumerate(orders):
        pl.when(at[3] == parity)(functools.partial(act, order))


def loop(count, body):
    def step(k, carry):
        body(k)
        return carry

    lax.fori_loop(0, count, step, 0)


def dot(left, right, dims, precision=None):
    return lax.dot_general(
        left, right, (dims, ((), ())), precision=precision, preferred_element_type=f32
    )


NN = ((1,), (0,))
NT = ((1,), (1,))
TN = ((0,), (0,))


class Item:
    def __init__(self, ref, start=0, size=None):
        self.ref, self.start = ref, start
        self.size = ref.shape[-1] if size is None else size
        self.part = self.size != ref.shape[-1]

    def tail(self):
        return (slice(None), slice(self.start, self.start + self.size)) if self.part else ()

    def at(self, index):
        return self.ref.at[tuple(index) + self.tail()]


def blocks_of(free, at, axes=4):
    return tuple(slice(None) if k in free else at[k] for k in range(axes))


class Gather:
    def __init__(self, sizes, at, shards, wholes, sems, late):
        self.sizes, self.at, self.late = sizes, at, late
        self.shards, self.wholes = shards, wholes
        self.send_sem, self.recv_sem, self.own_sem = sems
        self.done = {item: 0 for item in range(len(shards))}

    def copies(self, item, order, step, arriving):
        axis, free = order[step], order[:step]
        made = []
        for by in range(1, self.sizes[axis]):
            source = moved(self.sizes, self.at, axis, -by) if arriving else self.at
            place = self.wholes[item].at(blocks_of(free, source))
            made.append(
                pltpu.make_async_remote_copy(
                    src_ref=self.shards[item].at(()) if step == 0 and not arriving else place,
                    dst_ref=place,
                    send_sem=self.send_sem.at[item, step, by - 1],
                    recv_sem=self.recv_sem.at[item, step, by - 1],
                    device_id=device_of(self.sizes, moved(self.sizes, self.at, axis, by)),
                    device_id_type=MESH,
                )
            )
        return made

    def own(self, item):
        return pltpu.make_async_copy(
            self.shards[item].at(()),
            self.wholes[item].at(blocks_of((), self.at)),
            self.own_sem.at[item],
        )

    def begin(self, items):
        for item in items:

            def act(order, item=item):
                for copy in self.copies(item, order, 0, False):
                    copy.start()

            if item in self.late:
                by_order(self.sizes, self.at, act, True)
            else:
                act(orders_of(self.sizes)[0])
            self.own(item).start()

    def advance(self, item, step):
        while self.done[item] < step:
            now = self.done[item] = self.done[item] + 1
            if now == 1:
                self.own(item).wait()

            def act(order, now=now):
                for copy in self.copies(item, order, now - 1, True):
                    copy.wait_recv()
                if now < 4:
                    for copy in self.copies(item, order, now, False):
                        copy.start()

            by_order(self.sizes, self.at, act, item in self.late)

    def finish(self):
        for item in self.done:
            self.advance(item, 4)
        for late in (False, True):

            def act(order, late=late):
                for item in self.done:
                    if (item in self.late) == late:
                        for step in range(4):
                            for copy in self.copies(item, order, step, False):
                                copy.wait_send()

            by_order(self.sizes, self.at, act, late)


class Scatter:
    def __init__(self, sizes, at, sources, lands, sums, outs, sems, late, stop=0):
        self.sizes, self.at, self.late, self.stop = sizes, at, late, stop
        self.outs = outs
        self.sources, self.sums = sources, sums
        self.near, self.lands = lands[3], lands
        self.send_sem, self.recv_sem, self.load_sem, self.out_sem = sems
        self.left, self.sent, self.resumed = {}, {}, {}

    def copy(self, item, order, step, by):
        axis, free = order[step], order[:step]
        target = moved(self.sizes, self.at, axis, by)
        if step == 3:
            source = self.sources[item].at(blocks_of(free, target))
            landing = self.near[item]
        else:
            whole = self.resumed[item] if step == 1 and item in self.resumed else self.near[item]
            source = whole.at[blocks_of(free, target, 3)]
            landing = self.lands[step][item].at[by - 1]
        return pltpu.make_async_remote_copy(
            src_ref=source,
            dst_ref=landing,
            send_sem=self.send_sem.at[item, step, by - 1],
            recv_sem=self.recv_sem.at[item, step, by - 1],
            device_id=device_of(self.sizes, target),
            device_id_type=MESH,
        )

    def begin(self, item):
        self.left[item] = 4
        self.sent[item] = {3}
        self.copy(item, orders_of(self.sizes)[0], 3, 1).start()

    def load(self, item):
        return pltpu.make_async_copy(self.resumed[item], self.near[item], self.load_sem.at[item])

    def resume(self, item, far):
        self.left[item] = 2
        self.sent[item] = {1}
        self.resumed[item] = far
        self.load(item).start()

        def act(order):
            for by in range(1, self.sizes[order[1]]):
                self.copy(item, order, 1, by).start()

        by_order(self.sizes, self.at, act, item in self.late)

    def advance(self, item, step):
        while self.left[item] > max(step, self.stop):
            now = self.left[item] = self.left[item] - 1
            more = now > self.stop
            if more:
                self.sent[item].add(now - 1)
            if now == 1 and item in self.resumed:
                self.load(item).wait()

            def act(order, now=now, more=more):
                self.add(item, order, now)
                if more:
                    for by in range(1, self.sizes[order[now - 1]]):
                        self.copy(item, order, now - 1, by).start()

            by_order(self.sizes, self.at, act, item in self.late)
            if now == 0:
                self.out(item).start()

    def out(self, item):
        return pltpu.make_async_copy(
            self.sums[item].at(()), self.outs[item].at(()), self.out_sem.at[item]
        )

    def add(self, item, order, step):
        sizes, at = self.sizes, self.at
        axis, free = order[step], sorted(order[:step])
        near = self.near[item]
        for by in range(1, sizes[axis]):
            self.copy(item, order, step, by).wait_recv()
        if step == 0:
            total = near[at[0], at[1], at[2]].astype(f32)
            for by in range(1, sizes[axis]):
                total = total + self.lands[0][item][by - 1].astype(f32)
            kept = self.sums[item]
            kept.ref[:, kept.start : kept.start + kept.size] = total
            return

        def at_first(k):
            for j in range(sizes[free[1]] if len(free) > 1 else 1):
                for i in range(sizes[free[2]] if len(free) > 2 else 1):
                    within = (k, j, i)[: len(free)]
                    place = list(at[:3])
                    for axis_of, index in zip(free, within):
                        place[axis_of] = index
                    place = tuple(place)
                    total = near[place].astype(f32)
                    if step == 3:
                        source = self.sources[item]
                        mine = source.ref[place + (at[3],) + source.tail()]
                        total = total + mine.astype(f32)
                    else:
                        for by in range(1, sizes[axis]):
                            come = self.lands[step][item].at[by - 1]
                            total = total + come[within].astype(f32)
                    near[place] = total.astype(near.dtype)

        loop(sizes[free[0]], at_first)

    def release(self, item):
        self.advance(item, 3)
        self.sent[item].remove(3)
        self.copy(item, orders_of(self.sizes)[0], 3, 1).wait_send()

    def finish(self):
        for item in self.left:
            self.advance(item, 0)
            if self.stop == 0:
                self.out(item).wait()
        for late in (False, True):

            def act(order, late=late):
                for item in self.left:
                    if (item in self.late) == late:
                        for step in sorted(self.sent[item]):
                            for by in range(1, self.sizes[order[step]]):
                                self.copy(item, order, step, by).wait_send()

            by_order(self.sizes, self.at, act, late)


class Scan:
    def __init__(self, sizes, reverse, total, state, before_total, before_state, buffers, sems):
        self.sizes, self.reverse = sizes, reverse
        self.total, self.state = total, state
        self.before_total, self.before_state = before_total, before_state
        self.total_out, self.total_in, self.state_out, self.state_in = buffers
        self.sems = sems
        self.hops = hops_of(sizes)
        self.length = sizes[0] * sizes[1]
        self.place = self.length - 1 - lax.axis_index("seq") if reverse else lax.axis_index("seq")

    def copies(self, k):
        seq = lax.axis_index("seq")
        hop = self.length - self.hops[k] if self.reverse else self.hops[k]
        target = {"seq": lax.rem(seq + hop, self.length), "batch": lax.axis_index("batch")}
        pairs = ((self.total_out, self.total_in), (self.state_out, self.state_in))
        return [
            pltpu.make_async_remote_copy(
                src_ref=out.at[k],
                dst_ref=come.at[k],
                send_sem=self.sems.at[0, k, n],
                recv_sem=self.sems.at[1, k, n],
                device_id=target,
                device_id_type=MESH,
            )
            for n, (out, come) in enumerate(pairs)
        ]

    def send(self, k):
        if k == 0:
            self.before_total[...] = jnp.ones_like(self.before_total)
            self.before_state[...] = jnp.zeros_like(self.before_state)
        self.total_out[k] = self.total[...]
        for h in range(HEADS):
            self.state_out[k, h] = self.state[h].astype(bf16)

        @pl.when(self.place + self.hops[k] < self.length)
        def _():
            for copy in self.copies(k):
                copy.start()

    def receive(self, k):
        @pl.when(self.place >= self.hops[k])
        def _():
            for copy in self.copies(k):
                copy.wait_recv()
            come = self.total_in[k]
            for h in range(HEADS):
                keys = slice(h * KEY_DIM, (h + 1) * KEY_DIM)
                state = self.state_in[k, h].astype(f32)
                self.before_state[h] = (
                    self.before_state[h] + self.before_total[0:1, keys] * state
                )
                if k + 1 < len(self.hops):
                    self.state[h] = self.state[h] + self.total[0:1, keys] * state
            self.before_total[...] = self.before_total[...] * come
            if k + 1 < len(self.hops):
                self.total[...] = self.total[...] * come

    def finish(self):
        for k in range(len(self.hops)):

            @pl.when(self.place + self.hops[k] < self.length)
            def _(k=k):
                for copy in self.copies(k):
                    copy.wait_send()


def lower_mask():
    rows = lax.broadcasted_iota(jnp.int32, (GROUP, GROUP), 0)
    columns = lax.broadcasted_iota(jnp.int32, (GROUP, GROUP), 1)
    return jnp.where(rows >= columns, 1.0, 0.0).astype(f32)


def log_decay_of(decay_pre):
    return jax.nn.log_sigmoid(decay_pre) * (1.0 / 16.0)


def spread(block, offset, per, width):
    devices = width // per
    lane = lax.broadcasted_iota(jnp.int32, (LANES, width), 0)
    column = lax.broadcasted_iota(jnp.int32, (LANES, width), 1)
    pick = jnp.where(lane == offset + column % per, 1.0, 0.0).astype(bf16)
    wide = dot(block.astype(bf16), pick, NN)
    rows = block.shape[0] // devices
    wide = wide.reshape(devices, rows, width)
    device = lax.broadcasted_iota(jnp.int32, wide.shape, 0)
    column = lax.broadcasted_iota(jnp.int32, wide.shape, 2)
    return jnp.sum(jnp.where(device == column // per, wide, 0.0), axis=0)


def turned(array, precision=None):
    size = array.shape[0]
    rows = lax.broadcasted_iota(jnp.int32, (size, size), 0)
    columns = lax.broadcasted_iota(jnp.int32, (size, size), 1)
    return dot(array, jnp.where(rows == columns, 1.0, 0.0).astype(array.dtype), TN, precision)


def scan_scratch(sizes):
    hops = len(hops_of(sizes))
    keys = HEADS * KEY_DIM
    return dict(
        total=pltpu.VMEM((8, keys), f32),
        state=pltpu.VMEM((HEADS, VALUE_DIM, KEY_DIM), f32),
        before_total=pltpu.VMEM((8, keys), f32),
        before_state=pltpu.VMEM((HEADS, VALUE_DIM, KEY_DIM), f32),
        total_out=pltpu.VMEM((hops, 8, keys), f32),
        total_in=pltpu.VMEM((hops, 8, keys), f32),
        state_out=pltpu.VMEM((hops, HEADS, VALUE_DIM, KEY_DIM), bf16),
        state_in=pltpu.VMEM((hops, HEADS, VALUE_DIM, KEY_DIM), bf16),
        scan_sem=pltpu.SemaphoreType.DMA((2, hops, 2)),
    )


def scan_of(sizes, reverse, r):
    return Scan(
        sizes,
        reverse,
        r.total,
        r.state,
        r.before_total,
        r.before_state,
        (r.total_out, r.total_in, r.state_out, r.state_in),
        r.scan_sem,
    )


def head_slices(h):
    return slice(h * KEY_DIM, (h + 1) * KEY_DIM), slice(h * VALUE_DIM, (h + 1) * VALUE_DIM)


def tile(k, size):
    return pl.ds(pl.multiple_of(k * size, size), size)


def halves(columns):
    first = -(-columns // 512) * 256
    return ((0, first), (first, columns - first))


WEIGHTS = (N.decay_down, N.query, N.key, N.value, N.outgate, N.output, N.gate, N.up, N.down)
KEPT = WEIGHTS[:5]
LATE_GATHERED = (N.down1,)
GATHER_ORDER = (0, 3, 2, 1, 4, 5, 10, 6, 7, 12, 9, 11, 8)
FORWARD_PLAN = (
    1001, 1121, 1031, 1002, 1021, 1011, 1003, 1032, 1022, 1004, 0, 1012, 1, 1041, 1033, 1023,
    1034, 4, 1013, 1051, 1042, 1024, 3, 1014, 2, 1052, 1101, 1043, 1061, 1102, 1044, 5,
    6, 1071, 1062, 1053, 100, 1054, 7, 1103, 1072, 1104, 1063, 200, 101, 1081, 1064, 201,
    102, 1091, 1111, 1073, 1082, 1074, 202, 1122, 300, 8, 1092, 9, 1112, 1083, 1084, 10,
    1093, 1094, 1113, 11, 1123, 12, 1114, 1124, 14, 2003, 13, 16, 2013, 2002, 17, 15,
    2012,
)


def forward_kernel(sizes, names, *refs):
    r = SimpleNamespace(**dict(zip(names, refs)))
    r.mixed_grad, r.outgate_grad, r.middle_b = r.gated, r.normed, r.tokens
    at = coords_of(sizes)
    devices = sizes[0] * sizes[1] * sizes[2] * sizes[3]
    count_rows, width = r.tokens.shape
    keys, values = HEADS * KEY_DIM, HEADS * VALUE_DIM
    hidden = r.up_gate.shape[1]
    groups = count_rows // GROUP
    vectors = r.vectors
    per_feature, per_key, per_value = width // devices, keys // devices, VALUE_DIM // devices

    loads = [
        pltpu.make_async_copy(r.in_tokens, r.tokens, r.input_sem.at[0]),
        pltpu.make_async_copy(r.in_cotangent, r.cotangent, r.input_sem.at[1]),
    ]
    for copy in loads:
        copy.start()
    tiny = r.tiny_mine
    tiny[...] = jnp.zeros_like(tiny)
    tiny[:, 0:per_key] = r.w_decay_up[...].astype(f32)
    for k, name in enumerate((N.mixer_gain, N.feed_gain, N.decay_bias, N.head_gain)):
        vector = getattr(r, name)
        tiny[k : k + 1, VECTORS : VECTORS + vector.shape[1]] = vector[...].astype(f32)
    down_mine = r.down_mine
    down_mine[...] = jnp.zeros_like(down_mine)
    down_mine[:, 0:RANK] = turned(r.w_decay_down[...]).astype(bf16)
    greet(sizes, at)

    shards, wholes, index = [Item(tiny)], [Item(r.tiny_all)], {N.tiny: 0}
    late = set()

    def item(name, shard, whole, start=0, size=None):
        index[name] = len(shards)
        if name in LATE_GATHERED:
            late.add(len(shards))
        shards.append(Item(shard, start, size))
        wholes.append(Item(whole, start, size))

    item(N.decay_down, down_mine, r.all_decay_down)
    for name in (N.query, N.key, N.value, N.outgate, N.output):
        item(name, getattr(r, N.w_ + name), getattr(r, N.all_ + name))
    for k in range(2):
        for name in (N.gate, N.up):
            item(name + str(k), getattr(r, N.w_ + name), getattr(r, N.all_ + name), *halves(hidden)[k])
    for k in range(2):
        item(N.down + str(k), r.w_down, r.all_down, *halves(width)[k])
    gather = Gather(
        sizes, at, shards, wholes, (r.send_sem, r.recv_sem, r.own_sem), late
    )
    gather.begin(GATHER_ORDER)
    scan = scan_of(sizes, False, r)
    saved = []
    scatter = Scatter(
        sizes,
        at,
        [Item(r.down_grad, 0, size) for _, size in halves(width)],
        {3: (r.near_down0, r.near_down1), 2: (r.half_down0, r.half_down1)},
        None,
        None,
        (r.back_send_sem, r.back_recv_sem, None, None),
        (),
        2,
    )

    def save(*names_of):
        for name in names_of:
            source = getattr(r, N.all_ + name[7:]) if name.startswith(N.weight_) else getattr(r, name)
            copy = pltpu.make_async_copy(source, getattr(r, N.out_ + name), r.save_sem.at[len(saved)])
            copy.start()
            saved.append(copy)

    def need(*names_of):
        for name in names_of:
            gather.advance(index[name], 4)

    lower = lower_mask()

    def turn(source, target):
        def columns(k):
            target[tile(k, 256), :] = turned(source[:, tile(k, 256)]).astype(bf16)

        loop(source.shape[1] // 256, columns)

    def unpack():
        need(N.tiny)
        whole = r.tiny_all[...].reshape(devices, RANK, LANES)
        vectors[...] = jnp.zeros_like(vectors)
        vectors[0:1, :] = spread(whole[:, 0], VECTORS, per_feature, width)
        vectors[1:2, :] = spread(whole[:, 1], VECTORS, per_feature, width)
        vectors[2:3, 0:keys] = spread(whole[:, 2], VECTORS, per_key, keys)
        vectors[3:4, 0:VALUE_DIM] = spread(whole[:, 3], VECTORS, per_value, VALUE_DIM)
        decay_up = r.decay_up
        decay_up[...] = jnp.zeros_like(decay_up)
        lane = lax.broadcasted_iota(jnp.int32, (RANK, LANES), 1)
        together = LANES // per_key
        for group in range(keys // LANES):
            joined = jnp.zeros((RANK, LANES), f32)
            for k in range(together):
                block = r.tiny_all[place_of(sizes, group * together + k)]
                here = (lane >= k * per_key) & (lane < (k + 1) * per_key)
                joined = jnp.where(here, pltpu.roll(block, k * per_key, 1), joined)
            decay_up[0:RANK, group * LANES : (group + 1) * LANES] = joined.astype(bf16)
        save(N.vectors, N.decay_up)

    def norm():
        for copy in loads:
            copy.wait()

        def some(k):
            rows = tile(k, 32)
            plain = r.tokens[rows, :].astype(f32)
            scale = lax.rsqrt(jnp.mean(plain * plain, axis=-1, keepdims=True) + epsilon)
            r.normed[rows, :] = (plain * scale * vectors[0:1, :]).astype(bf16)
            r.grad_b[rows, :] = r.cotangent[rows, :].astype(bf16)

        loop(count_rows // 32, some)
        turn(r.normed, r.normed_t)
        save(N.normed_t)

    def project(name, into):
        need(name)
        weight = getattr(r, N.all_ + name)
        size = min(into.shape[1], 256)

        def columns(k):
            here = tile(k, size)
            panel = weight[..., here].reshape(width, size)
            into[:, here] = dot(r.normed[...], panel, NN).astype(into.dtype)

        loop(into.shape[1] // size, columns)
        save(N.weight_ + name)

    def decay():
        project(N.decay_down, r.rank_act)
        r.decay_pre[...] = (
            dot(r.rank_act[...], r.decay_up[...], NN) + vectors[2:3, 0:keys]
        )
        save(N.rank_act, N.decay_pre)

    def attention():
        total, state = r.total, r.state
        total[...] = jnp.zeros_like(total)
        state[...] = jnp.zeros_like(state)

        def group(k):
            rows = tile(k, GROUP)
            cumulative = dot(lower, log_decay_of(r.decay_pre[rows, :]), NN, highest)
            middle = cumulative[GROUP // 2 - 1 : GROUP // 2]
            ending = cumulative[GROUP - 1 :]
            query_scaled = r.query[rows, :].astype(f32) * key_scale
            key_full = r.key[rows, :].astype(f32)
            gated_query = query_scaled * jnp.exp(cumulative - middle)
            inverse_key = key_full * jnp.exp(middle - cumulative)
            tail_key = key_full * jnp.exp(ending - cumulative)
            state_query = query_scaled * jnp.exp(cumulative)
            r.query_dev[rows, :] = state_query * jnp.exp(total[0:1, :])
            r.offsets[k] = total[...]
            for h in range(HEADS):
                across, along = head_slices(h)
                value_full = r.value[rows, along].astype(f32)
                scores = dot(gated_query[:, across], inverse_key[:, across], NT, high) * lower
                start = state[h]
                r.starts[k, h] = start.astype(bf16)
                r.mixed[rows, along] = dot(state_query[:, across], start, NT, high) + dot(
                    scores, value_full, NN, high
                )
                state[h] = jnp.exp(ending[:, across]) * start + dot(
                    value_full, tail_key[:, across], TN, high
                )
            total[...] = total[...] + ending

        loop(groups, group)
        total[...] = jnp.exp(total[...])
        save(N.query, N.key, N.value)

    def heads():
        before = r.before_state

        def some(k):
            rows = tile(k, GROUP)
            factor = jnp.exp(r.offsets[k])
            for h in range(HEADS):
                across, along = head_slices(h)
                begin = r.starts[k, h].astype(f32) + factor[0:1, across] * before[h]
                r.starts[k, h] = begin.astype(bf16)
                whole = r.mixed[rows, along] + dot(
                    r.query_dev[rows, across], before[h], NT, high
                )
                r.mixed[rows, along] = whole
                scale = lax.rsqrt(jnp.mean(whole * whole, axis=-1, keepdims=True) + epsilon)
                gate = r.gate_pre[rows, along]
                swish = gate * jax.nn.sigmoid(gate)
                r.gated[rows, along] = (
                    whole * scale * vectors[3:4, 0:VALUE_DIM] * swish
                ).astype(bf16)

        loop(groups, some)
        turn(r.gated, r.gated_t)
        save(N.starts, N.gated_t)

    def middle():
        need(N.output)

        def columns(k):
            here = tile(k, 256)
            panel = r.all_output[..., here].reshape(values, 256)
            r.middle[:, here] = r.tokens[:, here].astype(f32) + dot(
                r.gated[...], panel, NN
            )

        loop(width // 256, columns)

        def some(k):
            rows = tile(k, 32)
            plain = r.middle[rows, :]
            scale = lax.rsqrt(jnp.mean(plain * plain, axis=-1, keepdims=True) + epsilon)
            r.normed_two[rows, :] = (plain * scale * vectors[1:2, :]).astype(bf16)

        loop(count_rows // 32, some)
        turn(r.normed_two, r.normed_two_t)
        save(N.normed_two_t)

    def up(half):
        need(N.gate + str(half), N.up + str(half))
        start, size = halves(hidden)[half]

        def columns(k):
            here = pl.ds(pl.multiple_of(start + k * 256, 256), 256)
            normed_two = r.normed_two[...]
            gate = dot(normed_two, r.all_gate[..., here].reshape(width, 256), NN)
            line = dot(normed_two, r.all_up[..., here].reshape(width, 256), NN)
            r.up_gate[:, here] = gate
            r.up_lin[:, here] = line
            r.activated[:, here] = (gate * jax.nn.sigmoid(gate) * line).astype(bf16)

        loop(size // 256, columns)

    def down_grad(half):
        if half > 0:
            scatter.release(half - 1)
        start, size = halves(width)[half]
        target = r.down_grad
        count = 2 if sizes[0] % 2 == 0 else 1
        some, wide = sizes[0] // count, hidden // count
        for k in range(count):
            left = r.activated[:, k * wide : (k + 1) * wide]

            def columns(m, left=left, k=k):
                made = dot(left, r.grad_b[:, pl.ds(pl.multiple_of(start + m * 256, 256), 256)], TN)
                shaped = made.reshape((some,) + target.shape[1:5] + (256,))
                target[k * some : (k + 1) * some, :, :, :, :, tile(m, 256)] = shaped.astype(bf16)

            loop(size // 256, columns)
        scatter.begin(half)

    down = r.all_down

    def act():
        need(N.down0, N.down1)
        count = 2 if sizes[0] % 2 == 0 else 1
        some, wide = down.shape[0] // count, hidden // count
        for k in range(count):
            for start, size in halves(width):
                along = slice(start, start + size)
                panel = down[k * some : (k + 1) * some, :, :, :, :, along].reshape(wide, size)
                made = dot(r.grad_b[:, along], panel, NT)
                r.act_grad[...] = made if start == 0 else r.act_grad[...] + made

            def finish(m, k=k):
                here = pl.ds(pl.multiple_of(k * wide + m * 128, 128), 128)
                grad, gate, line = r.act_grad[:, tile(m, 128)], r.up_gate[:, here], r.up_lin[:, here]
                sig = jax.nn.sigmoid(gate)
                r.gate_grad[:, here] = (grad * line * sig * (1.0 + gate * (1.0 - sig))).astype(bf16)
                r.lin_grad[:, here] = (grad * gate * sig).astype(bf16)

            loop(wide // 128, finish)

    def block():
        def columns(k):
            here = tile(k, 256)
            r.middle[:, here] = r.middle[:, here] + dot(
                r.activated[...], down[..., here].reshape(hidden, 256), NN
            )

        loop(width // 256, columns)
        save(N.middle)

    def feed_back():
        save(N.gate_grad, N.lin_grad)
        part = width // sizes[0]

        def features(a):
            here = tile(a, part)
            r.normed_two_grad[:, here] = dot(
                r.gate_grad[...], r.all_gate[a].reshape(part, hidden), NT
            ) + dot(r.lin_grad[...], r.all_up[a].reshape(part, hidden), NT)

        loop(sizes[0], features)
        side = r.side
        side[...] = jnp.zeros_like(side)

        def some(k):
            rows = tile(k, 32)
            before = r.middle[rows, :]
            scale = lax.rsqrt(jnp.mean(before * before, axis=-1, keepdims=True) + epsilon)
            plain = before * scale
            grad = r.normed_two_grad[rows, :]
            side[1:2, :] = side[1:2, :] + jnp.sum(grad * plain, axis=0, keepdims=True)
            grad = grad * vectors[1:2, :]
            whole = r.cotangent[rows, :] + scale * (
                grad - plain * jnp.mean(grad * plain, axis=-1, keepdims=True)
            )
            r.normed_two_grad[rows, :] = whole
            r.middle_b[rows, :] = whole.astype(bf16)

        loop(count_rows // 32, some)
        save(N.normed_two_grad, N.middle_b)

    def heads_back():
        side = r.side
        gain = vectors[3:4, 0:VALUE_DIM]
        part = values // sizes[0]
        for h in range(HEADS):
            across, along = head_slices(h)
            first, count = h * VALUE_DIM // part, max(VALUE_DIM // part, 1)
            weight = r.all_output[first : first + count].reshape(count * part, width)
            r.act_grad[:, 0:VALUE_DIM] = dot(r.middle_b[...], weight, NT)

            def some(k, along=along):
                rows = tile(k, GROUP)
                whole, gate = r.mixed[rows, along], r.gate_pre[rows, along]
                grad = r.act_grad[rows, 0:VALUE_DIM]
                scale = lax.rsqrt(jnp.mean(whole * whole, axis=-1, keepdims=True) + epsilon)
                sig = jax.nn.sigmoid(gate)
                plain = whole * scale
                through = grad * (gate * sig)
                side[3:4, 0:VALUE_DIM] = side[3:4, 0:VALUE_DIM] + jnp.sum(
                    through * plain, axis=0, keepdims=True
                )
                back = through * gain
                r.mixed_grad[rows, along] = (
                    scale * (back - plain * jnp.mean(back * plain, axis=-1, keepdims=True))
                ).astype(bf16)
                r.outgate_grad[rows, along] = (
                    grad * plain * gain * sig * (1.0 + gate * (1.0 - sig))
                ).astype(bf16)

            loop(groups, some)
        save(N.mixed_grad, N.outgate_grad, N.side)

    pieces = dict(
        unpack=unpack,
        norm=norm,
        decay=decay,
        query=lambda: project(N.query, r.query),
        key=lambda: project(N.key, r.key),
        value=lambda: project(N.value, r.value),
        attention=attention,
        outgate=lambda: project(N.outgate, r.gate_pre),
        heads=heads,
        middle=middle,
        up0=lambda: up(0),
        up1=lambda: up(1),
        down_grad0=lambda: down_grad(0),
        down_grad1=lambda: down_grad(1),
        act=act,
        block=block,
        feed_back=feed_back,
        heads_back=heads_back,
    )
    run_plan(
        FORWARD_PLAN,
        pieces,
        scan,
        lambda item, step: gather.advance(item, step),
        lambda item, step: scatter.advance(item, step),
    )
    scatter.finish()
    save(N.near_down0, N.near_down1)
    gather.finish()
    scan.finish()
    for copy in saved:
        copy.wait()


def run_plan(plan, pieces, scan, gather, scatter):
    hops = len(scan.hops)
    steps = list(pieces.values())
    for code in plan:
        if code >= 1000:
            (gather if code < 2000 else scatter)(code % 1000 // 10, code % 10)
        elif code < 100:
            steps[code]()
        elif code == 300:
            for k in range(3, hops):
                scan.send(k)
                scan.receive(k)
        elif code % 100 < hops:
            (scan.send if code < 200 else scan.receive)(code % 100)


def kernel_call(body, sizes, ins, outs, scratch, collective_id):
    vmem = pl.BlockSpec(memory_space=pltpu.VMEM)
    anywhere = pl.BlockSpec(memory_space=pl.ANY)
    names = list(ins) + list(outs) + list(scratch)
    assert len(set(names)) == len(names)
    results = pl.pallas_call(
        functools.partial(body, sizes, names),
        out_shape=[jax.ShapeDtypeStruct(o[0], o[1]) for o in outs.values()],
        in_specs=[vmem if i[1] else anywhere for i in ins.values()],
        out_specs=[vmem if o[2] else anywhere for o in outs.values()],
        scratch_shapes=list(scratch.values()),
        compiler_params=pltpu.CompilerParams(
            collective_id=collective_id, has_side_effects=True, vmem_limit_bytes=VMEM_LIMIT
        ),
    )(*(i[0] for i in ins.values()))
    return dict(zip(outs, results))


LANDINGS = {3: N.near_, 2: N.half_, 1: N.part_, 0: N.last_}


def landings(sizes, block, dtype, name, late, steps):
    order = orders_of(sizes, late)[0]
    made = {}
    for step in steps:
        lead = tuple(sizes[k] for k in order[:step])
        lead = sizes[:3] if step == 3 else (max(sizes[order[step]] - 1, 1),) + lead
        made[LANDINGS[step] + name] = pltpu.VMEM(lead + block, dtype)
    return made


def forward(sizes, tokens, cotangent, small, weights):
    rows, width = tokens.shape
    keys, values = HEADS * KEY_DIM, HEADS * VALUE_DIM
    hidden = weights[N.gate].shape[1]
    groups = rows // GROUP
    most = max(max(sizes) - 1, 1)
    mine = weights[N.query].shape[0]
    ins = {N.in_tokens: (tokens, False), N.in_cotangent: (cotangent, False)}
    ins.update({name: (a, True) for name, a in small.items()})
    ins.update({N.w_ + name: (a, name == N.decay_down) for name, a in weights.items()})
    shape_of = {name: sizes + a.shape for name, a in weights.items()}
    shape_of[N.decay_down] = sizes + (mine, LANES)
    made = dict(
        vectors=((8, width), f32),
        decay_up=((LANES, keys), bf16),
        normed_t=((width, rows), bf16),
        rank_act=((rows, LANES), bf16),
        decay_pre=((rows, keys), f32),
        query=((rows, keys), bf16),
        key=((rows, keys), bf16),
        value=((rows, values), bf16),
        starts=((groups, HEADS, VALUE_DIM, KEY_DIM), bf16),
        gated_t=((values, rows), bf16),
        normed_two_t=((width, rows), bf16),
        gate_grad=((rows, hidden), bf16),
        lin_grad=((rows, hidden), bf16),
        normed_two_grad=((rows, width), f32),
        middle_b=((rows, width), bf16),
        mixed_grad=((rows, values), bf16),
        outgate_grad=((rows, values), bf16),
        side=((8, width), f32),
        middle=((rows, width), f32),
    )
    for k, (_, size) in enumerate(halves(width)):
        made[N.near_down + str(k)] = (sizes[:3] + (weights[N.down].shape[0], size), bf16)
    outs = {N.out_weight_ + name: (shape_of[name], bf16, False) for name in KEPT}
    outs.update({N.out_ + name: o + (False,) for name, o in made.items()})
    scratch = {N.all_ + name: pltpu.VMEM(shape_of[name], bf16) for name in WEIGHTS}
    shared = (N.mixed_grad, N.outgate_grad, N.middle_b)
    scratch.update({name: pltpu.VMEM(*o) for name, o in made.items() if name not in shared})
    scratch.update(
        tokens=pltpu.VMEM((rows, width), tokens.dtype),
        cotangent=pltpu.VMEM((rows, width), f32),
        input_sem=pltpu.SemaphoreType.DMA((2,)),
        tiny_mine=pltpu.VMEM((RANK, LANES), f32),
        tiny_all=pltpu.VMEM(sizes + (RANK, LANES), f32),
        down_mine=pltpu.VMEM((mine, LANES), bf16),
        grad_b=pltpu.VMEM((rows, width), bf16),
        normed=pltpu.VMEM((rows, width), bf16),
        gated=pltpu.VMEM((rows, values), bf16),
        normed_two=pltpu.VMEM((rows, width), bf16),
        gate_pre=pltpu.VMEM((rows, values), f32),
        query_dev=pltpu.VMEM((rows, keys), f32),
        offsets=pltpu.VMEM((groups, 8, keys), f32),
        mixed=pltpu.VMEM((rows, values), f32),
        up_gate=pltpu.VMEM((rows, hidden), f32),
        up_lin=pltpu.VMEM((rows, hidden), f32),
        activated=pltpu.VMEM((rows, hidden), bf16),
        act_grad=pltpu.VMEM((rows, hidden // (2 if sizes[0] % 2 == 0 else 1)), f32),
        down_grad=pltpu.VMEM(sizes + (weights[N.down].shape[0], halves(width)[0][1]), bf16),
        send_sem=pltpu.SemaphoreType.DMA((13, 4, most)),
        recv_sem=pltpu.SemaphoreType.DMA((13, 4, most)),
        own_sem=pltpu.SemaphoreType.DMA((13,)),
        save_sem=pltpu.SemaphoreType.DMA((len(made) + len(KEPT),)),
        back_send_sem=pltpu.SemaphoreType.DMA((2, 4, most)),
        back_recv_sem=pltpu.SemaphoreType.DMA((2, 4, most)),
    )
    for k, (_, size) in enumerate(halves(width)):
        block = (weights[N.down].shape[0], size)
        scratch.update(landings(sizes, block, bf16, N.down + str(k), False, (2,)))
    scratch.update(scan_scratch(sizes))
    results = kernel_call(forward_kernel, sizes, ins, outs, scratch, 0)
    return {name[4:]: a for name, a in results.items()}


LATE_SCATTERED = (N.decay_down,)
BACKWARD_PLAN = (
    0, 100, 2, 3, 6, 2001, 7, 2023, 4, 2033, 5, 2011, 2063, 2073, 2000, 200,
    2043, 2022, 101, 2053, 2010, 2032, 201, 102, 2021, 2062, 2031, 202, 2072, 300, 1, 2061,
    2020, 2071, 10, 8, 9, 11, 12, 2030, 2042, 2083, 2093, 2103, 2113, 2060, 2070, 2052,
    13, 2123, 2112, 2041, 2082, 2092, 2051, 2040, 2102, 2081, 2122, 2111, 2050, 2091, 2101, 2121,
    2110, 2080, 2090, 2100, 2120,
)
NORMED_BACK = (
    (N.decay_down, N.rank_grad),
    (N.query, N.query_grad),
    (N.key, N.key_grad),
    (N.value, N.value_grad),
    (N.outgate, N.outgate_grad),
)
LOADED = (
    N.query,
    N.decay_pre,
    N.mixed_grad,
    N.vectors,
    N.normed_two_t,
    N.gate_grad,
    N.lin_grad,
    N.gated_t,
    N.middle_b,
    N.normed_t,
    N.outgate_grad,
    N.key,
    N.value,
    N.starts,
    N.decay_up,
    N.rank_act,
    N.side,
    N.tokens,
)


def scatter_items(hidden, width):
    keys, values = HEADS * KEY_DIM, HEADS * VALUE_DIM
    items = {}
    for k, (start, size) in enumerate(halves(width)):
        items[N.down + str(k)] = (size, None, N.down, start)
    for k, (start, size) in enumerate(halves(hidden)):
        items[N.gate + str(k)] = (size, N.panel + str(k), N.gate, start)
    for k, (start, size) in enumerate(halves(hidden)):
        items[N.up + str(k)] = (size, N.panel + str(k), N.up, start)
    items[N.output] = (width, N.square0, N.output, 0)
    items[N.outgate] = (values, N.square1, N.outgate, 0)
    items[N.value] = (values, N.square0, N.value, 0)
    items[N.query] = (keys, N.query, N.query, 0)
    items[N.key] = (keys, N.key, N.key, 0)
    items[N.decay_down] = (LANES, N.decay_down, N.decay_down, 0)
    items[N.tiny] = (LANES, N.tiny, N.tiny, 0)
    return items


def backward_kernel(sizes, names, *refs):
    r = SimpleNamespace(**dict(zip(names, refs)))
    at = coords_of(sizes)
    devices = sizes[0] * sizes[1] * sizes[2] * sizes[3]
    count_rows, width = r.tokens.shape
    keys, values = HEADS * KEY_DIM, HEADS * VALUE_DIM
    hidden = r.gate_grad.shape[1]
    groups = count_rows // GROUP
    part = width // sizes[0]
    vectors, rows_sum = r.vectors, r.rows_sum
    per_feature, per_key, per_value = width // devices, keys // devices, VALUE_DIM // devices

    loads = {}
    for name in LOADED:
        loads[name] = pltpu.make_async_copy(
            getattr(r, N.in_ + name), getattr(r, name), r.load_sem.at[len(loads)]
        )
        loads[name].start()
    middle_load = pltpu.make_async_copy(
        r.in_normed_two_grad, r.input_grad, r.load_sem.at[len(loads)]
    )
    middle_load.start()
    result = pltpu.make_async_copy(
        r.input_grad, r.out_input_grad, r.out_sem.at[r.out_sem.shape[0] - 1]
    )

    def ready(*names_of):
        for name in names_of:
            if name in loads:
                loads.pop(name).wait()

    greet(sizes, at)
    items = scatter_items(hidden, width)
    index = {name: k for k, name in enumerate(items)}
    sources, sums, outs = {}, {}, {}
    for name, (size, slot, out, start) in items.items():
        k = index[name]
        if slot is not None:
            sources[k] = Item(getattr(r, N.slot_ + slot), 0, size)
        sums[k] = Item(getattr(r, N.sum_ + out), start, size)
        outs[k] = Item(getattr(r, N.out_ + out), start, size)
    scatter = Scatter(
        sizes,
        at,
        sources,
        {
            step: [getattr(r, kind + name, None) for name in items]
            for step, kind in LANDINGS.items()
        },
        sums,
        outs,
        (r.send_sem, r.recv_sem, r.own_sem, r.out_sem),
        {index[name] for name in LATE_SCATTERED},
    )
    for k in range(2):
        scatter.resume(index[N.down + str(k)], getattr(r, N.in_near_down + str(k)))
    scan = scan_of(sizes, True, r)
    in_slot = {}

    def take_slot(name):
        slot = items[name][1]
        if slot in in_slot:
            scatter.release(index[in_slot[slot]])
        in_slot[slot] = name
        return getattr(r, N.slot_ + slot)

    lower = lower_mask()

    def weight_grad(name, left, right, start=0):
        ready(left, right)
        target, columns_of = take_slot(name), items[name][0]
        size = min(columns_of, 256)

        def columns(k):
            here = pl.ds(pl.multiple_of(start + k * size, size), size)
            made = dot(getattr(r, left)[...], getattr(r, right)[:, here], NN)
            target[..., tile(k, size)] = made.reshape(target.shape[:5] + (size,)).astype(bf16)

        loop(columns_of // size, columns)
        scatter.begin(index[name])

    def begin_state():
        total, state, query_dev = r.total, r.state, r.query_grad
        rows_sum[...] = jnp.zeros_like(rows_sum)
        total[...] = jnp.zeros_like(total)
        ready(N.query, N.decay_pre, N.mixed_grad, N.vectors)

        def some(k):
            rows = tile(k, GROUP)
            cumulative = dot(lower, log_decay_of(r.decay_pre[rows, :]), NN, highest)
            r.cumulative[rows, :] = cumulative
            query_scaled = r.query[rows, :].astype(f32) * key_scale
            query_dev[rows, :] = (query_scaled * jnp.exp(cumulative + total[0:1, :])).astype(bf16)
            total[...] = total[...] + cumulative[GROUP - 1 :]

        loop(groups, some)
        for h in range(HEADS):
            across, along = head_slices(h)
            state[h] = dot(r.mixed_grad[:, along], query_dev[:, across], TN)
        total[...] = jnp.exp(total[...])

    def attention():
        ready(N.key, N.value, N.starts)
        after_state = r.before_state

        def group(k):
            g = groups - 1 - k
            rows = tile(g, GROUP)
            cumulative = r.cumulative[rows, :]
            middle = cumulative[GROUP // 2 - 1 : GROUP // 2]
            ending = cumulative[GROUP - 1 :]
            query_scaled = r.query[rows, :].astype(f32) * key_scale
            key_full = r.key[rows, :].astype(f32)
            from_middle, to_middle = jnp.exp(cumulative - middle), jnp.exp(middle - cumulative)
            to_end, from_start = jnp.exp(ending - cumulative), jnp.exp(cumulative)
            decay_end = jnp.exp(ending)
            gated_query = (query_scaled * from_middle).astype(bf16)
            inverse_key = (key_full * to_middle).astype(bf16)
            tail_key = (key_full * to_end).astype(bf16)
            state_query = (query_scaled * from_start).astype(bf16)
            grad_cumul, through_end = [], []
            for h in range(HEADS):
                across, along = head_slices(h)
                start_b, after = r.starts[g, h], after_state[h]
                start, after_b = start_b.astype(f32), after.astype(bf16)
                grad_out = r.mixed_grad[rows, along]
                value_b = r.value[rows, along]
                query_h, key_h, tail_h = (
                    gated_query[:, across],
                    inverse_key[:, across],
                    tail_key[:, across],
                )
                scores = (dot(query_h, key_h, NT) * lower).astype(bf16)
                grad_scores = (dot(grad_out, value_b, NT) * lower).astype(bf16)
                to_query = from_start[:, across] * dot(grad_out, start_b, NN)
                to_query = to_query + from_middle[:, across] * dot(grad_scores, key_h, NN)
                to_key = to_middle[:, across] * dot(grad_scores, query_h, TN)
                to_key = to_key + to_end[:, across] * dot(value_b, after_b, NN)
                to_value = dot(scores, grad_out, TN) + dot(tail_h, after_b, NT)
                end_state = decay_end[:, across] * start + dot(value_b, tail_h, TN)
                through_end.append(jnp.sum(end_state * after, axis=0, keepdims=True))
                grad_cumul.append(
                    query_scaled[:, across] * to_query - key_full[:, across] * to_key
                )
                after_state[h] = decay_end[:, across] * after + dot(
                    grad_out, state_query[:, across], TN
                )
                r.query_grad[rows, across] = (to_query * key_scale).astype(bf16)
                r.key_grad[rows, across] = to_key.astype(bf16)
                r.value_grad[rows, along] = to_value.astype(bf16)
            log_grad = dot(lower, jnp.concatenate(grad_cumul, axis=1), TN, highest)
            log_grad = log_grad + jnp.concatenate(through_end, axis=1)
            to_decay = log_grad * jax.nn.sigmoid(-r.decay_pre[rows, :]) * (1.0 / 16.0)
            rows_sum[2:3, 0:keys] = rows_sum[2:3, 0:keys] + jnp.sum(
                to_decay, axis=0, keepdims=True
            )
            r.decay_grad[rows, :] = to_decay.astype(bf16)

        loop(groups, group)

    def decay_down():
        ready(N.decay_up)
        r.rank_grad[...] = dot(r.decay_grad[...], r.decay_up[...], NT).astype(bf16)
        weight_grad(N.decay_down, N.normed_t, N.rank_grad)

    def input_grad():
        def panel(a, slot):
            return [
                pltpu.make_async_copy(
                    getattr(r, N.in_weight_ + name).at[a],
                    getattr(r, N.panel_ + name).at[slot],
                    r.panel_sem.at[k, slot],
                )
                for k, (name, _) in enumerate(NORMED_BACK)
            ]

        for a in range(min(2, sizes[0])):
            for copy in panel(a, a):
                copy.start()

        def features(a):
            slot = lax.rem(a, 2)
            for copy in panel(a, slot):
                copy.wait()
            made = None
            for name, grad in NORMED_BACK:
                weight = getattr(r, N.panel_ + name).at[slot]
                term = dot(getattr(r, grad)[...], weight[...].reshape(part, weight.shape[-1]), NT)
                made = term if made is None else made + term
            r.normed_grad[:, tile(a, part)] = made

            @pl.when(a + 2 < sizes[0])
            def _():
                for copy in panel(a + 2, slot):
                    copy.start()

        loop(sizes[0], features)
        middle_load.wait()
        ready(N.tokens)

        def some(k):
            rows = tile(k, 32)
            before = r.tokens[rows, :].astype(f32)
            scale = lax.rsqrt(jnp.mean(before * before, axis=-1, keepdims=True) + epsilon)
            plain = before * scale
            grad = r.normed_grad[rows, :]
            rows_sum[0:1, :] = rows_sum[0:1, :] + jnp.sum(grad * plain, axis=0, keepdims=True)
            grad = grad * vectors[0:1, :]
            r.input_grad[rows, :] = r.input_grad[rows, :] + scale * (
                grad - plain * jnp.mean(grad * plain, axis=-1, keepdims=True)
            )

        loop(count_rows // 32, some)
        result.start()

    def tiny():
        ready(N.rank_act, N.side)
        side = r.side
        decay_up_grad = dot(r.rank_act[...], r.decay_grad[...], TN)[0:RANK]
        row = lax.broadcasted_iota(jnp.int32, (RANK, LANES), 0)
        lane = lax.broadcasted_iota(jnp.int32, (RANK, LANES), 1)
        vectors_of = (
            (rows_sum[0:1, :], per_feature),
            (side[1:2, :], per_feature),
            (rows_sum[2:3, 0:keys], per_key),
            (side[3:4, 0:VALUE_DIM], per_value),
        )

        def cut(values_of, device, per, offset):
            group, first = divmod(device * per, LANES)
            piece = values_of[:, group * LANES : (group + 1) * LANES]
            return pltpu.roll(piece, (offset - first) % LANES, 1)

        target = take_slot(N.tiny)
        for device in range(devices):
            whole = jnp.where(lane < per_key, cut(decay_up_grad, device, per_key, 0), 0.0)
            for k, (vector, per) in enumerate(vectors_of):
                wide = jnp.broadcast_to(vector, (RANK, vector.shape[1]))
                here = (row == k) & (lane >= VECTORS) & (lane < VECTORS + per)
                whole = jnp.where(here, cut(wide, device, per, VECTORS), whole)
            target[place_of(sizes, device)] = whole
        scatter.begin(index[N.tiny])

    first = halves(hidden)[1][0]
    pieces = dict(
        state=begin_state,
        attention=attention,
        gate0=lambda: weight_grad(N.gate0, N.normed_two_t, N.gate_grad),
        gate1=lambda: weight_grad(N.gate1, N.normed_two_t, N.gate_grad, first),
        up0=lambda: weight_grad(N.up0, N.normed_two_t, N.lin_grad),
        up1=lambda: weight_grad(N.up1, N.normed_two_t, N.lin_grad, first),
        output=lambda: weight_grad(N.output, N.gated_t, N.middle_b),
        outgate=lambda: weight_grad(N.outgate, N.normed_t, N.outgate_grad),
        query=lambda: weight_grad(N.query, N.normed_t, N.query_grad),
        key=lambda: weight_grad(N.key, N.normed_t, N.key_grad),
        value=lambda: weight_grad(N.value, N.normed_t, N.value_grad),
        decay_down=decay_down,
        input_grad=input_grad,
        tiny=tiny,
    )
    run_plan(
        BACKWARD_PLAN,
        pieces,
        scan,
        None,
        lambda item, step: scatter.advance(item, step),
    )
    scatter.finish()
    scan.finish()
    ready(*list(loads))
    result.wait()


def backward(sizes, tokens, saved):
    outer, inner, side, core = sizes
    devices = outer * inner * side * core
    most = max(max(sizes) - 1, 1)
    rows, width = tokens.shape
    hidden = saved[N.gate_grad].shape[1]
    keys, values = HEADS * KEY_DIM, HEADS * VALUE_DIM
    mine = width // devices
    saved = dict(saved, tokens=tokens)
    ins = {N.in_ + name: (saved[name], False) for name in LOADED}
    ins[N.in_normed_two_grad] = (saved[N.normed_two_grad], False)
    for k in range(2):
        ins[N.in_near_down + str(k)] = (saved[N.near_down + str(k)], False)
    ins.update({N.in_weight_ + name: (saved[N.weight_ + name], False) for name in KEPT})
    items = scatter_items(hidden, width)
    block, scratch, sums = {}, {}, {}
    for name, (size, slot, out, start) in items.items():
        rows_of = RANK if out == N.tiny else mine
        if slot is None:
            rows_of = saved[N.near_down0].shape[3]
        dtype = f32 if out == N.tiny else bf16
        block = (rows_of, size)
        sums[N.out_ + out] = ((rows_of, start + size), f32, False)
        scratch[N.sum_ + out] = pltpu.VMEM((rows_of, start + size), f32)
        if slot is not None and N.slot_ + slot not in scratch:
            scratch[N.slot_ + slot] = pltpu.VMEM(sizes + block, dtype)
        steps = (3, 1, 0) if slot is None else (3, 2, 1, 0)
        scratch.update(landings(sizes, block, dtype, name, name in LATE_SCATTERED, steps))
    scratch.update({n: pltpu.VMEM(saved[n].shape, saved[n].dtype) for n in LOADED})
    scratch.update(
        {
            N.panel_ + n: pltpu.VMEM((2,) + saved[N.weight_ + n].shape[1:], bf16)
            for n, _ in NORMED_BACK
        }
    )
    scratch.update(
        rows_sum=pltpu.VMEM((8, width), f32),
        cumulative=pltpu.VMEM((rows, keys), f32),
        query_grad=pltpu.VMEM((rows, keys), bf16),
        key_grad=pltpu.VMEM((rows, keys), bf16),
        value_grad=pltpu.VMEM((rows, values), bf16),
        decay_grad=pltpu.VMEM((rows, keys), bf16),
        rank_grad=pltpu.VMEM((rows, LANES), bf16),
        normed_grad=pltpu.VMEM((rows, width), f32),
        send_sem=pltpu.SemaphoreType.DMA((len(items), 4, most)),
        recv_sem=pltpu.SemaphoreType.DMA((len(items), 4, most)),
        input_grad=pltpu.VMEM((rows, width), f32),
        own_sem=pltpu.SemaphoreType.DMA((2,)),
        out_sem=pltpu.SemaphoreType.DMA((len(items) + 1,)),
        load_sem=pltpu.SemaphoreType.DMA((len(LOADED) + 1,)),
        panel_sem=pltpu.SemaphoreType.DMA((len(NORMED_BACK), 2)),
    )
    scratch.update(scan_scratch(sizes))
    outs = dict(sums, out_input_grad=((rows, width), f32, False))
    return kernel_call(backward_kernel, sizes, ins, outs, scratch, 1)


def hand_out_kernel(count, cuts, *refs):
    whole, down, tiny = refs[:count], refs[count], refs[count + 1]
    refs = refs[count + 2 :]
    outs, small, held, sems = refs[:count], refs[count : -count - 1], refs[-count - 1 : -1], refs[-1]
    loads, copies = [], []
    for k in range(count):
        loads.append(pltpu.make_async_copy(whole[k], held[k], sems.at[0, k]))
        loads[-1].start()
        copies.append(pltpu.make_async_copy(held[k], outs[k], sems.at[1, k]))
    small[0][...] = turned(down[...], highest)[0 : small[0].shape[0]]
    for target, (row, column) in zip(small[1:], cuts):
        target[...] = tiny[row : row + target.shape[0], column : column + target.shape[1]]
    for load, copy in zip(loads, copies):
        load.wait()
        copy.start()
    for copy in copies:
        copy.wait()


def hand_out(arrays, decay_down, tiny, cuts):
    vmem = pl.BlockSpec(memory_space=pltpu.VMEM)
    anywhere = pl.BlockSpec(memory_space=pl.ANY)
    shapes = [a.shape for a in arrays] + [(RANK, decay_down.shape[0])] + [c[0] for c in cuts]
    return pl.pallas_call(
        functools.partial(hand_out_kernel, len(arrays), [c[1] for c in cuts]),
        out_shape=[jax.ShapeDtypeStruct(s, f32) for s in shapes],
        in_specs=[anywhere] * len(arrays) + [vmem] * 2,
        out_specs=[anywhere] * len(arrays) + [vmem] * (len(cuts) + 1),
        scratch_shapes=[pltpu.VMEM(a.shape, f32) for a in arrays]
        + [pltpu.SemaphoreType.DMA((2, len(arrays)))],
        compiler_params=pltpu.CompilerParams(vmem_limit_bytes=VMEM_LIMIT),
    )(*arrays, decay_down, tiny)


def local(
    sizes,
    inputs,
    cotangent,
    mixer_gain,
    feed_gain,
    w_query,
    w_key,
    w_value,
    w_outgate,
    w_decay_down,
    w_decay_up,
    decay_bias,
    head_gain,
    w_output,
    w_gate,
    w_up,
    w_down,
):
    width = inputs.shape[2]
    rows = inputs.shape[0] * inputs.shape[1]
    per_feature, per_key, per_value = (
        mixer_gain.shape[0],
        decay_bias.shape[0],
        head_gain.shape[0],
    )
    tokens = inputs.reshape(rows, width)
    small = dict(
        w_decay_up=w_decay_up,
        mixer_gain=mixer_gain.reshape(1, -1),
        feed_gain=feed_gain.reshape(1, -1),
        decay_bias=decay_bias.reshape(1, -1),
        head_gain=head_gain.reshape(1, -1),
    )
    weights = dict(
        decay_down=w_decay_down.T,
        query=w_query,
        key=w_key,
        value=w_value,
        outgate=w_outgate,
        output=w_output,
        gate=w_gate,
        up=w_up,
        down=w_down,
    )
    saved = forward(sizes, tokens, cotangent.reshape(rows, width), small, weights)
    got = backward(sizes, tokens, saved)
    names = (N.query, N.key, N.value, N.outgate, N.output, N.gate, N.up, N.down)
    handed = hand_out(
        [saved[N.middle], got[N.out_input_grad]]
        + [got[N.out_ + name] for name in names],
        got[N.out_decay_down],
        got[N.out_tiny],
        (
            ((RANK, per_key), (0, 0)),
            ((1, per_feature), (0, VECTORS)),
            ((1, per_feature), (1, VECTORS)),
            ((1, per_key), (2, VECTORS)),
            ((1, per_value), (3, VECTORS)),
        ),
    )
    result, input_grad = (a.reshape(inputs.shape) for a in handed[:2])
    g_query, g_key, g_value, g_outgate, g_output, g_gate, g_up, g_down = handed[2:10]
    decay_down, decay_up = handed[10:12]
    g_mixer, g_feed, g_bias, g_head = (a.reshape(-1) for a in handed[12:])
    return (
        result,
        input_grad,
        g_mixer,
        g_feed,
        g_query,
        g_key,
        g_value,
        g_outgate,
        decay_down.T,
        decay_up,
        g_bias,
        g_head,
        g_output,
        g_gate,
        g_up,
        g_down,
    )


def solution(mesh):
    placed = (
        P("batch", "seq", None),
        P("batch", "seq", None),
        P(("seq", "batch")),
        P(("seq", "batch")),
        P(("seq", "batch"), None),
        P(("seq", "batch"), None),
        P(("seq", "batch"), None),
        P(("seq", "batch"), None),
        P(("seq", "batch"), None),
        P(None, ("seq", "batch")),
        P(("seq", "batch")),
        P(("seq", "batch")),
        P(("seq", "batch"), None),
        P(("seq", "batch"), None),
        P(("seq", "batch"), None),
        P(("seq", "batch"), None),
    )
    return jax.shard_map(
        functools.partial(local, grid_of(mesh.shape)),
        mesh=mesh,
        in_specs=placed,
        out_specs=(
            P("batch", "seq", None),
            P("batch", "seq", None),
            P(("seq", "batch")),
            P(("seq", "batch")),
            P(("seq", "batch"), None),
            P(("seq", "batch"), None),
            P(("seq", "batch"), None),
            P(("seq", "batch"), None),
            P(("seq", "batch"), None),
            P(None, ("seq", "batch")),
            P(("seq", "batch")),
            P(("seq", "batch")),
            P(("seq", "batch"), None),
            P(("seq", "batch"), None),
            P(("seq", "batch"), None),
            P(("seq", "batch"), None),
        ),
        check_vma=False,
    )
```

```python
import functools
from types import SimpleNamespace

import jax
import jax.numpy as jnp
from jax import lax
from jax.experimental import pallas as pl
from jax.experimental.pallas import tpu as pltpu
from jax.sharding import PartitionSpec as P

HEADS = 4
KEY_DIM = 128
VALUE_DIM = 256
GROUP = 64
LANES = 128
RANK = 16
VECTORS = 32
MESH = pl.DeviceIdType.MESH
VMEM_LIMIT = 67_000_000


class Names:
    def __getattr__(self, name):
        return name


N = Names()
epsilon = 1e-06
key_scale = KEY_DIM ** (-0.5)
highest = lax.Precision.HIGHEST
high = lax.Precision.HIGH
f32 = jnp.float32
bf16 = jnp.bfloat16


def grid_of(shape):
    seq, batch = shape["seq"], shape["batch"]
    outer = 4 if seq % 4 == 0 else seq
    core = 2 if batch % 2 == 0 else 1
    return (outer, seq // outer, batch // core, core)


def coords_of(sizes):
    seq, batch = lax.axis_index("seq"), lax.axis_index("batch")
    return (seq // sizes[1], seq % sizes[1], batch // sizes[3], batch % sizes[3])


def device_of(sizes, at):
    return {"seq": at[0] * sizes[1] + at[1], "batch": at[2] * sizes[3] + at[3]}


def place_of(sizes, device):
    place = []
    for size in reversed(sizes):
        device, last = divmod(device, size)
        place.insert(0, last)
    return tuple(place)


def moved(sizes, at, axis, by):
    new = list(at)
    new[axis] = lax.rem(at[axis] + (by % sizes[axis]), sizes[axis])
    return tuple(new)


def region(ref, free, at):
    return ref.at[tuple(slice(None) if k in free else at[k] for k in range(4))]


def orders_of(sizes, late=False):
    orders = ((1, 2, 0, 3), (2, 1, 0, 3)) if late else ((0, 1, 2, 3), (0, 2, 1, 3))
    return orders if sizes[1] == sizes[2] and sizes[3] == 2 else orders[:1]


def hops_of(sizes):
    length, hops = sizes[0] * sizes[1], []
    while 2 ** len(hops) < length:
        hops.append(2 ** len(hops))
    return hops


def greet(sizes, at):
    barrier = pltpu.get_barrier_semaphore()
    length = sizes[0] * sizes[1]
    seq, batch = lax.axis_index("seq"), lax.axis_index("batch")
    targets = [
        device_of(sizes, moved(sizes, at, axis, by))
        for axis in range(4)
        for by in range(1, sizes[axis])
    ]
    for hop in hops_of(sizes):
        for by in (hop, length - hop):
            targets.append({"seq": lax.rem(seq + by, length), "batch": batch})
    for target in targets:
        pl.semaphore_signal(barrier, inc=1, device_id=target, device_id_type=MESH)
    pl.semaphore_wait(barrier, len(targets))


def by_order(sizes, at, act, late=False):
    orders = orders_of(sizes, late)
    if len(orders) == 1:
        act(orders[0])
        return
    for parity, order in enumerate(orders):
        pl.when(at[3] == parity)(functools.partial(act, order))


def loop(count, body, together=1):
    together = min(together, count)
    while count % together:
        together -= 1

    def step(k, carry):
        for j in range(together):
            body(k * together + j)
        return carry

    lax.fori_loop(0, count // together, step, 0)


def dot(left, right, dims, precision=None):
    return lax.dot_general(
        left, right, (dims, ((), ())), precision=precision, preferred_element_type=f32
    )


NN = ((1,), (0,))
NT = ((1,), (1,))
TN = ((0,), (0,))


class Item:
    def __init__(self, ref, start=0, size=None):
        self.ref, self.start = ref, start
        self.size = ref.shape[-1] if size is None else size
        self.part = self.size != ref.shape[-1]

    def tail(self):
        return (slice(None), slice(self.start, self.start + self.size)) if self.part else ()

    def at(self, index):
        return self.ref.at[tuple(index) + self.tail()]


def blocks_of(free, at, axes=4):
    return tuple(slice(None) if k in free else at[k] for k in range(axes))


class Gather:
    def __init__(self, sizes, at, shards, wholes, sems, late):
        self.sizes, self.at, self.late = sizes, at, late
        self.shards, self.wholes = shards, wholes
        self.send_sem, self.recv_sem, self.own_sem = sems
        self.done = {item: 0 for item in range(len(shards))}

    def copies(self, item, order, step, arriving):
        axis, free = order[step], order[:step]
        made = []
        for by in range(1, self.sizes[axis]):
            source = moved(self.sizes, self.at, axis, -by) if arriving else self.at
            place = self.wholes[item].at(blocks_of(free, source))
            made.append(
                pltpu.make_async_remote_copy(
                    src_ref=self.shards[item].at(()) if step == 0 and not arriving else place,
                    dst_ref=place,
                    send_sem=self.send_sem.at[item, step, by - 1],
                    recv_sem=self.recv_sem.at[item, step, by - 1],
                    device_id=device_of(self.sizes, moved(self.sizes, self.at, axis, by)),
                    device_id_type=MESH,
                )
            )
        return made

    def own(self, item):
        return pltpu.make_async_copy(
            self.shards[item].at(()),
            self.wholes[item].at(blocks_of((), self.at)),
            self.own_sem.at[item],
        )

    def begin(self, items):
        for item in items:

            def act(order, item=item):
                for copy in self.copies(item, order, 0, False):
                    copy.start()

            if item in self.late:
                by_order(self.sizes, self.at, act, True)
            else:
                act(orders_of(self.sizes)[0])
            self.own(item).start()

    def advance(self, item, step):
        while self.done[item] < step:
            now = self.done[item] = self.done[item] + 1
            if now == 1:
                self.own(item).wait()

            def act(order, now=now):
                for copy in self.copies(item, order, now - 1, True):
                    copy.wait_recv()
                if now < 4:
                    for copy in self.copies(item, order, now, False):
                        copy.start()

            by_order(self.sizes, self.at, act, item in self.late)

    def finish(self):
        for item in self.done:
            self.advance(item, 4)
        for late in (False, True):

            def act(order, late=late):
                for item in self.done:
                    if (item in self.late) == late:
                        for step in range(4):
                            for copy in self.copies(item, order, step, False):
                                copy.wait_send()

            by_order(self.sizes, self.at, act, late)


class Scatter:
    def __init__(self, sizes, at, sources, lands, sums, outs, sems, late, stop=0):
        self.sizes, self.at, self.late, self.stop = sizes, at, late, stop
        self.outs = outs
        self.sources, self.sums = sources, sums
        self.near, self.lands = lands[3], lands
        self.send_sem, self.recv_sem, self.load_sem, self.out_sem = sems
        self.left, self.sent, self.resumed = {}, {}, {}

    def copy(self, item, order, step, by):
        axis, free = order[step], order[:step]
        target = moved(self.sizes, self.at, axis, by)
        if step == 3:
            source = self.sources[item].at(blocks_of(free, target))
            landing = self.near[item]
        else:
            whole = self.resumed[item] if step == 1 and item in self.resumed else self.near[item]
            source = whole.at[blocks_of(free, target, 3)]
            landing = self.lands[step][item].at[by - 1]
        return pltpu.make_async_remote_copy(
            src_ref=source,
            dst_ref=landing,
            send_sem=self.send_sem.at[item, step, by - 1],
            recv_sem=self.recv_sem.at[item, step, by - 1],
            device_id=device_of(self.sizes, target),
            device_id_type=MESH,
        )

    def begin(self, item):
        self.left[item] = 4
        self.sent[item] = {3}
        self.copy(item, orders_of(self.sizes)[0], 3, 1).start()

    def load(self, item):
        return pltpu.make_async_copy(self.resumed[item], self.near[item], self.load_sem.at[item])

    def resume(self, item, far):
        self.left[item] = 2
        self.sent[item] = {1}
        self.resumed[item] = far
        self.load(item).start()

        def act(order):
            for by in range(1, self.sizes[order[1]]):
                self.copy(item, order, 1, by).start()

        by_order(self.sizes, self.at, act, item in self.late)

    def advance(self, item, step):
        while self.left[item] > max(step, self.stop):
            now = self.left[item] = self.left[item] - 1
            more = now > self.stop
            if more:
                self.sent[item].add(now - 1)
            if now == 1 and item in self.resumed:
                self.load(item).wait()

            def act(order, now=now, more=more):
                self.add(item, order, now)
                if more:
                    for by in range(1, self.sizes[order[now - 1]]):
                        self.copy(item, order, now - 1, by).start()

            by_order(self.sizes, self.at, act, item in self.late)
            if now == 0:
                self.out(item).start()

    def out(self, item):
        return pltpu.make_async_copy(
            self.sums[item].at(()), self.outs[item].at(()), self.out_sem.at[item]
        )

    def add(self, item, order, step):
        sizes, at = self.sizes, self.at
        axis, free = order[step], sorted(order[:step])
        near = self.near[item]
        for by in range(1, sizes[axis]):
            self.copy(item, order, step, by).wait_recv()
        if step == 0:
            total = near[at[0], at[1], at[2]].astype(f32)
            for by in range(1, sizes[axis]):
                total = total + self.lands[0][item][by - 1].astype(f32)
            kept = self.sums[item]
            kept.ref[:, kept.start : kept.start + kept.size] = total
            return

        def at_first(k):
            for j in range(sizes[free[1]] if len(free) > 1 else 1):
                for i in range(sizes[free[2]] if len(free) > 2 else 1):
                    within = (k, j, i)[: len(free)]
                    place = list(at[:3])
                    for axis_of, index in zip(free, within):
                        place[axis_of] = index
                    place = tuple(place)
                    total = near[place].astype(f32)
                    if step == 3:
                        source = self.sources[item]
                        mine = source.ref[place + (at[3],) + source.tail()]
                        total = total + mine.astype(f32)
                    else:
                        for by in range(1, sizes[axis]):
                            come = self.lands[step][item].at[by - 1]
                            total = total + come[within].astype(f32)
                    near[place] = total.astype(near.dtype)

        loop(sizes[free[0]], at_first)

    def release(self, item):
        self.advance(item, 3)
        self.sent[item].remove(3)
        self.copy(item, orders_of(self.sizes)[0], 3, 1).wait_send()

    def finish(self):
        for item in self.left:
            self.advance(item, 0)
            if self.stop == 0:
                self.out(item).wait()
        for late in (False, True):

            def act(order, late=late):
                for item in self.left:
                    if (item in self.late) == late:
                        for step in sorted(self.sent[item]):
                            for by in range(1, self.sizes[order[step]]):
                                self.copy(item, order, step, by).wait_send()

            by_order(self.sizes, self.at, act, late)


class Scan:
    def __init__(self, sizes, reverse, total, state, before_total, before_state, buffers, sems):
        self.sizes, self.reverse = sizes, reverse
        self.total, self.state = total, state
        self.before_total, self.before_state = before_total, before_state
        self.total_out, self.total_in, self.state_out, self.state_in = buffers
        self.sems = sems
        self.hops = hops_of(sizes)
        self.length = sizes[0] * sizes[1]
        self.place = self.length - 1 - lax.axis_index("seq") if reverse else lax.axis_index("seq")

    def copies(self, k):
        seq = lax.axis_index("seq")
        hop = self.length - self.hops[k] if self.reverse else self.hops[k]
        target = {"seq": lax.rem(seq + hop, self.length), "batch": lax.axis_index("batch")}
        pairs = ((self.total_out, self.total_in), (self.state_out, self.state_in))
        return [
            pltpu.make_async_remote_copy(
                src_ref=out.at[k],
                dst_ref=come.at[k],
                send_sem=self.sems.at[0, k, n],
                recv_sem=self.sems.at[1, k, n],
                device_id=target,
                device_id_type=MESH,
            )
            for n, (out, come) in enumerate(pairs)
        ]

    def send(self, k):
        if k == 0:
            self.before_total[...] = jnp.ones_like(self.before_total)
            self.before_state[...] = jnp.zeros_like(self.before_state)
        self.total_out[k] = self.total[...]
        for h in range(HEADS):
            self.state_out[k, h] = self.state[h].astype(bf16)

        @pl.when(self.place + self.hops[k] < self.length)
        def _():
            for copy in self.copies(k):
                copy.start()

    def receive(self, k):
        @pl.when(self.place >= self.hops[k])
        def _():
            for copy in self.copies(k):
                copy.wait_recv()
            come = self.total_in[k]
            for h in range(HEADS):
                keys = slice(h * KEY_DIM, (h + 1) * KEY_DIM)
                state = self.state_in[k, h].astype(f32)
                self.before_state[h] = (
                    self.before_state[h] + self.before_total[0:1, keys] * state
                )
                if k + 1 < len(self.hops):
                    self.state[h] = self.state[h] + self.total[0:1, keys] * state
            self.before_total[...] = self.before_total[...] * come
            if k + 1 < len(self.hops):
                self.total[...] = self.total[...] * come

    def finish(self):
        for k in range(len(self.hops)):

            @pl.when(self.place + self.hops[k] < self.length)
            def _(k=k):
                for copy in self.copies(k):
                    copy.wait_send()


def lower_mask():
    rows = lax.broadcasted_iota(jnp.int32, (GROUP, GROUP), 0)
    columns = lax.broadcasted_iota(jnp.int32, (GROUP, GROUP), 1)
    return jnp.where(rows >= columns, 1.0, 0.0).astype(f32)


def log_decay_of(decay_pre):
    return jax.nn.log_sigmoid(decay_pre) * (1.0 / 16.0)


def spread(block, offset, per, width):
    devices = width // per
    lane = lax.broadcasted_iota(jnp.int32, (LANES, width), 0)
    column = lax.broadcasted_iota(jnp.int32, (LANES, width), 1)
    pick = jnp.where(lane == offset + column % per, 1.0, 0.0).astype(bf16)
    wide = dot(block.astype(bf16), pick, NN)
    rows = block.shape[0] // devices
    wide = wide.reshape(devices, rows, width)
    device = lax.broadcasted_iota(jnp.int32, wide.shape, 0)
    column = lax.broadcasted_iota(jnp.int32, wide.shape, 2)
    return jnp.sum(jnp.where(device == column // per, wide, 0.0), axis=0)


def turned(array, precision=None):
    size = array.shape[1]
    rows = lax.broadcasted_iota(jnp.int32, (size, size), 0)
    columns = lax.broadcasted_iota(jnp.int32, (size, size), 1)
    return dot(jnp.where(rows == columns, 1.0, 0.0).astype(array.dtype), array, NT, precision)


def scan_scratch(sizes):
    hops = len(hops_of(sizes))
    keys = HEADS * KEY_DIM
    return dict(
        total=pltpu.VMEM((8, keys), f32),
        state=pltpu.VMEM((HEADS, VALUE_DIM, KEY_DIM), f32),
        before_total=pltpu.VMEM((8, keys), f32),
        before_state=pltpu.VMEM((HEADS, VALUE_DIM, KEY_DIM), f32),
        total_out=pltpu.VMEM((hops, 8, keys), f32),
        total_in=pltpu.VMEM((hops, 8, keys), f32),
        state_out=pltpu.VMEM((hops, HEADS, VALUE_DIM, KEY_DIM), bf16),
        state_in=pltpu.VMEM((hops, HEADS, VALUE_DIM, KEY_DIM), bf16),
        scan_sem=pltpu.SemaphoreType.DMA((2, hops, 2)),
    )


def scan_of(sizes, reverse, r):
    return Scan(
        sizes,
        reverse,
        r.total,
        r.state,
        r.before_total,
        r.before_state,
        (r.total_out, r.total_in, r.state_out, r.state_in),
        r.scan_sem,
    )


def head_slices(h):
    return slice(h * KEY_DIM, (h + 1) * KEY_DIM), slice(h * VALUE_DIM, (h + 1) * VALUE_DIM)


def tile(k, size):
    return pl.ds(pl.multiple_of(k * size, size), size)


def halves(columns):
    first = -(-columns // 512) * 256
    return ((0, first), (first, columns - first))


WEIGHTS = (N.decay_down, N.query, N.key, N.value, N.outgate, N.output, N.gate, N.up, N.down)
KEPT = WEIGHTS[:5]
LATE_GATHERED = (N.down1,)
GATHER_ORDER = (0, 3, 2, 1, 4, 5, 10, 6, 7, 12, 9, 11, 8)
FORWARD_PLAN = (
    1001, 1121, 1031, 1002, 1021, 1011, 1003, 1032, 1022, 1004, 0, 1012, 1, 1041, 1033, 1023,
    1034, 4, 1013, 1051, 1042, 1024, 3, 1014, 2, 1052, 1101, 1043, 1061, 1102, 1044, 5,
    6, 1071, 1062, 1053, 100, 1054, 7, 1103, 1072, 1104, 1063, 200, 101, 1081, 1064, 201,
    102, 1091, 1111, 1073, 1082, 1074, 202, 1122, 300, 8, 1092, 9, 1112, 1083, 1084, 10,
    1093, 1094, 1113, 11, 12, 1123, 2003, 13, 1114, 2013, 1124, 14, 16, 2002, 17, 15,
    2012,
)


def forward_kernel(sizes, names, *refs):
    r = SimpleNamespace(**dict(zip(names, refs)))
    r.mixed_grad, r.outgate_grad, r.middle_b = r.gated, r.normed, r.tokens
    at = coords_of(sizes)
    devices = sizes[0] * sizes[1] * sizes[2] * sizes[3]
    count_rows, width = r.tokens.shape
    keys, values = HEADS * KEY_DIM, HEADS * VALUE_DIM
    hidden = r.up_gate.shape[1]
    groups = count_rows // GROUP
    vectors = r.vectors
    per_feature, per_key, per_value = width // devices, keys // devices, VALUE_DIM // devices

    loads = [
        pltpu.make_async_copy(r.in_tokens, r.tokens, r.input_sem.at[0]),
        pltpu.make_async_copy(r.in_cotangent, r.cotangent, r.input_sem.at[1]),
    ]
    for copy in loads:
        copy.start()
    tiny = r.tiny_mine
    tiny[...] = jnp.zeros_like(tiny)
    tiny[:, 0:per_key] = r.w_decay_up[...].astype(f32)
    for k, name in enumerate((N.mixer_gain, N.feed_gain, N.decay_bias, N.head_gain)):
        vector = getattr(r, name)
        tiny[k : k + 1, VECTORS : VECTORS + vector.shape[1]] = vector[...].astype(f32)
    down_mine = r.down_mine
    down_mine[...] = jnp.zeros_like(down_mine)
    down_mine[:, 0:RANK] = turned(r.w_decay_down[...]).astype(bf16)
    greet(sizes, at)

    shards, wholes, index = [Item(tiny)], [Item(r.tiny_all)], {N.tiny: 0}
    late = set()

    def item(name, shard, whole, start=0, size=None):
        index[name] = len(shards)
        if name in LATE_GATHERED:
            late.add(len(shards))
        shards.append(Item(shard, start, size))
        wholes.append(Item(whole, start, size))

    item(N.decay_down, down_mine, r.all_decay_down)
    for name in (N.query, N.key, N.value, N.outgate, N.output):
        item(name, getattr(r, N.w_ + name), getattr(r, N.all_ + name))
    for k in range(2):
        for name in (N.gate, N.up):
            item(name + str(k), getattr(r, N.w_ + name), getattr(r, N.all_ + name), *halves(hidden)[k])
    for k in range(2):
        item(N.down + str(k), r.w_down, r.all_down, *halves(width)[k])
    gather = Gather(
        sizes, at, shards, wholes, (r.send_sem, r.recv_sem, r.own_sem), late
    )
    gather.begin(GATHER_ORDER)
    scan = scan_of(sizes, False, r)
    saved = []
    scatter = Scatter(
        sizes,
        at,
        [Item(r.down_grad, 0, size) for _, size in halves(width)],
        {3: (r.near_down0, r.near_down1), 2: (r.half_down0, r.half_down1)},
        None,
        None,
        (r.back_send_sem, r.back_recv_sem, None, None),
        (),
        2,
    )

    def save(*names_of):
        for name in names_of:
            source = getattr(r, N.all_ + name[7:]) if name.startswith(N.weight_) else getattr(r, name)
            copy = pltpu.make_async_copy(source, getattr(r, N.out_ + name), r.save_sem.at[len(saved)])
            copy.start()
            saved.append(copy)

    def need(*names_of):
        for name in names_of:
            gather.advance(index[name], 4)

    lower = lower_mask()

    def turn(source, target):
        def columns(k):
            target[tile(k, 256), :] = turned(source[:, tile(k, 256)]).astype(bf16)

        loop(source.shape[1] // 256, columns)

    def unpack():
        need(N.tiny)
        whole = r.tiny_all[...].reshape(devices, RANK, LANES)
        vectors[...] = jnp.zeros_like(vectors)
        vectors[0:1, :] = spread(whole[:, 0], VECTORS, per_feature, width)
        vectors[1:2, :] = spread(whole[:, 1], VECTORS, per_feature, width)
        vectors[2:3, 0:keys] = spread(whole[:, 2], VECTORS, per_key, keys)
        vectors[3:4, 0:VALUE_DIM] = spread(whole[:, 3], VECTORS, per_value, VALUE_DIM)
        decay_up = r.decay_up
        decay_up[...] = jnp.zeros_like(decay_up)
        lane = lax.broadcasted_iota(jnp.int32, (RANK, LANES), 1)
        together = LANES // per_key
        for group in range(keys // LANES):
            joined = jnp.zeros((RANK, LANES), f32)
            for k in range(together):
                block = r.tiny_all[place_of(sizes, group * together + k)]
                here = (lane >= k * per_key) & (lane < (k + 1) * per_key)
                joined = jnp.where(here, pltpu.roll(block, k * per_key, 1), joined)
            decay_up[0:RANK, group * LANES : (group + 1) * LANES] = joined.astype(bf16)
        save(N.vectors, N.decay_up)

    def norm():
        for copy in loads:
            copy.wait()

        def some(k):
            rows = tile(k, 32)
            plain = r.tokens[rows, :].astype(f32)
            scale = lax.rsqrt(jnp.mean(plain * plain, axis=-1, keepdims=True) + epsilon)
            r.normed[rows, :] = (plain * scale * vectors[0:1, :]).astype(bf16)
            r.grad_b[rows, :] = r.cotangent[rows, :].astype(bf16)

        loop(count_rows // 32, some, 4)
        turn(r.normed, r.normed_t)
        save(N.normed_t)

    def project(name, into):
        need(name)
        weight = getattr(r, N.all_ + name)
        size = min(into.shape[1], 256)

        def columns(k):
            here = tile(k, size)
            panel = weight[..., here].reshape(width, size)
            into[:, here] = dot(r.normed[...], panel, NN).astype(into.dtype)

        loop(into.shape[1] // size, columns)
        save(N.weight_ + name)

    def decay():
        project(N.decay_down, r.rank_act)
        r.decay_pre[...] = (
            dot(r.rank_act[...], r.decay_up[...], NN) + vectors[2:3, 0:keys]
        )
        save(N.rank_act, N.decay_pre)

    def attention():
        total, state = r.total, r.state
        total[...] = jnp.zeros_like(total)
        state[...] = jnp.zeros_like(state)

        def group(k):
            rows = tile(k, GROUP)
            cumulative = dot(lower, log_decay_of(r.decay_pre[rows, :]), NN, highest)
            middle = cumulative[GROUP // 2 - 1 : GROUP // 2]
            ending = cumulative[GROUP - 1 :]
            query_scaled = r.query[rows, :].astype(f32) * key_scale
            key_full = r.key[rows, :].astype(f32)
            gated_query = query_scaled * jnp.exp(cumulative - middle)
            inverse_key = key_full * jnp.exp(middle - cumulative)
            tail_key = key_full * jnp.exp(ending - cumulative)
            state_query = query_scaled * jnp.exp(cumulative)
            r.query_dev[rows, :] = state_query * jnp.exp(total[0:1, :])
            r.offsets[k] = total[...]
            for h in range(HEADS):
                across, along = head_slices(h)
                value_full = r.value[rows, along].astype(f32)
                scores = dot(gated_query[:, across], inverse_key[:, across], NT, high) * lower
                start = state[h]
                r.starts[k, h] = start.astype(bf16)
                r.mixed[rows, along] = dot(state_query[:, across], start, NT, high) + dot(
                    scores, value_full, NN, high
                )
                state[h] = jnp.exp(ending[:, across]) * start + dot(
                    value_full, tail_key[:, across], TN, high
                )
            total[...] = total[...] + ending

        loop(groups, group, 2)
        total[...] = jnp.exp(total[...])
        save(N.query, N.key, N.value)

    def heads():
        before = r.before_state

        def some(k):
            rows = tile(k, GROUP)
            factor = jnp.exp(r.offsets[k])
            for h in range(HEADS):
                across, along = head_slices(h)
                begin = r.starts[k, h].astype(f32) + factor[0:1, across] * before[h]
                r.starts[k, h] = begin.astype(bf16)
                whole = r.mixed[rows, along] + dot(
                    r.query_dev[rows, across], before[h], NT, high
                )
                r.mixed[rows, along] = whole
                scale = lax.rsqrt(jnp.mean(whole * whole, axis=-1, keepdims=True) + epsilon)
                gate = r.gate_pre[rows, along]
                swish = gate * jax.nn.sigmoid(gate)
                r.gated[rows, along] = (
                    whole * scale * vectors[3:4, 0:VALUE_DIM] * swish
                ).astype(bf16)

        loop(groups, some, 2)
        turn(r.gated, r.gated_t)
        save(N.starts, N.gated_t)

    def middle():
        need(N.output)

        def columns(k):
            here = tile(k, 256)
            panel = r.all_output[..., here].reshape(values, 256)
            r.middle[:, here] = r.tokens[:, here].astype(f32) + dot(
                r.gated[...], panel, NN
            )

        loop(width // 256, columns)

        def some(k):
            rows = tile(k, 32)
            plain = r.middle[rows, :]
            scale = lax.rsqrt(jnp.mean(plain * plain, axis=-1, keepdims=True) + epsilon)
            r.normed_two[rows, :] = (plain * scale * vectors[1:2, :]).astype(bf16)

        loop(count_rows // 32, some, 4)
        turn(r.normed_two, r.normed_two_t)
        save(N.normed_two_t)

    def up(half):
        need(N.gate + str(half), N.up + str(half))
        start, size = halves(hidden)[half]

        def columns(k):
            here = pl.ds(pl.multiple_of(start + k * 256, 256), 256)
            normed_two = r.normed_two[...]
            gate = dot(normed_two, r.all_gate[..., here].reshape(width, 256), NN)
            line = dot(normed_two, r.all_up[..., here].reshape(width, 256), NN)
            r.up_gate[:, here] = gate
            r.up_lin[:, here] = line
            activated = (gate * jax.nn.sigmoid(gate) * line).astype(bf16)
            r.activated_t[here, :] = turned(activated).astype(bf16)

        loop(size // 256, columns)

    def down_grad(half):
        if half > 0:
            scatter.release(half - 1)
        start, size = halves(width)[half]
        target = r.down_grad
        count = 2 if sizes[0] % 2 == 0 else 1
        some, wide = sizes[0] // count, hidden // count
        for k in range(count):
            left = r.activated_t[k * wide : (k + 1) * wide, :]

            def columns(m, left=left, k=k):
                made = dot(left, r.grad_b[:, pl.ds(pl.multiple_of(start + m * 256, 256), 256)], NN)
                shaped = made.reshape((some,) + target.shape[1:5] + (256,))
                target[k * some : (k + 1) * some, :, :, :, :, tile(m, 256)] = shaped.astype(bf16)

            loop(size // 256, columns)
        scatter.begin(half)

    down = r.all_down

    def act():
        need(N.down0, N.down1)
        count = 2 if sizes[0] % 2 == 0 else 1
        some, wide = down.shape[0] // count, hidden // count
        for k in range(count):
            for start, size in halves(width):
                along = slice(start, start + size)
                panel = down[k * some : (k + 1) * some, :, :, :, :, along].reshape(wide, size)
                made = dot(r.grad_b[:, along], panel, NT)
                r.act_grad[...] = made if start == 0 else r.act_grad[...] + made

            def finish(m, k=k):
                here = pl.ds(pl.multiple_of(k * wide + m * 128, 128), 128)
                grad, gate, line = r.act_grad[:, tile(m, 128)], r.up_gate[:, here], r.up_lin[:, here]
                sig = jax.nn.sigmoid(gate)
                r.gate_grad[:, here] = (grad * line * sig * (1.0 + gate * (1.0 - sig))).astype(bf16)
                r.lin_grad[:, here] = (grad * gate * sig).astype(bf16)

            loop(wide // 128, finish, 2)

    def block():
        def columns(k):
            here = tile(k, 256)
            r.middle[:, here] = r.middle[:, here] + dot(
                r.activated_t[...], down[..., here].reshape(hidden, 256), TN
            )

        loop(width // 256, columns)
        save(N.middle)

    def feed_back():
        save(N.gate_grad, N.lin_grad)
        part = width // sizes[0]

        def features(a):
            here = tile(a, part)
            r.normed_two_grad[:, here] = dot(
                r.gate_grad[...], r.all_gate[a].reshape(part, hidden), NT
            ) + dot(r.lin_grad[...], r.all_up[a].reshape(part, hidden), NT)

        loop(sizes[0], features)
        side = r.side
        side[...] = jnp.zeros_like(side)

        def some(k):
            rows = tile(k, 32)
            before = r.middle[rows, :]
            scale = lax.rsqrt(jnp.mean(before * before, axis=-1, keepdims=True) + epsilon)
            plain = before * scale
            grad = r.normed_two_grad[rows, :]
            side[1:2, :] = side[1:2, :] + jnp.sum(grad * plain, axis=0, keepdims=True)
            grad = grad * vectors[1:2, :]
            whole = r.cotangent[rows, :] + scale * (
                grad - plain * jnp.mean(grad * plain, axis=-1, keepdims=True)
            )
            r.normed_two_grad[rows, :] = whole
            r.middle_b[rows, :] = whole.astype(bf16)

        loop(count_rows // 32, some, 4)
        save(N.normed_two_grad, N.middle_b)

    def heads_back():
        side = r.side
        gain = vectors[3:4, 0:VALUE_DIM]
        part = values // sizes[0]
        for h in range(HEADS):
            across, along = head_slices(h)
            first, count = h * VALUE_DIM // part, max(VALUE_DIM // part, 1)
            weight = r.all_output[first : first + count].reshape(count * part, width)
            r.act_grad[:, 0:VALUE_DIM] = dot(r.middle_b[...], weight, NT)

            def some(k, along=along):
                rows = tile(k, GROUP)
                whole, gate = r.mixed[rows, along], r.gate_pre[rows, along]
                grad = r.act_grad[rows, 0:VALUE_DIM]
                scale = lax.rsqrt(jnp.mean(whole * whole, axis=-1, keepdims=True) + epsilon)
                sig = jax.nn.sigmoid(gate)
                plain = whole * scale
                through = grad * (gate * sig)
                side[3:4, 0:VALUE_DIM] = side[3:4, 0:VALUE_DIM] + jnp.sum(
                    through * plain, axis=0, keepdims=True
                )
                back = through * gain
                r.mixed_grad[rows, along] = (
                    scale * (back - plain * jnp.mean(back * plain, axis=-1, keepdims=True))
                ).astype(bf16)
                r.outgate_grad[rows, along] = (
                    grad * plain * gain * sig * (1.0 + gate * (1.0 - sig))
                ).astype(bf16)

            loop(groups, some, 4)
        save(N.mixed_grad, N.outgate_grad, N.side)

    pieces = dict(
        unpack=unpack,
        norm=norm,
        decay=decay,
        query=lambda: project(N.query, r.query),
        key=lambda: project(N.key, r.key),
        value=lambda: project(N.value, r.value),
        attention=attention,
        outgate=lambda: project(N.outgate, r.gate_pre),
        heads=heads,
        middle=middle,
        up0=lambda: up(0),
        up1=lambda: up(1),
        down_grad0=lambda: down_grad(0),
        down_grad1=lambda: down_grad(1),
        act=act,
        block=block,
        feed_back=feed_back,
        heads_back=heads_back,
    )
    run_plan(
        FORWARD_PLAN,
        pieces,
        scan,
        lambda item, step: gather.advance(item, step),
        lambda item, step: scatter.advance(item, step),
    )
    scatter.finish()
    save(N.near_down0, N.near_down1)
    gather.finish()
    scan.finish()
    for copy in saved:
        copy.wait()


def run_plan(plan, pieces, scan, gather, scatter):
    hops = len(scan.hops)
    steps = list(pieces.values())
    for code in plan:
        if code >= 1000:
            (gather if code < 2000 else scatter)(code % 1000 // 10, code % 10)
        elif code < 100:
            steps[code]()
        elif code == 300:
            for k in range(3, hops):
                scan.send(k)
                scan.receive(k)
        elif code % 100 < hops:
            (scan.send if code < 200 else scan.receive)(code % 100)


def kernel_call(body, sizes, ins, outs, scratch, collective_id):
    vmem = pl.BlockSpec(memory_space=pltpu.VMEM)
    anywhere = pl.BlockSpec(memory_space=pl.ANY)
    names = list(ins) + list(outs) + list(scratch)
    assert len(set(names)) == len(names)
    results = pl.pallas_call(
        functools.partial(body, sizes, names),
        out_shape=[jax.ShapeDtypeStruct(o[0], o[1]) for o in outs.values()],
        in_specs=[vmem if i[1] else anywhere for i in ins.values()],
        out_specs=[vmem if o[2] else anywhere for o in outs.values()],
        scratch_shapes=list(scratch.values()),
        compiler_params=pltpu.CompilerParams(
            collective_id=collective_id, has_side_effects=True, vmem_limit_bytes=VMEM_LIMIT
        ),
    )(*(i[0] for i in ins.values()))
    return dict(zip(outs, results))


LANDINGS = {3: N.near_, 2: N.half_, 1: N.part_, 0: N.last_}


def landings(sizes, block, dtype, name, late, steps):
    order = orders_of(sizes, late)[0]
    made = {}
    for step in steps:
        lead = tuple(sizes[k] for k in order[:step])
        lead = sizes[:3] if step == 3 else (max(sizes[order[step]] - 1, 1),) + lead
        made[LANDINGS[step] + name] = pltpu.VMEM(lead + block, dtype)
    return made


def forward(sizes, tokens, cotangent, small, weights):
    rows, width = tokens.shape
    keys, values = HEADS * KEY_DIM, HEADS * VALUE_DIM
    hidden = weights[N.gate].shape[1]
    groups = rows // GROUP
    most = max(max(sizes) - 1, 1)
    mine = weights[N.query].shape[0]
    ins = {N.in_tokens: (tokens, False), N.in_cotangent: (cotangent, False)}
    ins.update({name: (a, True) for name, a in small.items()})
    ins.update({N.w_ + name: (a, name == N.decay_down) for name, a in weights.items()})
    shape_of = {name: sizes + a.shape for name, a in weights.items()}
    shape_of[N.decay_down] = sizes + (mine, LANES)
    made = dict(
        vectors=((8, width), f32),
        decay_up=((LANES, keys), bf16),
        normed_t=((width, rows), bf16),
        rank_act=((rows, LANES), bf16),
        decay_pre=((rows, keys), f32),
        query=((rows, keys), bf16),
        key=((rows, keys), bf16),
        value=((rows, values), bf16),
        starts=((groups, HEADS, VALUE_DIM, KEY_DIM), bf16),
        gated_t=((values, rows), bf16),
        normed_two_t=((width, rows), bf16),
        gate_grad=((rows, hidden), bf16),
        lin_grad=((rows, hidden), bf16),
        normed_two_grad=((rows, width), f32),
        middle_b=((rows, width), bf16),
        mixed_grad=((rows, values), bf16),
        outgate_grad=((rows, values), bf16),
        side=((8, width), f32),
        middle=((rows, width), f32),
    )
    for k, (_, size) in enumerate(halves(width)):
        made[N.near_down + str(k)] = (sizes[:3] + (weights[N.down].shape[0], size), bf16)
    outs = {N.out_weight_ + name: (shape_of[name], bf16, False) for name in KEPT}
    outs.update({N.out_ + name: o + (False,) for name, o in made.items()})
    scratch = {N.all_ + name: pltpu.VMEM(shape_of[name], bf16) for name in WEIGHTS}
    shared = (N.mixed_grad, N.outgate_grad, N.middle_b)
    scratch.update({name: pltpu.VMEM(*o) for name, o in made.items() if name not in shared})
    scratch.update(
        tokens=pltpu.VMEM((rows, width), tokens.dtype),
        cotangent=pltpu.VMEM((rows, width), f32),
        input_sem=pltpu.SemaphoreType.DMA((2,)),
        tiny_mine=pltpu.VMEM((RANK, LANES), f32),
        tiny_all=pltpu.VMEM(sizes + (RANK, LANES), f32),
        down_mine=pltpu.VMEM((mine, LANES), bf16),
        grad_b=pltpu.VMEM((rows, width), bf16),
        normed=pltpu.VMEM((rows, width), bf16),
        gated=pltpu.VMEM((rows, values), bf16),
        normed_two=pltpu.VMEM((rows, width), bf16),
        gate_pre=pltpu.VMEM((rows, values), f32),
        query_dev=pltpu.VMEM((rows, keys), f32),
        offsets=pltpu.VMEM((groups, 8, keys), f32),
        mixed=pltpu.VMEM((rows, values), f32),
        up_gate=pltpu.VMEM((rows, hidden), f32),
        up_lin=pltpu.VMEM((rows, hidden), f32),
        activated_t=pltpu.VMEM((hidden, rows), bf16),
        act_grad=pltpu.VMEM((rows, hidden // (2 if sizes[0] % 2 == 0 else 1)), f32),
        down_grad=pltpu.VMEM(sizes + (weights[N.down].shape[0], halves(width)[0][1]), bf16),
        send_sem=pltpu.SemaphoreType.DMA((13, 4, most)),
        recv_sem=pltpu.SemaphoreType.DMA((13, 4, most)),
        own_sem=pltpu.SemaphoreType.DMA((13,)),
        save_sem=pltpu.SemaphoreType.DMA((len(made) + len(KEPT),)),
        back_send_sem=pltpu.SemaphoreType.DMA((2, 4, most)),
        back_recv_sem=pltpu.SemaphoreType.DMA((2, 4, most)),
    )
    for k, (_, size) in enumerate(halves(width)):
        block = (weights[N.down].shape[0], size)
        scratch.update(landings(sizes, block, bf16, N.down + str(k), False, (2,)))
    scratch.update(scan_scratch(sizes))
    results = kernel_call(forward_kernel, sizes, ins, outs, scratch, 0)
    return {name[4:]: a for name, a in results.items()}


LATE_SCATTERED = (N.decay_down,)
BACKWARD_PLAN = (
    0, 100, 3, 6, 7, 2, 2001, 2033, 5, 2011, 2023, 4, 2000, 2053, 2032, 200,
    101, 2063, 2043, 2010, 2031, 201, 102, 2022, 2030, 2052, 2021, 2062, 202, 2051, 300, 1,
    2073, 2061, 2042, 2020, 10, 8, 11, 9, 12, 2050, 2083, 2072, 2060, 2093, 2113, 2103,
    2041, 13, 2112, 2123, 2071, 2082, 2040, 2092, 2081, 2070, 2091, 2102, 2111, 2122, 2101, 2110,
    2121, 2080, 2090, 2100, 2120,
)
NORMED_BACK = (
    (N.decay_down, N.rank_grad),
    (N.query, N.query_grad),
    (N.key, N.key_grad),
    (N.value, N.value_grad),
    (N.outgate, N.outgate_grad),
)
LOADED = (
    N.query,
    N.decay_pre,
    N.mixed_grad,
    N.vectors,
    N.normed_two_t,
    N.gate_grad,
    N.lin_grad,
    N.gated_t,
    N.middle_b,
    N.normed_t,
    N.outgate_grad,
    N.key,
    N.value,
    N.starts,
    N.decay_up,
    N.rank_act,
    N.side,
    N.tokens,
)


def scatter_items(hidden, width):
    keys, values = HEADS * KEY_DIM, HEADS * VALUE_DIM
    items = {}
    for k, (start, size) in enumerate(halves(width)):
        items[N.down + str(k)] = (size, None, N.down, start)
    for k, (start, size) in enumerate(halves(hidden)):
        items[N.gate + str(k)] = (size, N.panel + str(k), N.gate, start)
    for k, (start, size) in enumerate(halves(hidden)):
        items[N.up + str(k)] = (size, N.panel + str(k), N.up, start)
    items[N.output] = (width, N.square0, N.output, 0)
    items[N.outgate] = (values, N.square1, N.outgate, 0)
    items[N.value] = (values, N.square0, N.value, 0)
    items[N.query] = (keys, N.query, N.query, 0)
    items[N.key] = (keys, N.key, N.key, 0)
    items[N.decay_down] = (LANES, N.decay_down, N.decay_down, 0)
    items[N.tiny] = (LANES, N.tiny, N.tiny, 0)
    return items


def backward_kernel(sizes, names, *refs):
    r = SimpleNamespace(**dict(zip(names, refs)))
    at = coords_of(sizes)
    devices = sizes[0] * sizes[1] * sizes[2] * sizes[3]
    count_rows, width = r.tokens.shape
    keys, values = HEADS * KEY_DIM, HEADS * VALUE_DIM
    hidden = r.gate_grad.shape[1]
    groups = count_rows // GROUP
    part = width // sizes[0]
    vectors, rows_sum = r.vectors, r.rows_sum
    per_feature, per_key, per_value = width // devices, keys // devices, VALUE_DIM // devices

    loads = {}
    for name in LOADED:
        loads[name] = pltpu.make_async_copy(
            getattr(r, N.in_ + name), getattr(r, name), r.load_sem.at[len(loads)]
        )
        loads[name].start()
    middle_load = pltpu.make_async_copy(
        r.in_normed_two_grad, r.input_grad, r.load_sem.at[len(loads)]
    )
    middle_load.start()
    result = pltpu.make_async_copy(
        r.input_grad, r.out_input_grad, r.out_sem.at[r.out_sem.shape[0] - 1]
    )

    def ready(*names_of):
        for name in names_of:
            if name in loads:
                loads.pop(name).wait()

    greet(sizes, at)
    items = scatter_items(hidden, width)
    index = {name: k for k, name in enumerate(items)}
    sources, sums, outs = {}, {}, {}
    for name, (size, slot, out, start) in items.items():
        k = index[name]
        if slot is not None:
            sources[k] = Item(getattr(r, N.slot_ + slot), 0, size)
        sums[k] = Item(getattr(r, N.sum_ + out), start, size)
        outs[k] = Item(getattr(r, N.out_ + out), start, size)
    scatter = Scatter(
        sizes,
        at,
        sources,
        {
            step: [getattr(r, kind + name, None) for name in items]
            for step, kind in LANDINGS.items()
        },
        sums,
        outs,
        (r.send_sem, r.recv_sem, r.own_sem, r.out_sem),
        {index[name] for name in LATE_SCATTERED},
    )
    for k in range(2):
        scatter.resume(index[N.down + str(k)], getattr(r, N.in_near_down + str(k)))
    scan = scan_of(sizes, True, r)
    in_slot = {}

    def take_slot(name):
        slot = items[name][1]
        if slot in in_slot:
            scatter.release(index[in_slot[slot]])
        in_slot[slot] = name
        return getattr(r, N.slot_ + slot)

    lower = lower_mask()

    def weight_grad(name, left, right, start=0):
        ready(left, right)
        target, columns_of = take_slot(name), items[name][0]
        size = min(columns_of, 256)

        def columns(k):
            here = pl.ds(pl.multiple_of(start + k * size, size), size)
            made = dot(getattr(r, left)[...], getattr(r, right)[:, here], NN)
            target[..., tile(k, size)] = made.reshape(target.shape[:5] + (size,)).astype(bf16)

        loop(columns_of // size, columns)
        scatter.begin(index[name])

    def begin_state():
        total, state, query_dev = r.total, r.state, r.query_grad
        rows_sum[...] = jnp.zeros_like(rows_sum)
        total[...] = jnp.zeros_like(total)
        ready(N.query, N.decay_pre, N.mixed_grad, N.vectors)

        def some(k):
            rows = tile(k, GROUP)
            cumulative = dot(lower, log_decay_of(r.decay_pre[rows, :]), NN, highest)
            r.cumulative[rows, :] = cumulative
            query_scaled = r.query[rows, :].astype(f32) * key_scale
            query_dev[rows, :] = (query_scaled * jnp.exp(cumulative + total[0:1, :])).astype(bf16)
            total[...] = total[...] + cumulative[GROUP - 1 :]

        loop(groups, some, 4)
        for h in range(HEADS):
            across, along = head_slices(h)
            state[h] = dot(r.mixed_grad[:, along], query_dev[:, across], TN)
        total[...] = jnp.exp(total[...])

    def attention():
        ready(N.key, N.value, N.starts)
        after_state = r.before_state

        def group(k):
            g = groups - 1 - k
            rows = tile(g, GROUP)
            cumulative = r.cumulative[rows, :]
            middle = cumulative[GROUP // 2 - 1 : GROUP // 2]
            ending = cumulative[GROUP - 1 :]
            query_scaled = r.query[rows, :].astype(f32) * key_scale
            key_full = r.key[rows, :].astype(f32)
            from_middle, to_middle = jnp.exp(cumulative - middle), jnp.exp(middle - cumulative)
            to_end, from_start = jnp.exp(ending - cumulative), jnp.exp(cumulative)
            decay_end = jnp.exp(ending)
            gated_query = (query_scaled * from_middle).astype(bf16)
            inverse_key = (key_full * to_middle).astype(bf16)
            tail_key = (key_full * to_end).astype(bf16)
            state_query = (query_scaled * from_start).astype(bf16)
            grad_cumul, through_end = [], []
            for h in range(HEADS):
                across, along = head_slices(h)
                start_b, after = r.starts[g, h], after_state[h]
                start, after_b = start_b.astype(f32), after.astype(bf16)
                grad_out = r.mixed_grad[rows, along]
                value_b = r.value[rows, along]
                query_h, key_h, tail_h = (
                    gated_query[:, across],
                    inverse_key[:, across],
                    tail_key[:, across],
                )
                scores = (dot(query_h, key_h, NT) * lower).astype(bf16)
                grad_scores = (dot(grad_out, value_b, NT) * lower).astype(bf16)
                to_query = from_start[:, across] * dot(grad_out, start_b, NN)
                to_query = to_query + from_middle[:, across] * dot(grad_scores, key_h, NN)
                to_key = to_middle[:, across] * dot(grad_scores, query_h, TN)
                to_key = to_key + to_end[:, across] * dot(value_b, after_b, NN)
                to_value = dot(scores, grad_out, TN) + dot(tail_h, after_b, NT)
                end_state = decay_end[:, across] * start + dot(value_b, tail_h, TN)
                through_end.append(jnp.sum(end_state * after, axis=0, keepdims=True))
                grad_cumul.append(
                    query_scaled[:, across] * to_query - key_full[:, across] * to_key
                )
                after_state[h] = decay_end[:, across] * after + dot(
                    grad_out, state_query[:, across], TN
                )
                r.query_grad[rows, across] = (to_query * key_scale).astype(bf16)
                r.key_grad[rows, across] = to_key.astype(bf16)
                r.value_grad[rows, along] = to_value.astype(bf16)
            log_grad = dot(lower, jnp.concatenate(grad_cumul, axis=1), TN, highest)
            log_grad = log_grad + jnp.concatenate(through_end, axis=1)
            to_decay = log_grad * jax.nn.sigmoid(-r.decay_pre[rows, :]) * (1.0 / 16.0)
            rows_sum[2:3, 0:keys] = rows_sum[2:3, 0:keys] + jnp.sum(
                to_decay, axis=0, keepdims=True
            )
            r.decay_grad[rows, :] = to_decay.astype(bf16)

        loop(groups, group, 2)

    def decay_down():
        ready(N.decay_up)
        r.rank_grad[...] = dot(r.decay_grad[...], r.decay_up[...], NT).astype(bf16)
        weight_grad(N.decay_down, N.normed_t, N.rank_grad)

    def input_grad():
        def panel(a, slot):
            return [
                pltpu.make_async_copy(
                    getattr(r, N.in_weight_ + name).at[a],
                    getattr(r, N.panel_ + name).at[slot],
                    r.panel_sem.at[k, slot],
                )
                for k, (name, _) in enumerate(NORMED_BACK)
            ]

        for a in range(min(2, sizes[0])):
            for copy in panel(a, a):
                copy.start()

        def features(a):
            slot = lax.rem(a, 2)
            for copy in panel(a, slot):
                copy.wait()
            made = None
            for name, grad in NORMED_BACK:
                weight = getattr(r, N.panel_ + name).at[slot]
                term = dot(getattr(r, grad)[...], weight[...].reshape(part, weight.shape[-1]), NT)
                made = term if made is None else made + term
            r.normed_grad[:, tile(a, part)] = made

            @pl.when(a + 2 < sizes[0])
            def _():
                for copy in panel(a + 2, slot):
                    copy.start()

        loop(sizes[0], features)
        middle_load.wait()
        ready(N.tokens)

        def some(k):
            rows = tile(k, 32)
            before = r.tokens[rows, :].astype(f32)
            scale = lax.rsqrt(jnp.mean(before * before, axis=-1, keepdims=True) + epsilon)
            plain = before * scale
            grad = r.normed_grad[rows, :]
            rows_sum[0:1, :] = rows_sum[0:1, :] + jnp.sum(grad * plain, axis=0, keepdims=True)
            grad = grad * vectors[0:1, :]
            r.input_grad[rows, :] = r.input_grad[rows, :] + scale * (
                grad - plain * jnp.mean(grad * plain, axis=-1, keepdims=True)
            )

        loop(count_rows // 32, some, 4)
        result.start()

    def tiny():
        ready(N.rank_act, N.side)
        side = r.side
        decay_up_grad = dot(r.rank_act[...], r.decay_grad[...], TN)[0:RANK]
        row = lax.broadcasted_iota(jnp.int32, (RANK, LANES), 0)
        lane = lax.broadcasted_iota(jnp.int32, (RANK, LANES), 1)
        vectors_of = (
            (rows_sum[0:1, :], per_feature),
            (side[1:2, :], per_feature),
            (rows_sum[2:3, 0:keys], per_key),
            (side[3:4, 0:VALUE_DIM], per_value),
        )

        def cut(values_of, device, per, offset):
            group, first = divmod(device * per, LANES)
            piece = values_of[:, group * LANES : (group + 1) * LANES]
            return pltpu.roll(piece, (offset - first) % LANES, 1)

        target = take_slot(N.tiny)
        for device in range(devices):
            whole = jnp.where(lane < per_key, cut(decay_up_grad, device, per_key, 0), 0.0)
            for k, (vector, per) in enumerate(vectors_of):
                wide = jnp.broadcast_to(vector, (RANK, vector.shape[1]))
                here = (row == k) & (lane >= VECTORS) & (lane < VECTORS + per)
                whole = jnp.where(here, cut(wide, device, per, VECTORS), whole)
            target[place_of(sizes, device)] = whole
        scatter.begin(index[N.tiny])

    first = halves(hidden)[1][0]
    pieces = dict(
        state=begin_state,
        attention=attention,
        gate0=lambda: weight_grad(N.gate0, N.normed_two_t, N.gate_grad),
        gate1=lambda: weight_grad(N.gate1, N.normed_two_t, N.gate_grad, first),
        up0=lambda: weight_grad(N.up0, N.normed_two_t, N.lin_grad),
        up1=lambda: weight_grad(N.up1, N.normed_two_t, N.lin_grad, first),
        output=lambda: weight_grad(N.output, N.gated_t, N.middle_b),
        outgate=lambda: weight_grad(N.outgate, N.normed_t, N.outgate_grad),
        query=lambda: weight_grad(N.query, N.normed_t, N.query_grad),
        key=lambda: weight_grad(N.key, N.normed_t, N.key_grad),
        value=lambda: weight_grad(N.value, N.normed_t, N.value_grad),
        decay_down=decay_down,
        input_grad=input_grad,
        tiny=tiny,
    )
    run_plan(
        BACKWARD_PLAN,
        pieces,
        scan,
        None,
        lambda item, step: scatter.advance(item, step),
    )
    scatter.finish()
    scan.finish()
    ready(*list(loads))
    result.wait()


def backward(sizes, tokens, saved):
    outer, inner, side, core = sizes
    devices = outer * inner * side * core
    most = max(max(sizes) - 1, 1)
    rows, width = tokens.shape
    hidden = saved[N.gate_grad].shape[1]
    keys, values = HEADS * KEY_DIM, HEADS * VALUE_DIM
    mine = width // devices
    saved = dict(saved, tokens=tokens)
    ins = {N.in_ + name: (saved[name], False) for name in LOADED}
    ins[N.in_normed_two_grad] = (saved[N.normed_two_grad], False)
    for k in range(2):
        ins[N.in_near_down + str(k)] = (saved[N.near_down + str(k)], False)
    ins.update({N.in_weight_ + name: (saved[N.weight_ + name], False) for name in KEPT})
    items = scatter_items(hidden, width)
    block, scratch, sums = {}, {}, {}
    for name, (size, slot, out, start) in items.items():
        rows_of = RANK if out == N.tiny else mine
        if slot is None:
            rows_of = saved[N.near_down0].shape[3]
        dtype = f32 if out == N.tiny else bf16
        block = (rows_of, size)
        sums[N.out_ + out] = ((rows_of, start + size), f32, False)
        scratch[N.sum_ + out] = pltpu.VMEM((rows_of, start + size), f32)
        if slot is not None and N.slot_ + slot not in scratch:
            scratch[N.slot_ + slot] = pltpu.VMEM(sizes + block, dtype)
        steps = (3, 1, 0) if slot is None else (3, 2, 1, 0)
        scratch.update(landings(sizes, block, dtype, name, name in LATE_SCATTERED, steps))
    scratch.update({n: pltpu.VMEM(saved[n].shape, saved[n].dtype) for n in LOADED})
    scratch.update(
        {
            N.panel_ + n: pltpu.VMEM((2,) + saved[N.weight_ + n].shape[1:], bf16)
            for n, _ in NORMED_BACK
        }
    )
    scratch.update(
        rows_sum=pltpu.VMEM((8, width), f32),
        cumulative=pltpu.VMEM((rows, keys), f32),
        query_grad=pltpu.VMEM((rows, keys), bf16),
        key_grad=pltpu.VMEM((rows, keys), bf16),
        value_grad=pltpu.VMEM((rows, values), bf16),
        decay_grad=pltpu.VMEM((rows, keys), bf16),
        rank_grad=pltpu.VMEM((rows, LANES), bf16),
        normed_grad=pltpu.VMEM((rows, width), f32),
        send_sem=pltpu.SemaphoreType.DMA((len(items), 4, most)),
        recv_sem=pltpu.SemaphoreType.DMA((len(items), 4, most)),
        input_grad=pltpu.VMEM((rows, width), f32),
        own_sem=pltpu.SemaphoreType.DMA((2,)),
        out_sem=pltpu.SemaphoreType.DMA((len(items) + 1,)),
        load_sem=pltpu.SemaphoreType.DMA((len(LOADED) + 1,)),
        panel_sem=pltpu.SemaphoreType.DMA((len(NORMED_BACK), 2)),
    )
    scratch.update(scan_scratch(sizes))
    outs = dict(sums, out_input_grad=((rows, width), f32, False))
    return kernel_call(backward_kernel, sizes, ins, outs, scratch, 1)


def hand_out_kernel(count, cuts, *refs):
    whole, down, tiny = refs[:count], refs[count], refs[count + 1]
    refs = refs[count + 2 :]
    outs, small, held, sems = refs[:count], refs[count : -count - 1], refs[-count - 1 : -1], refs[-1]
    loads, copies = [], []
    for k in range(count):
        loads.append(pltpu.make_async_copy(whole[k], held[k], sems.at[0, k]))
        loads[-1].start()
        copies.append(pltpu.make_async_copy(held[k], outs[k], sems.at[1, k]))
    small[0][...] = turned(down[...], highest)[0 : small[0].shape[0]]
    for target, (row, column) in zip(small[1:], cuts):
        target[...] = tiny[row : row + target.shape[0], column : column + target.shape[1]]
    for load, copy in zip(loads, copies):
        load.wait()
        copy.start()
    for copy in copies:
        copy.wait()


def hand_out(arrays, decay_down, tiny, cuts):
    vmem = pl.BlockSpec(memory_space=pltpu.VMEM)
    anywhere = pl.BlockSpec(memory_space=pl.ANY)
    shapes = [a.shape for a in arrays] + [(RANK, decay_down.shape[0])] + [c[0] for c in cuts]
    return pl.pallas_call(
        functools.partial(hand_out_kernel, len(arrays), [c[1] for c in cuts]),
        out_shape=[jax.ShapeDtypeStruct(s, f32) for s in shapes],
        in_specs=[anywhere] * len(arrays) + [vmem] * 2,
        out_specs=[anywhere] * len(arrays) + [vmem] * (len(cuts) + 1),
        scratch_shapes=[pltpu.VMEM(a.shape, f32) for a in arrays]
        + [pltpu.SemaphoreType.DMA((2, len(arrays)))],
        compiler_params=pltpu.CompilerParams(vmem_limit_bytes=VMEM_LIMIT),
    )(*arrays, decay_down, tiny)


def local(
    sizes,
    inputs,
    cotangent,
    mixer_gain,
    feed_gain,
    w_query,
    w_key,
    w_value,
    w_outgate,
    w_decay_down,
    w_decay_up,
    decay_bias,
    head_gain,
    w_output,
    w_gate,
    w_up,
    w_down,
):
    width = inputs.shape[2]
    rows = inputs.shape[0] * inputs.shape[1]
    per_feature, per_key, per_value = (
        mixer_gain.shape[0],
        decay_bias.shape[0],
        head_gain.shape[0],
    )
    tokens = inputs.reshape(rows, width)
    small = dict(
        w_decay_up=w_decay_up,
        mixer_gain=mixer_gain.reshape(1, -1),
        feed_gain=feed_gain.reshape(1, -1),
        decay_bias=decay_bias.reshape(1, -1),
        head_gain=head_gain.reshape(1, -1),
    )
    weights = dict(
        decay_down=w_decay_down.T,
        query=w_query,
        key=w_key,
        value=w_value,
        outgate=w_outgate,
        output=w_output,
        gate=w_gate,
        up=w_up,
        down=w_down,
    )
    saved = forward(sizes, tokens, cotangent.reshape(rows, width), small, weights)
    got = backward(sizes, tokens, saved)
    names = (N.query, N.key, N.value, N.outgate, N.output, N.gate, N.up, N.down)
    handed = hand_out(
        [saved[N.middle], got[N.out_input_grad]]
        + [got[N.out_ + name] for name in names],
        got[N.out_decay_down],
        got[N.out_tiny],
        (
            ((RANK, per_key), (0, 0)),
            ((1, per_feature), (0, VECTORS)),
            ((1, per_feature), (1, VECTORS)),
            ((1, per_key), (2, VECTORS)),
            ((1, per_value), (3, VECTORS)),
        ),
    )
    result, input_grad = (a.reshape(inputs.shape) for a in handed[:2])
    g_query, g_key, g_value, g_outgate, g_output, g_gate, g_up, g_down = handed[2:10]
    decay_down, decay_up = handed[10:12]
    g_mixer, g_feed, g_bias, g_head = (a.reshape(-1) for a in handed[12:])
    return (
        result,
        input_grad,
        g_mixer,
        g_feed,
        g_query,
        g_key,
        g_value,
        g_outgate,
        decay_down.T,
        decay_up,
        g_bias,
        g_head,
        g_output,
        g_gate,
        g_up,
        g_down,
    )


def solution(mesh):
    placed = (
        P("batch", "seq", None),
        P("batch", "seq", None),
        P(("seq", "batch")),
        P(("seq", "batch")),
        P(("seq", "batch"), None),
        P(("seq", "batch"), None),
        P(("seq", "batch"), None),
        P(("seq", "batch"), None),
        P(("seq", "batch"), None),
        P(None, ("seq", "batch")),
        P(("seq", "batch")),
        P(("seq", "batch")),
        P(("seq", "batch"), None),
        P(("seq", "batch"), None),
        P(("seq", "batch"), None),
        P(("seq", "batch"), None),
    )
    return jax.shard_map(
        functools.partial(local, grid_of(mesh.shape)),
        mesh=mesh,
        in_specs=placed,
        out_specs=(
            P("batch", "seq", None),
            P("batch", "seq", None),
            P(("seq", "batch")),
            P(("seq", "batch")),
            P(("seq", "batch"), None),
            P(("seq", "batch"), None),
            P(("seq", "batch"), None),
            P(("seq", "batch"), None),
            P(("seq", "batch"), None),
            P(None, ("seq", "batch")),
            P(("seq", "batch")),
            P(("seq", "batch")),
            P(("seq", "batch"), None),
            P(("seq", "batch"), None),
            P(("seq", "batch"), None),
            P(("seq", "batch"), None),
        ),
        check_vma=False,
    )
```

```python
import functools
from types import SimpleNamespace

import jax
import jax.numpy as jnp
from jax import lax
from jax.experimental import pallas as pl
from jax.experimental.pallas import tpu as pltpu
from jax.sharding import PartitionSpec as P

HEADS = 4
KEY_DIM = 128
VALUE_DIM = 256
GROUP = 64
LANES = 128
RANK = 16
VECTORS = 32
MESH = pl.DeviceIdType.MESH
VMEM_LIMIT = 67_000_000


class Names:
    def __getattr__(self, name):
        return name


N = Names()
epsilon = 1e-06
key_scale = KEY_DIM ** (-0.5)
highest = lax.Precision.HIGHEST
high = lax.Precision.HIGH
f32 = jnp.float32
bf16 = jnp.bfloat16


def grid_of(shape):
    seq, batch = shape["seq"], shape["batch"]
    outer = 4 if seq % 4 == 0 else seq
    core = 2 if batch % 2 == 0 else 1
    return (outer, seq // outer, batch // core, core)


def coords_of(sizes):
    seq, batch = lax.axis_index("seq"), lax.axis_index("batch")
    return (seq // sizes[1], seq % sizes[1], batch // sizes[3], batch % sizes[3])


def device_of(sizes, at):
    return {"seq": at[0] * sizes[1] + at[1], "batch": at[2] * sizes[3] + at[3]}


def place_of(sizes, device):
    place = []
    for size in reversed(sizes):
        device, last = divmod(device, size)
        place.insert(0, last)
    return tuple(place)


def others(size):
    return sorted(range(1, size), key=lambda by: min(by, size - by))


def moved(sizes, at, axis, by):
    new = list(at)
    new[axis] = lax.rem(at[axis] + (by % sizes[axis]), sizes[axis])
    return tuple(new)


def region(ref, free, at):
    return ref.at[tuple(slice(None) if k in free else at[k] for k in range(4))]


def orders_of(sizes, late=False):
    orders = ((1, 2, 0, 3), (2, 1, 0, 3)) if late else ((0, 1, 2, 3), (0, 2, 1, 3))
    return orders if sizes[1] == sizes[2] and sizes[3] == 2 else orders[:1]


def hops_of(sizes):
    length, hops = sizes[0] * sizes[1], []
    while 2 ** len(hops) < length:
        hops.append(2 ** len(hops))
    return hops


def greet(sizes, at):
    barrier = pltpu.get_barrier_semaphore()
    length = sizes[0] * sizes[1]
    seq, batch = lax.axis_index("seq"), lax.axis_index("batch")
    targets = [
        device_of(sizes, moved(sizes, at, axis, by))
        for axis in range(4)
        for by in range(1, sizes[axis])
    ]
    for hop in hops_of(sizes):
        for by in (hop, length - hop):
            targets.append({"seq": lax.rem(seq + by, length), "batch": batch})
    for target in targets:
        pl.semaphore_signal(barrier, inc=1, device_id=target, device_id_type=MESH)
    pl.semaphore_wait(barrier, len(targets))


def by_order(sizes, at, act, late=False):
    orders = orders_of(sizes, late)
    if len(orders) == 1:
        act(orders[0])
        return
    for parity, order in enumerate(orders):
        pl.when(at[3] == parity)(functools.partial(act, order))


def loop(count, body, together=1):
    together = min(together, count)
    while count % together:
        together -= 1

    def step(k, carry):
        for j in range(together):
            body(k * together + j)
        return carry

    lax.fori_loop(0, count // together, step, 0)


def dot(left, right, dims, precision=None):
    return lax.dot_general(
        left, right, (dims, ((), ())), precision=precision, preferred_element_type=f32
    )


NN = ((1,), (0,))
NT = ((1,), (1,))
TN = ((0,), (0,))


class Item:
    def __init__(self, ref, start=0, size=None):
        self.ref, self.start = ref, start
        self.size = ref.shape[-1] if size is None else size
        self.part = self.size != ref.shape[-1]

    def tail(self):
        return (slice(None), slice(self.start, self.start + self.size)) if self.part else ()

    def at(self, index):
        return self.ref.at[tuple(index) + self.tail()]


def blocks_of(free, at, axes=4):
    return tuple(slice(None) if k in free else at[k] for k in range(axes))


class Gather:
    def __init__(self, sizes, at, shards, wholes, sems, late):
        self.sizes, self.at, self.late = sizes, at, late
        self.shards, self.wholes = shards, wholes
        self.send_sem, self.recv_sem, self.own_sem = sems
        self.done = {item: 0 for item in range(len(shards))}

    def copies(self, item, order, step, arriving):
        axis, free = order[step], order[:step]
        made = []
        for by in others(self.sizes[axis]):
            source = moved(self.sizes, self.at, axis, -by) if arriving else self.at
            place = self.wholes[item].at(blocks_of(free, source))
            made.append(
                pltpu.make_async_remote_copy(
                    src_ref=self.shards[item].at(()) if step == 0 and not arriving else place,
                    dst_ref=place,
                    send_sem=self.send_sem.at[item, step, by - 1],
                    recv_sem=self.recv_sem.at[item, step, by - 1],
                    device_id=device_of(self.sizes, moved(self.sizes, self.at, axis, by)),
                    device_id_type=MESH,
                )
            )
        return made

    def own(self, item):
        return pltpu.make_async_copy(
            self.shards[item].at(()),
            self.wholes[item].at(blocks_of((), self.at)),
            self.own_sem.at[item],
        )

    def begin(self, items):
        for item in items:

            def act(order, item=item):
                for copy in self.copies(item, order, 0, False):
                    copy.start()

            if item in self.late:
                by_order(self.sizes, self.at, act, True)
            else:
                act(orders_of(self.sizes)[0])
            self.own(item).start()

    def advance(self, item, step):
        while self.done[item] < step:
            now = self.done[item] = self.done[item] + 1
            if now == 1:
                self.own(item).wait()

            def act(order, now=now):
                for copy in self.copies(item, order, now - 1, True):
                    copy.wait_recv()
                if now < 4:
                    for copy in self.copies(item, order, now, False):
                        copy.start()

            by_order(self.sizes, self.at, act, item in self.late)

    def finish(self):
        for item in self.done:
            self.advance(item, 4)
        for late in (False, True):

            def act(order, late=late):
                for item in self.done:
                    if (item in self.late) == late:
                        for step in range(4):
                            for copy in self.copies(item, order, step, False):
                                copy.wait_send()

            by_order(self.sizes, self.at, act, late)


class Scatter:
    def __init__(self, sizes, at, sources, lands, sums, outs, sems, late, stop=0):
        self.sizes, self.at, self.late, self.stop = sizes, at, late, stop
        self.outs = outs
        self.sources, self.sums = sources, sums
        self.near, self.lands = lands[3], lands
        self.send_sem, self.recv_sem, self.load_sem, self.out_sem = sems
        self.left, self.sent, self.resumed = {}, {}, {}

    def copy(self, item, order, step, by):
        axis, free = order[step], order[:step]
        target = moved(self.sizes, self.at, axis, by)
        if step == 3:
            source = self.sources[item].at(blocks_of(free, target))
            landing = self.near[item]
        else:
            whole = self.resumed[item] if step == 1 and item in self.resumed else self.near[item]
            source = whole.at[blocks_of(free, target, 3)]
            landing = self.lands[step][item].at[by - 1]
        return pltpu.make_async_remote_copy(
            src_ref=source,
            dst_ref=landing,
            send_sem=self.send_sem.at[item, step, by - 1],
            recv_sem=self.recv_sem.at[item, step, by - 1],
            device_id=device_of(self.sizes, target),
            device_id_type=MESH,
        )

    def begin(self, item):
        self.left[item] = 4
        self.sent[item] = {3}
        self.copy(item, orders_of(self.sizes)[0], 3, 1).start()

    def load(self, item):
        return pltpu.make_async_copy(self.resumed[item], self.near[item], self.load_sem.at[item])

    def resume(self, item, far):
        self.left[item] = 2
        self.sent[item] = {1}
        self.resumed[item] = far
        self.load(item).start()

        def act(order):
            for by in range(1, self.sizes[order[1]]):
                self.copy(item, order, 1, by).start()

        by_order(self.sizes, self.at, act, item in self.late)

    def advance(self, item, step):
        while self.left[item] > max(step, self.stop):
            now = self.left[item] = self.left[item] - 1
            more = now > self.stop
            if more:
                self.sent[item].add(now - 1)
            if now == 1 and item in self.resumed:
                self.load(item).wait()

            def act(order, now=now, more=more):
                self.add(item, order, now)
                if more:
                    for by in others(self.sizes[order[now - 1]]):
                        self.copy(item, order, now - 1, by).start()

            by_order(self.sizes, self.at, act, item in self.late)
            if now == 0:
                self.out(item).start()

    def out(self, item):
        return pltpu.make_async_copy(
            self.sums[item].at(()), self.outs[item].at(()), self.out_sem.at[item]
        )

    def add(self, item, order, step):
        sizes, at = self.sizes, self.at
        axis, free = order[step], sorted(order[:step])
        near = self.near[item]
        for by in range(1, sizes[axis]):
            self.copy(item, order, step, by).wait_recv()
        if step == 0:
            total = near[at[0], at[1], at[2]].astype(f32)
            for by in range(1, sizes[axis]):
                total = total + self.lands[0][item][by - 1].astype(f32)
            kept = self.sums[item]
            kept.ref[:, kept.start : kept.start + kept.size] = total
            return

        def at_first(k):
            for j in range(sizes[free[1]] if len(free) > 1 else 1):
                for i in range(sizes[free[2]] if len(free) > 2 else 1):
                    within = (k, j, i)[: len(free)]
                    place = list(at[:3])
                    for axis_of, index in zip(free, within):
                        place[axis_of] = index
                    place = tuple(place)
                    total = near[place].astype(f32)
                    if step == 3:
                        source = self.sources[item]
                        mine = source.ref[place + (at[3],) + source.tail()]
                        total = total + mine.astype(f32)
                    else:
                        for by in range(1, sizes[axis]):
                            come = self.lands[step][item].at[by - 1]
                            total = total + come[within].astype(f32)
                    near[place] = total.astype(near.dtype)

        loop(sizes[free[0]], at_first)

    def release(self, item):
        self.advance(item, 3)
        self.sent[item].remove(3)
        self.copy(item, orders_of(self.sizes)[0], 3, 1).wait_send()

    def finish(self):
        for item in self.left:
            self.advance(item, 0)
            if self.stop == 0:
                self.out(item).wait()
        for late in (False, True):

            def act(order, late=late):
                for item in self.left:
                    if (item in self.late) == late:
                        for step in sorted(self.sent[item]):
                            for by in range(1, self.sizes[order[step]]):
                                self.copy(item, order, step, by).wait_send()

            by_order(self.sizes, self.at, act, late)


class Scan:
    def __init__(self, sizes, reverse, total, state, before_total, before_state, buffers, sems):
        self.sizes, self.reverse = sizes, reverse
        self.total, self.state = total, state
        self.before_total, self.before_state = before_total, before_state
        self.total_out, self.total_in, self.state_out, self.state_in = buffers
        self.sems = sems
        self.hops = hops_of(sizes)
        self.length = sizes[0] * sizes[1]
        self.place = self.length - 1 - lax.axis_index("seq") if reverse else lax.axis_index("seq")

    def copies(self, k):
        seq = lax.axis_index("seq")
        hop = self.length - self.hops[k] if self.reverse else self.hops[k]
        target = {"seq": lax.rem(seq + hop, self.length), "batch": lax.axis_index("batch")}
        pairs = ((self.total_out, self.total_in), (self.state_out, self.state_in))
        return [
            pltpu.make_async_remote_copy(
                src_ref=out.at[k],
                dst_ref=come.at[k],
                send_sem=self.sems.at[0, k, n],
                recv_sem=self.sems.at[1, k, n],
                device_id=target,
                device_id_type=MESH,
            )
            for n, (out, come) in enumerate(pairs)
        ]

    def send(self, k):
        if k == 0:
            self.before_total[...] = jnp.ones_like(self.before_total)
            self.before_state[...] = jnp.zeros_like(self.before_state)
        self.total_out[k] = self.total[...]
        for h in range(HEADS):
            self.state_out[k, h] = self.state[h].astype(bf16)

        @pl.when(self.place + self.hops[k] < self.length)
        def _():
            for copy in self.copies(k):
                copy.start()

    def receive(self, k):
        @pl.when(self.place >= self.hops[k])
        def _():
            for copy in self.copies(k):
                copy.wait_recv()
            come = self.total_in[k]
            for h in range(HEADS):
                keys = slice(h * KEY_DIM, (h + 1) * KEY_DIM)
                state = self.state_in[k, h].astype(f32)
                self.before_state[h] = (
                    self.before_state[h] + self.before_total[0:1, keys] * state
                )
                if k + 1 < len(self.hops):
                    self.state[h] = self.state[h] + self.total[0:1, keys] * state
            self.before_total[...] = self.before_total[...] * come
            if k + 1 < len(self.hops):
                self.total[...] = self.total[...] * come

    def finish(self):
        for k in range(len(self.hops)):

            @pl.when(self.place + self.hops[k] < self.length)
            def _(k=k):
                for copy in self.copies(k):
                    copy.wait_send()


def lower_mask():
    rows = lax.broadcasted_iota(jnp.int32, (GROUP, GROUP), 0)
    columns = lax.broadcasted_iota(jnp.int32, (GROUP, GROUP), 1)
    return jnp.where(rows >= columns, 1.0, 0.0).astype(f32)


def log_decay_of(decay_pre):
    return jax.nn.log_sigmoid(decay_pre) * (1.0 / 16.0)


def spread(block, offset, per, width):
    devices = width // per
    lane = lax.broadcasted_iota(jnp.int32, (LANES, width), 0)
    column = lax.broadcasted_iota(jnp.int32, (LANES, width), 1)
    pick = jnp.where(lane == offset + column % per, 1.0, 0.0).astype(bf16)
    wide = dot(block.astype(bf16), pick, NN)
    rows = block.shape[0] // devices
    wide = wide.reshape(devices, rows, width)
    device = lax.broadcasted_iota(jnp.int32, wide.shape, 0)
    column = lax.broadcasted_iota(jnp.int32, wide.shape, 2)
    return jnp.sum(jnp.where(device == column // per, wide, 0.0), axis=0)


def turned(array, precision=None):
    size = array.shape[1]
    rows = lax.broadcasted_iota(jnp.int32, (size, size), 0)
    columns = lax.broadcasted_iota(jnp.int32, (size, size), 1)
    return dot(jnp.where(rows == columns, 1.0, 0.0).astype(array.dtype), array, NT, precision)


def scan_scratch(sizes):
    hops = len(hops_of(sizes))
    keys = HEADS * KEY_DIM
    return dict(
        total=pltpu.VMEM((8, keys), f32),
        state=pltpu.VMEM((HEADS, VALUE_DIM, KEY_DIM), f32),
        before_total=pltpu.VMEM((8, keys), f32),
        before_state=pltpu.VMEM((HEADS, VALUE_DIM, KEY_DIM), f32),
        total_out=pltpu.VMEM((hops, 8, keys), f32),
        total_in=pltpu.VMEM((hops, 8, keys), f32),
        state_out=pltpu.VMEM((hops, HEADS, VALUE_DIM, KEY_DIM), bf16),
        state_in=pltpu.VMEM((hops, HEADS, VALUE_DIM, KEY_DIM), bf16),
        scan_sem=pltpu.SemaphoreType.DMA((2, hops, 2)),
    )


def scan_of(sizes, reverse, r):
    return Scan(
        sizes,
        reverse,
        r.total,
        r.state,
        r.before_total,
        r.before_state,
        (r.total_out, r.total_in, r.state_out, r.state_in),
        r.scan_sem,
    )


def head_slices(h):
    return slice(h * KEY_DIM, (h + 1) * KEY_DIM), slice(h * VALUE_DIM, (h + 1) * VALUE_DIM)


def tile(k, size):
    return pl.ds(pl.multiple_of(k * size, size), size)


def halves(columns):
    first = -(-columns // 512) * 256
    return ((0, first), (first, columns - first))


WEIGHTS = (N.decay_down, N.query, N.key, N.value, N.outgate, N.output, N.gate, N.up, N.down)
KEPT = WEIGHTS[:5]
LATE_GATHERED = (N.down1,)
GATHER_ORDER = (0, 3, 2, 1, 4, 5, 10, 6, 7, 12, 9, 11, 8)
FORWARD_PLAN = (
    1001, 1121, 1031, 1002, 1021, 1011, 1003, 1032, 1022, 1004, 0, 1012, 1, 1041, 1033, 1023,
    1034, 4, 1013, 1051, 1042, 1024, 3, 1014, 2, 1052, 1101, 1043, 1061, 1102, 1044, 5,
    6, 1071, 1062, 1053, 100, 1054, 7, 1103, 1072, 1104, 1063, 200, 101, 1081, 1064, 201,
    102, 1091, 1111, 1073, 1082, 1074, 202, 1122, 300, 8, 1092, 9, 1112, 1083, 1084, 10,
    1093, 1094, 1113, 11, 12, 1123, 2003, 13, 1114, 2013, 1124, 14, 16, 2002, 17, 15,
    2012,
)


def forward_kernel(sizes, names, *refs):
    r = SimpleNamespace(**dict(zip(names, refs)))
    r.mixed_grad, r.outgate_grad, r.middle_b = r.gated, r.normed, r.tokens
    at = coords_of(sizes)
    devices = sizes[0] * sizes[1] * sizes[2] * sizes[3]
    count_rows, width = r.tokens.shape
    keys, values = HEADS * KEY_DIM, HEADS * VALUE_DIM
    hidden = r.up_gate.shape[1]
    groups = count_rows // GROUP
    vectors = r.vectors
    per_feature, per_key, per_value = width // devices, keys // devices, VALUE_DIM // devices

    loads = [
        pltpu.make_async_copy(r.in_tokens, r.tokens, r.input_sem.at[0]),
        pltpu.make_async_copy(r.in_cotangent, r.cotangent, r.input_sem.at[1]),
    ]
    for copy in loads:
        copy.start()
    tiny = r.tiny_mine
    tiny[...] = jnp.zeros_like(tiny)
    tiny[:, 0:per_key] = r.w_decay_up[...].astype(f32)
    for k, name in enumerate((N.mixer_gain, N.feed_gain, N.decay_bias, N.head_gain)):
        vector = getattr(r, name)
        tiny[k : k + 1, VECTORS : VECTORS + vector.shape[1]] = vector[...].astype(f32)
    down_mine = r.down_mine
    down_mine[...] = jnp.zeros_like(down_mine)
    down_mine[:, 0:RANK] = turned(r.w_decay_down[...]).astype(bf16)
    greet(sizes, at)

    shards, wholes, index = [Item(tiny)], [Item(r.tiny_all)], {N.tiny: 0}
    late = set()

    def item(name, shard, whole, start=0, size=None):
        index[name] = len(shards)
        if name in LATE_GATHERED:
            late.add(len(shards))
        shards.append(Item(shard, start, size))
        wholes.append(Item(whole, start, size))

    item(N.decay_down, down_mine, r.all_decay_down)
    for name in (N.query, N.key, N.value, N.outgate, N.output):
        item(name, getattr(r, N.w_ + name), getattr(r, N.all_ + name))
    for k in range(2):
        for name in (N.gate, N.up):
            item(name + str(k), getattr(r, N.w_ + name), getattr(r, N.all_ + name), *halves(hidden)[k])
    for k in range(2):
        item(N.down + str(k), r.w_down, r.all_down, *halves(width)[k])
    gather = Gather(
        sizes, at, shards, wholes, (r.send_sem, r.recv_sem, r.own_sem), late
    )
    gather.begin(GATHER_ORDER)
    scan = scan_of(sizes, False, r)
    saved = []
    scatter = Scatter(
        sizes,
        at,
        [Item(r.down_grad, 0, size) for _, size in halves(width)],
        {3: (r.near_down0, r.near_down1), 2: (r.half_down0, r.half_down1)},
        None,
        None,
        (r.back_send_sem, r.back_recv_sem, None, None),
        (),
        2,
    )

    def save(*names_of):
        for name in names_of:
            source = getattr(r, N.all_ + name[7:]) if name.startswith(N.weight_) else getattr(r, name)
            copy = pltpu.make_async_copy(source, getattr(r, N.out_ + name), r.save_sem.at[len(saved)])
            copy.start()
            saved.append(copy)

    def need(*names_of):
        for name in names_of:
            gather.advance(index[name], 4)

    lower = lower_mask()

    def turn(source, target):
        def columns(k):
            target[tile(k, 256), :] = turned(source[:, tile(k, 256)]).astype(bf16)

        loop(source.shape[1] // 256, columns)

    def unpack():
        need(N.tiny)
        whole = r.tiny_all[...].reshape(devices, RANK, LANES)
        vectors[...] = jnp.zeros_like(vectors)
        vectors[0:1, :] = spread(whole[:, 0], VECTORS, per_feature, width)
        vectors[1:2, :] = spread(whole[:, 1], VECTORS, per_feature, width)
        vectors[2:3, 0:keys] = spread(whole[:, 2], VECTORS, per_key, keys)
        vectors[3:4, 0:VALUE_DIM] = spread(whole[:, 3], VECTORS, per_value, VALUE_DIM)
        decay_up = r.decay_up
        decay_up[...] = jnp.zeros_like(decay_up)
        lane = lax.broadcasted_iota(jnp.int32, (RANK, LANES), 1)
        together = LANES // per_key
        for group in range(keys // LANES):
            joined = jnp.zeros((RANK, LANES), f32)
            for k in range(together):
                block = r.tiny_all[place_of(sizes, group * together + k)]
                here = (lane >= k * per_key) & (lane < (k + 1) * per_key)
                joined = jnp.where(here, pltpu.roll(block, k * per_key, 1), joined)
            decay_up[0:RANK, group * LANES : (group + 1) * LANES] = joined.astype(bf16)
        save(N.vectors, N.decay_up)

    def norm():
        for copy in loads:
            copy.wait()

        def some(k):
            rows = tile(k, 32)
            plain = r.tokens[rows, :].astype(f32)
            scale = lax.rsqrt(jnp.mean(plain * plain, axis=-1, keepdims=True) + epsilon)
            r.normed[rows, :] = (plain * scale * vectors[0:1, :]).astype(bf16)
            r.grad_b[rows, :] = r.cotangent[rows, :].astype(bf16)

        loop(count_rows // 32, some, 4)
        turn(r.normed, r.normed_t)
        save(N.normed_t)

    def project(name, into):
        need(name)
        weight = getattr(r, N.all_ + name)
        size = min(into.shape[1], 256)

        def columns(k):
            here = tile(k, size)
            panel = weight[..., here].reshape(width, size)
            into[:, here] = dot(r.normed[...], panel, NN).astype(into.dtype)

        loop(into.shape[1] // size, columns)
        save(N.weight_ + name)

    def decay():
        project(N.decay_down, r.rank_act)
        r.decay_pre[...] = (
            dot(r.rank_act[...], r.decay_up[...], NN) + vectors[2:3, 0:keys]
        )
        save(N.rank_act, N.decay_pre)

    def attention():
        total, state = r.total, r.state
        total[...] = jnp.zeros_like(total)
        state[...] = jnp.zeros_like(state)

        def group(k):
            rows = tile(k, GROUP)
            cumulative = dot(lower, log_decay_of(r.decay_pre[rows, :]), NN, highest)
            middle = cumulative[GROUP // 2 - 1 : GROUP // 2]
            ending = cumulative[GROUP - 1 :]
            query_scaled = r.query[rows, :].astype(f32) * key_scale
            key_full = r.key[rows, :].astype(f32)
            gated_query = query_scaled * jnp.exp(cumulative - middle)
            inverse_key = key_full * jnp.exp(middle - cumulative)
            tail_key = key_full * jnp.exp(ending - cumulative)
            state_query = query_scaled * jnp.exp(cumulative)
            r.query_dev[rows, :] = state_query * jnp.exp(total[0:1, :])
            r.offsets[k] = total[...]
            for h in range(HEADS):
                across, along = head_slices(h)
                value_full = r.value[rows, along].astype(f32)
                scores = dot(gated_query[:, across], inverse_key[:, across], NT, high) * lower
                start = state[h]
                r.starts[k, h] = start.astype(bf16)
                r.mixed[rows, along] = dot(state_query[:, across], start, NT, high) + dot(
                    scores, value_full, NN, high
                )
                state[h] = jnp.exp(ending[:, across]) * start + dot(
                    value_full, tail_key[:, across], TN, high
                )
            total[...] = total[...] + ending

        loop(groups, group, 2)
        total[...] = jnp.exp(total[...])
        save(N.query, N.key, N.value)

    def heads():
        before = r.before_state

        def some(k):
            rows = tile(k, GROUP)
            factor = jnp.exp(r.offsets[k])
            for h in range(HEADS):
                across, along = head_slices(h)
                begin = r.starts[k, h].astype(f32) + factor[0:1, across] * before[h]
                r.starts[k, h] = begin.astype(bf16)
                whole = r.mixed[rows, along] + dot(
                    r.query_dev[rows, across], before[h], NT, high
                )
                r.mixed[rows, along] = whole
                scale = lax.rsqrt(jnp.mean(whole * whole, axis=-1, keepdims=True) + epsilon)
                gate = r.gate_pre[rows, along]
                swish = gate * jax.nn.sigmoid(gate)
                r.gated[rows, along] = (
                    whole * scale * vectors[3:4, 0:VALUE_DIM] * swish
                ).astype(bf16)

        loop(groups, some, 2)
        turn(r.gated, r.gated_t)
        save(N.starts, N.gated_t)

    def middle():
        need(N.output)

        def columns(k):
            here = tile(k, 256)
            panel = r.all_output[..., here].reshape(values, 256)
            r.middle[:, here] = r.tokens[:, here].astype(f32) + dot(
                r.gated[...], panel, NN
            )

        loop(width // 256, columns)

        def some(k):
            rows = tile(k, 32)
            plain = r.middle[rows, :]
            scale = lax.rsqrt(jnp.mean(plain * plain, axis=-1, keepdims=True) + epsilon)
            r.normed_two[rows, :] = (plain * scale * vectors[1:2, :]).astype(bf16)

        loop(count_rows // 32, some, 4)
        turn(r.normed_two, r.normed_two_t)
        save(N.normed_two_t)

    def up(half):
        need(N.gate + str(half), N.up + str(half))
        start, size = halves(hidden)[half]

        def columns(k):
            here = pl.ds(pl.multiple_of(start + k * 256, 256), 256)
            normed_two = r.normed_two[...]
            gate = dot(normed_two, r.all_gate[..., here].reshape(width, 256), NN)
            line = dot(normed_two, r.all_up[..., here].reshape(width, 256), NN)
            r.up_gate[:, here] = gate
            r.up_lin[:, here] = line
            activated = (gate * jax.nn.sigmoid(gate) * line).astype(bf16)
            r.activated_t[here, :] = turned(activated).astype(bf16)

        loop(size // 256, columns)

    def down_grad(half):
        if half > 0:
            scatter.release(half - 1)
        start, size = halves(width)[half]
        target = r.down_grad
        count = 2 if sizes[0] % 2 == 0 else 1
        some, wide = sizes[0] // count, hidden // count
        for k in range(count):
            left = r.activated_t[k * wide : (k + 1) * wide, :]

            def columns(m, left=left, k=k):
                made = dot(left, r.grad_b[:, pl.ds(pl.multiple_of(start + m * 256, 256), 256)], NN)
                shaped = made.reshape((some,) + target.shape[1:5] + (256,))
                target[k * some : (k + 1) * some, :, :, :, :, tile(m, 256)] = shaped.astype(bf16)

            loop(size // 256, columns)
        scatter.begin(half)

    down = r.all_down

    def act():
        need(N.down0, N.down1)
        count = 2 if sizes[0] % 2 == 0 else 1
        some, wide = down.shape[0] // count, hidden // count
        for k in range(count):
            for start, size in halves(width):
                along = slice(start, start + size)
                panel = down[k * some : (k + 1) * some, :, :, :, :, along].reshape(wide, size)
                made = dot(r.grad_b[:, along], panel, NT)
                r.act_grad[...] = made if start == 0 else r.act_grad[...] + made

            def finish(m, k=k):
                here = pl.ds(pl.multiple_of(k * wide + m * 128, 128), 128)
                grad, gate, line = r.act_grad[:, tile(m, 128)], r.up_gate[:, here], r.up_lin[:, here]
                sig = jax.nn.sigmoid(gate)
                r.gate_grad[:, here] = (grad * line * sig * (1.0 + gate * (1.0 - sig))).astype(bf16)
                r.lin_grad[:, here] = (grad * gate * sig).astype(bf16)

            loop(wide // 128, finish, 2)

    def block():
        def columns(k):
            here = tile(k, 256)
            r.middle[:, here] = r.middle[:, here] + dot(
                r.activated_t[...], down[..., here].reshape(hidden, 256), TN
            )

        loop(width // 256, columns)
        save(N.middle)

    def feed_back():
        save(N.gate_grad, N.lin_grad)
        part = width // sizes[0]

        def features(a):
            here = tile(a, part)
            r.normed_two_grad[:, here] = dot(
                r.gate_grad[...], r.all_gate[a].reshape(part, hidden), NT
            ) + dot(r.lin_grad[...], r.all_up[a].reshape(part, hidden), NT)

        loop(sizes[0], features)
        side = r.side
        side[...] = jnp.zeros_like(side)

        def some(k):
            rows = tile(k, 32)
            before = r.middle[rows, :]
            scale = lax.rsqrt(jnp.mean(before * before, axis=-1, keepdims=True) + epsilon)
            plain = before * scale
            grad = r.normed_two_grad[rows, :]
            side[1:2, :] = side[1:2, :] + jnp.sum(grad * plain, axis=0, keepdims=True)
            grad = grad * vectors[1:2, :]
            whole = r.cotangent[rows, :] + scale * (
                grad - plain * jnp.mean(grad * plain, axis=-1, keepdims=True)
            )
            r.normed_two_grad[rows, :] = whole
            r.middle_b[rows, :] = whole.astype(bf16)

        loop(count_rows // 32, some, 4)
        save(N.normed_two_grad, N.middle_b)

    def heads_back():
        side = r.side
        gain = vectors[3:4, 0:VALUE_DIM]
        part = values // sizes[0]
        for h in range(HEADS):
            across, along = head_slices(h)
            first, count = h * VALUE_DIM // part, max(VALUE_DIM // part, 1)
            weight = r.all_output[first : first + count].reshape(count * part, width)
            r.act_grad[:, 0:VALUE_DIM] = dot(r.middle_b[...], weight, NT)

            def some(k, along=along):
                rows = tile(k, GROUP)
                whole, gate = r.mixed[rows, along], r.gate_pre[rows, along]
                grad = r.act_grad[rows, 0:VALUE_DIM]
                scale = lax.rsqrt(jnp.mean(whole * whole, axis=-1, keepdims=True) + epsilon)
                sig = jax.nn.sigmoid(gate)
                plain = whole * scale
                through = grad * (gate * sig)
                side[3:4, 0:VALUE_DIM] = side[3:4, 0:VALUE_DIM] + jnp.sum(
                    through * plain, axis=0, keepdims=True
                )
                back = through * gain
                r.mixed_grad[rows, along] = (
                    scale * (back - plain * jnp.mean(back * plain, axis=-1, keepdims=True))
                ).astype(bf16)
                r.outgate_grad[rows, along] = (
                    grad * plain * gain * sig * (1.0 + gate * (1.0 - sig))
                ).astype(bf16)

            loop(groups, some, 4)
        save(N.mixed_grad, N.outgate_grad, N.side)

    pieces = dict(
        unpack=unpack,
        norm=norm,
        decay=decay,
        query=lambda: project(N.query, r.query),
        key=lambda: project(N.key, r.key),
        value=lambda: project(N.value, r.value),
        attention=attention,
        outgate=lambda: project(N.outgate, r.gate_pre),
        heads=heads,
        middle=middle,
        up0=lambda: up(0),
        up1=lambda: up(1),
        down_grad0=lambda: down_grad(0),
        down_grad1=lambda: down_grad(1),
        act=act,
        block=block,
        feed_back=feed_back,
        heads_back=heads_back,
    )
    run_plan(
        FORWARD_PLAN,
        pieces,
        scan,
        lambda item, step: gather.advance(item, step),
        lambda item, step: scatter.advance(item, step),
    )
    scatter.finish()
    save(N.near_down0, N.near_down1)
    gather.finish()
    scan.finish()
    for copy in saved:
        copy.wait()


def run_plan(plan, pieces, scan, gather, scatter):
    hops = len(scan.hops)
    steps = list(pieces.values())
    for code in plan:
        if code >= 1000:
            (gather if code < 2000 else scatter)(code % 1000 // 10, code % 10)
        elif code < 100:
            steps[code]()
        elif code == 300:
            for k in range(3, hops):
                scan.send(k)
                scan.receive(k)
        elif code % 100 < hops:
            (scan.send if code < 200 else scan.receive)(code % 100)


def kernel_call(body, sizes, ins, outs, scratch, collective_id):
    vmem = pl.BlockSpec(memory_space=pltpu.VMEM)
    anywhere = pl.BlockSpec(memory_space=pl.ANY)
    names = list(ins) + list(outs) + list(scratch)
    assert len(set(names)) == len(names)
    results = pl.pallas_call(
        functools.partial(body, sizes, names),
        out_shape=[jax.ShapeDtypeStruct(o[0], o[1]) for o in outs.values()],
        in_specs=[vmem if i[1] else anywhere for i in ins.values()],
        out_specs=[vmem if o[2] else anywhere for o in outs.values()],
        scratch_shapes=list(scratch.values()),
        compiler_params=pltpu.CompilerParams(
            collective_id=collective_id, has_side_effects=True, vmem_limit_bytes=VMEM_LIMIT
        ),
    )(*(i[0] for i in ins.values()))
    return dict(zip(outs, results))


LANDINGS = {3: N.near_, 2: N.half_, 1: N.part_, 0: N.last_}


def landings(sizes, block, dtype, name, late, steps):
    order = orders_of(sizes, late)[0]
    made = {}
    for step in steps:
        lead = tuple(sizes[k] for k in order[:step])
        lead = sizes[:3] if step == 3 else (max(sizes[order[step]] - 1, 1),) + lead
        made[LANDINGS[step] + name] = pltpu.VMEM(lead + block, dtype)
    return made


def forward(sizes, tokens, cotangent, small, weights):
    rows, width = tokens.shape
    keys, values = HEADS * KEY_DIM, HEADS * VALUE_DIM
    hidden = weights[N.gate].shape[1]
    groups = rows // GROUP
    most = max(max(sizes) - 1, 1)
    mine = weights[N.query].shape[0]
    ins = {N.in_tokens: (tokens, False), N.in_cotangent: (cotangent, False)}
    ins.update({name: (a, True) for name, a in small.items()})
    ins.update({N.w_ + name: (a, name == N.decay_down) for name, a in weights.items()})
    shape_of = {name: sizes + a.shape for name, a in weights.items()}
    shape_of[N.decay_down] = sizes + (mine, LANES)
    made = dict(
        vectors=((8, width), f32),
        decay_up=((LANES, keys), bf16),
        normed_t=((width, rows), bf16),
        rank_act=((rows, LANES), bf16),
        decay_pre=((rows, keys), f32),
        query=((rows, keys), bf16),
        key=((rows, keys), bf16),
        value=((rows, values), bf16),
        starts=((groups, HEADS, VALUE_DIM, KEY_DIM), bf16),
        gated_t=((values, rows), bf16),
        normed_two_t=((width, rows), bf16),
        gate_grad=((rows, hidden), bf16),
        lin_grad=((rows, hidden), bf16),
        normed_two_grad=((rows, width), f32),
        middle_b=((rows, width), bf16),
        mixed_grad=((rows, values), bf16),
        outgate_grad=((rows, values), bf16),
        side=((8, width), f32),
        middle=((rows, width), f32),
    )
    for k, (_, size) in enumerate(halves(width)):
        made[N.near_down + str(k)] = (sizes[:3] + (weights[N.down].shape[0], size), bf16)
    outs = {N.out_weight_ + name: (shape_of[name], bf16, False) for name in KEPT}
    outs.update({N.out_ + name: o + (False,) for name, o in made.items()})
    scratch = {N.all_ + name: pltpu.VMEM(shape_of[name], bf16) for name in WEIGHTS}
    shared = (N.mixed_grad, N.outgate_grad, N.middle_b)
    scratch.update({name: pltpu.VMEM(*o) for name, o in made.items() if name not in shared})
    scratch.update(
        tokens=pltpu.VMEM((rows, width), tokens.dtype),
        cotangent=pltpu.VMEM((rows, width), f32),
        input_sem=pltpu.SemaphoreType.DMA((2,)),
        tiny_mine=pltpu.VMEM((RANK, LANES), f32),
        tiny_all=pltpu.VMEM(sizes + (RANK, LANES), f32),
        down_mine=pltpu.VMEM((mine, LANES), bf16),
        grad_b=pltpu.VMEM((rows, width), bf16),
        normed=pltpu.VMEM((rows, width), bf16),
        gated=pltpu.VMEM((rows, values), bf16),
        normed_two=pltpu.VMEM((rows, width), bf16),
        gate_pre=pltpu.VMEM((rows, values), f32),
        query_dev=pltpu.VMEM((rows, keys), f32),
        offsets=pltpu.VMEM((groups, 8, keys), f32),
        mixed=pltpu.VMEM((rows, values), f32),
        up_gate=pltpu.VMEM((rows, hidden), f32),
        up_lin=pltpu.VMEM((rows, hidden), f32),
        activated_t=pltpu.VMEM((hidden, rows), bf16),
        act_grad=pltpu.VMEM((rows, hidden // (2 if sizes[0] % 2 == 0 else 1)), f32),
        down_grad=pltpu.VMEM(sizes + (weights[N.down].shape[0], halves(width)[0][1]), bf16),
        send_sem=pltpu.SemaphoreType.DMA((13, 4, most)),
        recv_sem=pltpu.SemaphoreType.DMA((13, 4, most)),
        own_sem=pltpu.SemaphoreType.DMA((13,)),
        save_sem=pltpu.SemaphoreType.DMA((len(made) + len(KEPT),)),
        back_send_sem=pltpu.SemaphoreType.DMA((2, 4, most)),
        back_recv_sem=pltpu.SemaphoreType.DMA((2, 4, most)),
    )
    for k, (_, size) in enumerate(halves(width)):
        block = (weights[N.down].shape[0], size)
        scratch.update(landings(sizes, block, bf16, N.down + str(k), False, (2,)))
    scratch.update(scan_scratch(sizes))
    results = kernel_call(forward_kernel, sizes, ins, outs, scratch, 0)
    return {name[4:]: a for name, a in results.items()}


LATE_SCATTERED = (N.decay_down,)
BACKWARD_PLAN = (
    0, 100, 3, 6, 7, 2, 2001, 2033, 5, 2011, 2023, 4, 2000, 2053, 2032, 200,
    101, 2063, 2043, 2010, 2031, 201, 102, 2022, 2030, 2052, 2021, 2062, 202, 2051, 300, 1,
    2073, 2061, 2042, 2020, 10, 8, 11, 9, 12, 2050, 2083, 2072, 2060, 2093, 2113, 2103,
    2041, 13, 2112, 2123, 2071, 2082, 2040, 2092, 2081, 2070, 2091, 2102, 2111, 2122, 2101, 2110,
    2121, 2080, 2090, 2100, 2120,
)
NORMED_BACK = (
    (N.decay_down, N.rank_grad),
    (N.query, N.query_grad),
    (N.key, N.key_grad),
    (N.value, N.value_grad),
    (N.outgate, N.outgate_grad),
)
LOADED = (
    N.query,
    N.decay_pre,
    N.mixed_grad,
    N.vectors,
    N.normed_two_t,
    N.gate_grad,
    N.lin_grad,
    N.gated_t,
    N.middle_b,
    N.normed_t,
    N.outgate_grad,
    N.key,
    N.value,
    N.starts,
    N.decay_up,
    N.rank_act,
    N.side,
    N.tokens,
)


def scatter_items(hidden, width):
    keys, values = HEADS * KEY_DIM, HEADS * VALUE_DIM
    items = {}
    for k, (start, size) in enumerate(halves(width)):
        items[N.down + str(k)] = (size, None, N.down, start)
    for k, (start, size) in enumerate(halves(hidden)):
        items[N.gate + str(k)] = (size, N.panel + str(k), N.gate, start)
    for k, (start, size) in enumerate(halves(hidden)):
        items[N.up + str(k)] = (size, N.panel + str(k), N.up, start)
    items[N.output] = (width, N.square0, N.output, 0)
    items[N.outgate] = (values, N.square1, N.outgate, 0)
    items[N.value] = (values, N.square0, N.value, 0)
    items[N.query] = (keys, N.query, N.query, 0)
    items[N.key] = (keys, N.key, N.key, 0)
    items[N.decay_down] = (LANES, N.decay_down, N.decay_down, 0)
    items[N.tiny] = (LANES, N.tiny, N.tiny, 0)
    return items


def backward_kernel(sizes, names, *refs):
    r = SimpleNamespace(**dict(zip(names, refs)))
    at = coords_of(sizes)
    devices = sizes[0] * sizes[1] * sizes[2] * sizes[3]
    count_rows, width = r.tokens.shape
    keys, values = HEADS * KEY_DIM, HEADS * VALUE_DIM
    hidden = r.gate_grad.shape[1]
    groups = count_rows // GROUP
    part = width // sizes[0]
    vectors, rows_sum = r.vectors, r.rows_sum
    per_feature, per_key, per_value = width // devices, keys // devices, VALUE_DIM // devices

    loads = {}
    for name in LOADED:
        loads[name] = pltpu.make_async_copy(
            getattr(r, N.in_ + name), getattr(r, name), r.load_sem.at[len(loads)]
        )
        loads[name].start()
    middle_load = pltpu.make_async_copy(
        r.in_normed_two_grad, r.input_grad, r.load_sem.at[len(loads)]
    )
    middle_load.start()
    result = pltpu.make_async_copy(
        r.input_grad, r.out_input_grad, r.out_sem.at[r.out_sem.shape[0] - 1]
    )

    def ready(*names_of):
        for name in names_of:
            if name in loads:
                loads.pop(name).wait()

    greet(sizes, at)
    items = scatter_items(hidden, width)
    index = {name: k for k, name in enumerate(items)}
    sources, sums, outs = {}, {}, {}
    for name, (size, slot, out, start) in items.items():
        k = index[name]
        if slot is not None:
            sources[k] = Item(getattr(r, N.slot_ + slot), 0, size)
        sums[k] = Item(getattr(r, N.sum_ + out), start, size)
        outs[k] = Item(getattr(r, N.out_ + out), start, size)
    scatter = Scatter(
        sizes,
        at,
        sources,
        {
            step: [getattr(r, kind + name, None) for name in items]
            for step, kind in LANDINGS.items()
        },
        sums,
        outs,
        (r.send_sem, r.recv_sem, r.own_sem, r.out_sem),
        {index[name] for name in LATE_SCATTERED},
    )
    for k in range(2):
        scatter.resume(index[N.down + str(k)], getattr(r, N.in_near_down + str(k)))
    scan = scan_of(sizes, True, r)
    in_slot = {}

    def take_slot(name):
        slot = items[name][1]
        if slot in in_slot:
            scatter.release(index[in_slot[slot]])
        in_slot[slot] = name
        return getattr(r, N.slot_ + slot)

    lower = lower_mask()

    def weight_grad(name, left, right, start=0):
        ready(left, right)
        target, columns_of = take_slot(name), items[name][0]
        size = min(columns_of, 256)

        def columns(k):
            here = pl.ds(pl.multiple_of(start + k * size, size), size)
            made = dot(getattr(r, left)[...], getattr(r, right)[:, here], NN)
            target[..., tile(k, size)] = made.reshape(target.shape[:5] + (size,)).astype(bf16)

        loop(columns_of // size, columns)
        scatter.begin(index[name])

    def begin_state():
        total, state, query_dev = r.total, r.state, r.query_grad
        rows_sum[...] = jnp.zeros_like(rows_sum)
        total[...] = jnp.zeros_like(total)
        ready(N.query, N.decay_pre, N.mixed_grad, N.vectors)

        def some(k):
            rows = tile(k, GROUP)
            cumulative = dot(lower, log_decay_of(r.decay_pre[rows, :]), NN, highest)
            r.cumulative[rows, :] = cumulative
            query_scaled = r.query[rows, :].astype(f32) * key_scale
            query_dev[rows, :] = (query_scaled * jnp.exp(cumulative + total[0:1, :])).astype(bf16)
            total[...] = total[...] + cumulative[GROUP - 1 :]

        loop(groups, some, 4)
        for h in range(HEADS):
            across, along = head_slices(h)
            state[h] = dot(r.mixed_grad[:, along], query_dev[:, across], TN)
        total[...] = jnp.exp(total[...])

    def attention():
        ready(N.key, N.value, N.starts)
        after_state = r.before_state

        def group(k):
            g = groups - 1 - k
            rows = tile(g, GROUP)
            cumulative = r.cumulative[rows, :]
            middle = cumulative[GROUP // 2 - 1 : GROUP // 2]
            ending = cumulative[GROUP - 1 :]
            query_scaled = r.query[rows, :].astype(f32) * key_scale
            key_full = r.key[rows, :].astype(f32)
            from_middle, to_middle = jnp.exp(cumulative - middle), jnp.exp(middle - cumulative)
            to_end, from_start = jnp.exp(ending - cumulative), jnp.exp(cumulative)
            decay_end = jnp.exp(ending)
            gated_query = (query_scaled * from_middle).astype(bf16)
            inverse_key = (key_full * to_middle).astype(bf16)
            tail_key = (key_full * to_end).astype(bf16)
            state_query = (query_scaled * from_start).astype(bf16)
            grad_cumul, through_end = [], []
            for h in range(HEADS):
                across, along = head_slices(h)
                start_b, after = r.starts[g, h], after_state[h]
                start, after_b = start_b.astype(f32), after.astype(bf16)
                grad_out = r.mixed_grad[rows, along]
                value_b = r.value[rows, along]
                query_h, key_h, tail_h = (
                    gated_query[:, across],
                    inverse_key[:, across],
                    tail_key[:, across],
                )
                scores = (dot(query_h, key_h, NT) * lower).astype(bf16)
                grad_scores = (dot(grad_out, value_b, NT) * lower).astype(bf16)
                to_query = from_start[:, across] * dot(grad_out, start_b, NN)
                to_query = to_query + from_middle[:, across] * dot(grad_scores, key_h, NN)
                to_key = to_middle[:, across] * dot(grad_scores, query_h, TN)
                to_key = to_key + to_end[:, across] * dot(value_b, after_b, NN)
                to_value = dot(scores, grad_out, TN) + dot(tail_h, after_b, NT)
                end_state = decay_end[:, across] * start + dot(value_b, tail_h, TN)
                through_end.append(jnp.sum(end_state * after, axis=0, keepdims=True))
                grad_cumul.append(
                    query_scaled[:, across] * to_query - key_full[:, across] * to_key
                )
                after_state[h] = decay_end[:, across] * after + dot(
                    grad_out, state_query[:, across], TN
                )
                r.query_grad[rows, across] = (to_query * key_scale).astype(bf16)
                r.key_grad[rows, across] = to_key.astype(bf16)
                r.value_grad[rows, along] = to_value.astype(bf16)
            log_grad = dot(lower, jnp.concatenate(grad_cumul, axis=1), TN, highest)
            log_grad = log_grad + jnp.concatenate(through_end, axis=1)
            to_decay = log_grad * jax.nn.sigmoid(-r.decay_pre[rows, :]) * (1.0 / 16.0)
            rows_sum[2:3, 0:keys] = rows_sum[2:3, 0:keys] + jnp.sum(
                to_decay, axis=0, keepdims=True
            )
            r.decay_grad[rows, :] = to_decay.astype(bf16)

        loop(groups, group, 2)

    def decay_down():
        ready(N.decay_up)
        r.rank_grad[...] = dot(r.decay_grad[...], r.decay_up[...], NT).astype(bf16)
        weight_grad(N.decay_down, N.normed_t, N.rank_grad)

    def input_grad():
        def panel(a, slot):
            return [
                pltpu.make_async_copy(
                    getattr(r, N.in_weight_ + name).at[a],
                    getattr(r, N.panel_ + name).at[slot],
                    r.panel_sem.at[k, slot],
                )
                for k, (name, _) in enumerate(NORMED_BACK)
            ]

        for a in range(min(2, sizes[0])):
            for copy in panel(a, a):
                copy.start()

        def features(a):
            slot = lax.rem(a, 2)
            for copy in panel(a, slot):
                copy.wait()
            made = None
            for name, grad in NORMED_BACK:
                weight = getattr(r, N.panel_ + name).at[slot]
                term = dot(getattr(r, grad)[...], weight[...].reshape(part, weight.shape[-1]), NT)
                made = term if made is None else made + term
            r.normed_grad[:, tile(a, part)] = made

            @pl.when(a + 2 < sizes[0])
            def _():
                for copy in panel(a + 2, slot):
                    copy.start()

        loop(sizes[0], features)
        middle_load.wait()
        ready(N.tokens)

        def some(k):
            rows = tile(k, 32)
            before = r.tokens[rows, :].astype(f32)
            scale = lax.rsqrt(jnp.mean(before * before, axis=-1, keepdims=True) + epsilon)
            plain = before * scale
            grad = r.normed_grad[rows, :]
            rows_sum[0:1, :] = rows_sum[0:1, :] + jnp.sum(grad * plain, axis=0, keepdims=True)
            grad = grad * vectors[0:1, :]
            r.input_grad[rows, :] = r.input_grad[rows, :] + scale * (
                grad - plain * jnp.mean(grad * plain, axis=-1, keepdims=True)
            )

        loop(count_rows // 32, some, 4)
        result.start()

    def tiny():
        ready(N.rank_act, N.side)
        side = r.side
        decay_up_grad = dot(r.rank_act[...], r.decay_grad[...], TN)[0:RANK]
        row = lax.broadcasted_iota(jnp.int32, (RANK, LANES), 0)
        lane = lax.broadcasted_iota(jnp.int32, (RANK, LANES), 1)
        vectors_of = (
            (rows_sum[0:1, :], per_feature),
            (side[1:2, :], per_feature),
            (rows_sum[2:3, 0:keys], per_key),
            (side[3:4, 0:VALUE_DIM], per_value),
        )

        def cut(values_of, device, per, offset):
            group, first = divmod(device * per, LANES)
            piece = values_of[:, group * LANES : (group + 1) * LANES]
            return pltpu.roll(piece, (offset - first) % LANES, 1)

        target = take_slot(N.tiny)
        for device in range(devices):
            whole = jnp.where(lane < per_key, cut(decay_up_grad, device, per_key, 0), 0.0)
            for k, (vector, per) in enumerate(vectors_of):
                wide = jnp.broadcast_to(vector, (RANK, vector.shape[1]))
                here = (row == k) & (lane >= VECTORS) & (lane < VECTORS + per)
                whole = jnp.where(here, cut(wide, device, per, VECTORS), whole)
            target[place_of(sizes, device)] = whole
        scatter.begin(index[N.tiny])

    first = halves(hidden)[1][0]
    pieces = dict(
        state=begin_state,
        attention=attention,
        gate0=lambda: weight_grad(N.gate0, N.normed_two_t, N.gate_grad),
        gate1=lambda: weight_grad(N.gate1, N.normed_two_t, N.gate_grad, first),
        up0=lambda: weight_grad(N.up0, N.normed_two_t, N.lin_grad),
        up1=lambda: weight_grad(N.up1, N.normed_two_t, N.lin_grad, first),
        output=lambda: weight_grad(N.output, N.gated_t, N.middle_b),
        outgate=lambda: weight_grad(N.outgate, N.normed_t, N.outgate_grad),
        query=lambda: weight_grad(N.query, N.normed_t, N.query_grad),
        key=lambda: weight_grad(N.key, N.normed_t, N.key_grad),
        value=lambda: weight_grad(N.value, N.normed_t, N.value_grad),
        decay_down=decay_down,
        input_grad=input_grad,
        tiny=tiny,
    )
    run_plan(
        BACKWARD_PLAN,
        pieces,
        scan,
        None,
        lambda item, step: scatter.advance(item, step),
    )
    scatter.finish()
    scan.finish()
    ready(*list(loads))
    result.wait()


def backward(sizes, tokens, saved):
    outer, inner, side, core = sizes
    devices = outer * inner * side * core
    most = max(max(sizes) - 1, 1)
    rows, width = tokens.shape
    hidden = saved[N.gate_grad].shape[1]
    keys, values = HEADS * KEY_DIM, HEADS * VALUE_DIM
    mine = width // devices
    saved = dict(saved, tokens=tokens)
    ins = {N.in_ + name: (saved[name], False) for name in LOADED}
    ins[N.in_normed_two_grad] = (saved[N.normed_two_grad], False)
    for k in range(2):
        ins[N.in_near_down + str(k)] = (saved[N.near_down + str(k)], False)
    ins.update({N.in_weight_ + name: (saved[N.weight_ + name], False) for name in KEPT})
    items = scatter_items(hidden, width)
    block, scratch, sums = {}, {}, {}
    for name, (size, slot, out, start) in items.items():
        rows_of = RANK if out == N.tiny else mine
        if slot is None:
            rows_of = saved[N.near_down0].shape[3]
        dtype = f32 if out == N.tiny else bf16
        block = (rows_of, size)
        sums[N.out_ + out] = ((rows_of, start + size), f32, False)
        scratch[N.sum_ + out] = pltpu.VMEM((rows_of, start + size), f32)
        if slot is not None and N.slot_ + slot not in scratch:
            scratch[N.slot_ + slot] = pltpu.VMEM(sizes + block, dtype)
        steps = (3, 1, 0) if slot is None else (3, 2, 1, 0)
        scratch.update(landings(sizes, block, dtype, name, name in LATE_SCATTERED, steps))
    scratch.update({n: pltpu.VMEM(saved[n].shape, saved[n].dtype) for n in LOADED})
    scratch.update(
        {
            N.panel_ + n: pltpu.VMEM((2,) + saved[N.weight_ + n].shape[1:], bf16)
            for n, _ in NORMED_BACK
        }
    )
    scratch.update(
        rows_sum=pltpu.VMEM((8, width), f32),
        cumulative=pltpu.VMEM((rows, keys), f32),
        query_grad=pltpu.VMEM((rows, keys), bf16),
        key_grad=pltpu.VMEM((rows, keys), bf16),
        value_grad=pltpu.VMEM((rows, values), bf16),
        decay_grad=pltpu.VMEM((rows, keys), bf16),
        rank_grad=pltpu.VMEM((rows, LANES), bf16),
        normed_grad=pltpu.VMEM((rows, width), f32),
        send_sem=pltpu.SemaphoreType.DMA((len(items), 4, most)),
        recv_sem=pltpu.SemaphoreType.DMA((len(items), 4, most)),
        input_grad=pltpu.VMEM((rows, width), f32),
        own_sem=pltpu.SemaphoreType.DMA((2,)),
        out_sem=pltpu.SemaphoreType.DMA((len(items) + 1,)),
        load_sem=pltpu.SemaphoreType.DMA((len(LOADED) + 1,)),
        panel_sem=pltpu.SemaphoreType.DMA((len(NORMED_BACK), 2)),
    )
    scratch.update(scan_scratch(sizes))
    outs = dict(sums, out_input_grad=((rows, width), f32, False))
    return kernel_call(backward_kernel, sizes, ins, outs, scratch, 1)


def hand_out_kernel(count, cuts, *refs):
    whole, down, tiny = refs[:count], refs[count], refs[count + 1]
    refs = refs[count + 2 :]
    outs, small, held, sems = refs[:count], refs[count : -count - 1], refs[-count - 1 : -1], refs[-1]
    loads, copies = [], []
    for k in range(count):
        loads.append(pltpu.make_async_copy(whole[k], held[k], sems.at[0, k]))
        loads[-1].start()
        copies.append(pltpu.make_async_copy(held[k], outs[k], sems.at[1, k]))
    small[0][...] = turned(down[...], highest)[0 : small[0].shape[0]]
    for target, (row, column) in zip(small[1:], cuts):
        target[...] = tiny[row : row + target.shape[0], column : column + target.shape[1]]
    for load, copy in zip(loads, copies):
        load.wait()
        copy.start()
    for copy in copies:
        copy.wait()


def hand_out(arrays, decay_down, tiny, cuts):
    vmem = pl.BlockSpec(memory_space=pltpu.VMEM)
    anywhere = pl.BlockSpec(memory_space=pl.ANY)
    shapes = [a.shape for a in arrays] + [(RANK, decay_down.shape[0])] + [c[0] for c in cuts]
    return pl.pallas_call(
        functools.partial(hand_out_kernel, len(arrays), [c[1] for c in cuts]),
        out_shape=[jax.ShapeDtypeStruct(s, f32) for s in shapes],
        in_specs=[anywhere] * len(arrays) + [vmem] * 2,
        out_specs=[anywhere] * len(arrays) + [vmem] * (len(cuts) + 1),
        scratch_shapes=[pltpu.VMEM(a.shape, f32) for a in arrays]
        + [pltpu.SemaphoreType.DMA((2, len(arrays)))],
        compiler_params=pltpu.CompilerParams(vmem_limit_bytes=VMEM_LIMIT),
    )(*arrays, decay_down, tiny)


def local(
    sizes,
    inputs,
    cotangent,
    mixer_gain,
    feed_gain,
    w_query,
    w_key,
    w_value,
    w_outgate,
    w_decay_down,
    w_decay_up,
    decay_bias,
    head_gain,
    w_output,
    w_gate,
    w_up,
    w_down,
):
    width = inputs.shape[2]
    rows = inputs.shape[0] * inputs.shape[1]
    per_feature, per_key, per_value = (
        mixer_gain.shape[0],
        decay_bias.shape[0],
        head_gain.shape[0],
    )
    tokens = inputs.reshape(rows, width)
    small = dict(
        w_decay_up=w_decay_up,
        mixer_gain=mixer_gain.reshape(1, -1),
        feed_gain=feed_gain.reshape(1, -1),
        decay_bias=decay_bias.reshape(1, -1),
        head_gain=head_gain.reshape(1, -1),
    )
    weights = dict(
        decay_down=w_decay_down.T,
        query=w_query,
        key=w_key,
        value=w_value,
        outgate=w_outgate,
        output=w_output,
        gate=w_gate,
        up=w_up,
        down=w_down,
    )
    saved = forward(sizes, tokens, cotangent.reshape(rows, width), small, weights)
    got = backward(sizes, tokens, saved)
    names = (N.query, N.key, N.value, N.outgate, N.output, N.gate, N.up, N.down)
    handed = hand_out(
        [saved[N.middle], got[N.out_input_grad]]
        + [got[N.out_ + name] for name in names],
        got[N.out_decay_down],
        got[N.out_tiny],
        (
            ((RANK, per_key), (0, 0)),
            ((1, per_feature), (0, VECTORS)),
            ((1, per_feature), (1, VECTORS)),
            ((1, per_key), (2, VECTORS)),
            ((1, per_value), (3, VECTORS)),
        ),
    )
    result, input_grad = (a.reshape(inputs.shape) for a in handed[:2])
    g_query, g_key, g_value, g_outgate, g_output, g_gate, g_up, g_down = handed[2:10]
    decay_down, decay_up = handed[10:12]
    g_mixer, g_feed, g_bias, g_head = (a.reshape(-1) for a in handed[12:])
    return (
        result,
        input_grad,
        g_mixer,
        g_feed,
        g_query,
        g_key,
        g_value,
        g_outgate,
        decay_down.T,
        decay_up,
        g_bias,
        g_head,
        g_output,
        g_gate,
        g_up,
        g_down,
    )


def solution(mesh):
    placed = (
        P("batch", "seq", None),
        P("batch", "seq", None),
        P(("seq", "batch")),
        P(("seq", "batch")),
        P(("seq", "batch"), None),
        P(("seq", "batch"), None),
        P(("seq", "batch"), None),
        P(("seq", "batch"), None),
        P(("seq", "batch"), None),
        P(None, ("seq", "batch")),
        P(("seq", "batch")),
        P(("seq", "batch")),
        P(("seq", "batch"), None),
        P(("seq", "batch"), None),
        P(("seq", "batch"), None),
        P(("seq", "batch"), None),
    )
    return jax.shard_map(
        functools.partial(local, grid_of(mesh.shape)),
        mesh=mesh,
        in_specs=placed,
        out_specs=(
            P("batch", "seq", None),
            P("batch", "seq", None),
            P(("seq", "batch")),
            P(("seq", "batch")),
            P(("seq", "batch"), None),
            P(("seq", "batch"), None),
            P(("seq", "batch"), None),
            P(("seq", "batch"), None),
            P(("seq", "batch"), None),
            P(None, ("seq", "batch")),
            P(("seq", "batch")),
            P(("seq", "batch")),
            P(("seq", "batch"), None),
            P(("seq", "batch"), None),
            P(("seq", "batch"), None),
            P(("seq", "batch"), None),
        ),
        check_vma=False,
    )
```
